8 devices in a mesh: dp: 2 (over z, y), ep: 4 (over x, core).
Axes of the slice: x: 2, y: 2, z: 1, core: 2. Of those that a mesh axis runs over, the one named last changes fastest.
Arguments:
- x_norm: bfloat16 [2048, 1536], P(('dp', 'ep'))
- route_idx: int32 [2048, 8], P(('dp', 'ep'))
- w_router: bfloat16 [1536, 40], replicated
- w_gate: bfloat16 [40, 1536, 512], P('ep')
- w_up: bfloat16 [40, 1536, 512], P('ep')
- w_down: bfloat16 [40, 512, 1536], P('ep')
- grad_out: bfloat16 [2048, 1536], P(('dp', 'ep'))
Outputs:
- output 1: bfloat16 [2048, 1536], P(('dp', 'ep'))
- output 2: float32 [40, 1536, 512], P('ep')
- output 3: float32 [40, 1536, 512], P('ep')
- output 4: float32 [40, 512, 1536], P('ep')
- output 5: float32 [1536, 40], replicated
All inputs are finite; a program needn't handle non-finite values.
Results may differ from the reference program's by a relative error of at most 0.00564174.
Values are sent between devices in bfloat16 or wider.
A program may use at most 1 GiB of HBM per device.

```python
import jax
import jax.numpy as jnp
from jax import lax

D = 1536
FF = 512
EXPERTS = 40
TOP = 8
TOK_DEV = 256
SHARDS = 8
CAP = 153
TOKENS = SHARDS * TOK_DEV
N_CHOICE = TOKENS * TOP


def shuffle_rows(row_key):
    return jax.random.permutation(row_key, TOK_DEV)


def permute_rows(shard_rows, row_order):
    return shard_rows[row_order]


def draw_routes(route_key):
    perm_key, shift_key, order_key = jax.random.split(route_key, 3)
    expert_order = jax.random.permutation(perm_key, EXPERTS).astype(jnp.int32)
    shifts = jax.random.randint(shift_key, (SHARDS,), 0, EXPERTS - 1, dtype=jnp.int32)
    tok_pos = jnp.arange(TOK_DEV, dtype=jnp.int32)
    choice_pos = jnp.arange(TOP, dtype=jnp.int32)
    is_hot = tok_pos < CAP
    cycle_pos = (tok_pos * TOP - jnp.minimum(tok_pos, CAP))[:, None] + choice_pos[None, :] - is_hot[:, None].astype(jnp.int32)
    labels = 1 + (cycle_pos[None, :, :] + shifts[:, None, None]) % (EXPERTS - 1)
    hot_slot = is_hot[:, None] & (choice_pos[None, :] == 0)
    labels = jnp.where(hot_slot[None, :, :], 0, labels)
    experts = expert_order[labels]
    row_orders = jax.vmap(shuffle_rows)(jax.random.split(order_key, SHARDS))
    experts = jax.vmap(permute_rows)(experts, row_orders)
    return experts.reshape(TOKENS, TOP).astype(jnp.int32)


def setup_inputs(seed: int = 0) -> dict:
    base_key = jax.random.key(seed)
    key_list = jax.random.split(base_key, 7)
    x_norm = jax.random.normal(key_list[0], (TOKENS, D), jnp.float32)
    w_router = jax.random.normal(key_list[2], (D, EXPERTS), jnp.float32) * D ** -0.5
    w_gate = jax.random.normal(key_list[3], (EXPERTS, D, FF), jnp.float32) * D ** -0.5
    w_up = jax.random.normal(key_list[4], (EXPERTS, D, FF), jnp.float32) * D ** -0.5
    w_down = jax.random.normal(key_list[5], (EXPERTS, FF, D), jnp.float32) * FF ** -0.5
    grad_out = jax.random.normal(key_list[6], (TOKENS, D), jnp.float32)
    return {
        "x_norm": x_norm.astype(jnp.bfloat16),
        "route_idx": draw_routes(key_list[1]),
        "w_router": w_router.astype(jnp.bfloat16),
        "w_gate": w_gate.astype(jnp.bfloat16),
        "w_up": w_up.astype(jnp.bfloat16),
        "w_down": w_down.astype(jnp.bfloat16),
        "grad_out": grad_out.astype(jnp.bfloat16),
    }


def expert_backward(x_rows, dy_rows, gate_rows, w_gate_e, w_up_e, w_down_e):
    z_gate = jnp.dot(x_rows, w_gate_e, preferred_element_type=jnp.float32)
    z_up = jnp.dot(x_rows, w_up_e, preferred_element_type=jnp.float32)
    sigmoid_z = jax.nn.sigmoid(z_gate)
    silu_z = z_gate * sigmoid_z
    act_rows = (silu_z * z_up).astype(jnp.bfloat16)
    out_rows = jnp.dot(act_rows, w_down_e, preferred_element_type=jnp.float32)
    dy_wide = dy_rows.astype(jnp.float32)
    dgate_rows = jnp.sum(out_rows * dy_wide, axis=1)
    d_out = (gate_rows[:, None] * dy_wide).astype(jnp.bfloat16)
    d_act = jnp.dot(d_out, w_down_e.T, preferred_element_type=jnp.float32)
    d_zgate = (d_act * z_up * sigmoid_z * (1.0 + z_gate * (1.0 - sigmoid_z))).astype(jnp.bfloat16)
    d_zup = (d_act * silu_z).astype(jnp.bfloat16)
    dx_rows = (jnp.dot(d_zgate, w_gate_e.T, preferred_element_type=jnp.float32) + jnp.dot(d_zup, w_up_e.T, preferred_element_type=jnp.float32)).astype(jnp.bfloat16)
    grad_gate = jnp.dot(x_rows.T, d_zgate, preferred_element_type=jnp.float32)
    grad_up = jnp.dot(x_rows.T, d_zup, preferred_element_type=jnp.float32)
    grad_down = jnp.dot(act_rows.T, d_out, preferred_element_type=jnp.float32)
    return dx_rows, dgate_rows, grad_gate, grad_up, grad_down


def reference(x_norm, route_idx, w_router, w_gate, w_up, w_down, grad_out):
    logits = jnp.dot(x_norm, w_router, preferred_element_type=jnp.float32)
    gate_probs = jax.nn.softmax(jnp.take_along_axis(logits, route_idx, axis=1), axis=-1)
    expert_ids = jnp.arange(EXPERTS, dtype=jnp.int32)
    shard_idx = route_idx.reshape(SHARDS, TOK_DEV * TOP)
    one_hot = (shard_idx[:, :, None] == expert_ids).astype(jnp.int32)
    rank_in = jnp.sum((jnp.cumsum(one_hot, axis=1) - one_hot) * one_hot, axis=2)
    slot_ids = (shard_idx * (SHARDS * CAP) + jnp.arange(SHARDS, dtype=jnp.int32)[:, None] * CAP + rank_in).reshape(N_CHOICE)
    slot_table = jnp.full((EXPERTS * SHARDS * CAP,), N_CHOICE, jnp.int32).at[slot_ids].set(jnp.arange(N_CHOICE, dtype=jnp.int32)).reshape(EXPERTS, SHARDS * CAP)
    gate_flat = gate_probs.reshape(N_CHOICE)

    def one_expert(operands):
        w_gate_e, w_up_e, w_down_e, choice_ids = operands
        is_valid = choice_ids < N_CHOICE
        safe_ids = jnp.minimum(choice_ids, N_CHOICE - 1)
        x_rows = jnp.where(is_valid[:, None], x_norm[safe_ids // TOP], 0.0)
        dy_rows = jnp.where(is_valid[:, None], grad_out[safe_ids // TOP], 0.0)
        gate_rows = jnp.where(is_valid, gate_flat[safe_ids], 0.0)
        return expert_backward(x_rows, dy_rows, gate_rows, w_gate_e, w_up_e, w_down_e)

    dx_rows, dgate_rows, grad_gate, grad_up, grad_down = lax.map(one_expert, (w_gate, w_up, w_down, slot_table))
    dx_choice = dx_rows.reshape(EXPERTS * SHARDS * CAP, D)[slot_ids].reshape(TOKENS, TOP, D)
    dgate = dgate_rows.reshape(EXPERTS * SHARDS * CAP)[slot_ids].reshape(TOKENS, TOP)
    d_sel = gate_probs * (dgate - jnp.sum(gate_probs * dgate, axis=1, keepdims=True))
    d_logits = jnp.sum(jnp.where(route_idx[:, :, None] == expert_ids, d_sel[:, :, None], 0.0), axis=1).astype(jnp.bfloat16)
    du_router = jnp.dot(d_logits, w_router.T, preferred_element_type=jnp.float32)
    grad_x = (jnp.sum(dx_choice.astype(jnp.float32), axis=1) + du_router).astype(jnp.bfloat16)
    grad_router = jnp.dot(x_norm.T, d_logits, preferred_element_type=jnp.float32)
    return grad_x, grad_gate, grad_up, grad_down, grad_router
```

```python
import functools

import jax
import jax.numpy as jnp
from jax import lax
from jax.experimental import pallas as pl
from jax.experimental.pallas import tpu as pltpu
from jax.sharding import PartitionSpec as P

SLOTS = 64
EXTRA = 96
PAD = 16
F32 = jnp.float32
BF16 = jnp.bfloat16
VMEM_LIMIT = 67043328
MESH = pl.DeviceIdType.MESH


def nt_dot(a, b):
    return lax.dot_general(a, b, (((1,), (1,)), ((), ())), preferred_element_type=F32)


def tn_dot(a, b):
    return lax.dot_general(a, b, (((0,), (0,)), ((), ())), preferred_element_type=F32)


def nn_dot(a, b):
    return jnp.dot(a, b, preferred_element_type=F32)


def slot_mask(rank_row, rows, first):
    slot = lax.broadcasted_iota(jnp.int32, (rows, rank_row.shape[1]), 0) + first
    return slot.astype(F32) == rank_row


def hot_rows(rank):
    return jnp.max(rank, axis=1, keepdims=True) >= SLOTS


def extra_rank(rank):
    return jnp.max(jnp.where(hot_rows(rank), rank, -1.0), axis=0, keepdims=True)


def route_kernel(groups, per_group, x_ref, wr_ref, idx_ref, out_ref):
    rows, toks = groups * PAD, x_ref.shape[0]
    logits = nt_dot(wr_ref[...], x_ref[...])
    row = lax.broadcasted_iota(jnp.int32, (rows, toks), 0)
    expert = jnp.where(row % PAD < per_group, (row // PAD) * per_group + row % PAD, -1)
    chosen = expert == idx_ref[0:1, :]
    for k in range(1, idx_ref.shape[0]):
        chosen = chosen | (expert == idx_ref[k : k + 1, :])
    before = lax.broadcasted_iota(jnp.int32, (toks, toks), 0) < lax.broadcasted_iota(jnp.int32, (toks, toks), 1)
    rank = nn_dot(chosen.astype(F32).astype(BF16), before.astype(F32).astype(BF16))
    top = jnp.max(jnp.where(chosen, logits, -jnp.inf), axis=0, keepdims=True)
    weight = jnp.where(chosen, jnp.exp(logits - top), 0.0)
    prob = weight / jnp.sum(weight, axis=0, keepdims=True)
    out_ref[0] = jnp.where(chosen, rank, -1.0).reshape(groups, PAD, toks)
    out_ref[1] = prob.reshape(groups, PAD, toks)


def gather_rows(me, per_group, m_ref, x_ref, g_ref, x_out, d_out, g_out):
    step = per_group // 2

    def emit(masks, probs, where):
        pick = jnp.concatenate([m.astype(F32).astype(BF16) for m in masks], axis=0)
        gate = jnp.concatenate([jnp.sum(jnp.where(m, p, 0.0), axis=1, keepdims=True) for m, p in zip(masks, probs)], axis=0)
        x_out[where, :] = nn_dot(pick, x_ref[...]).astype(BF16)
        rows_g = nn_dot(pick, g_ref[...])
        if g_out is not None:
            g_out[where, :] = rows_g.astype(BF16)
        d_out[where, :] = (gate * rows_g).astype(BF16)

    def part(i, carry):
        ranks = [m_ref[0, me, pl.ds(i * step + k, 1), :] for k in range(step)]
        probs = [m_ref[1, me, pl.ds(i * step + k, 1), :] for k in range(step)]
        emit([slot_mask(r, SLOTS, 0) for r in ranks], probs, pl.ds(pl.multiple_of(i * (step * SLOTS), SLOTS), step * SLOTS))
        return carry

    lax.fori_loop(0, 2, part, 0)
    rank, prob = m_ref[0, me], m_ref[1, me]
    prob_hot = jnp.sum(jnp.where(hot_rows(rank), prob, 0.0), axis=0, keepdims=True)
    emit([slot_mask(extra_rank(rank), EXTRA, SLOTS)], [prob_hot], pl.ds(per_group * SLOTS, EXTRA))


class Stage:
    def __init__(self, main, bufs, sems, outs):
        self.main, self.bufs, self.sems, self.outs, self.busy = main, bufs, sems, outs, {}

    def gather(self, i, kinds, me, per_group, m_ref, x_ref, g_ref):
        slot = i % 2
        self.drain(slot)
        views = [self.bufs[k].at[slot] for k in range(kinds)]
        gather_rows(me, per_group, m_ref, x_ref, g_ref, *(views + [None])[:3])
        copies = []
        for k in range(kinds):
            copies.append(pltpu.make_async_copy(views[k].at[pl.ds(0, self.main)], self.outs[2 * k].at[i], self.sems.at[slot, 2 * k]))
            copies.append(pltpu.make_async_copy(views[k].at[pl.ds(self.main, EXTRA)], self.outs[2 * k + 1].at[i], self.sems.at[slot, 2 * k + 1]))
        for c in copies:
            c.start()
        self.busy[slot] = copies

    def drain(self, slot):
        for c in self.busy.pop(slot, ()):
            c.wait()


def device_of(bit):
    return (lax.axis_index("dp") ^ (bit >> 2), lax.axis_index("ep") ^ (bit & 3))


def greet(bits):
    barrier = pltpu.get_barrier_semaphore()
    for bit in bits:
        pl.semaphore_signal(barrier, inc=1, device_id=device_of(bit), device_id_type=MESH)
    pl.semaphore_wait(barrier, len(bits))


def near_kernel(per_group, x_ref, g_ref, m_ref, *refs):
    rows_out, (xs_out, ms_out, g2_out) = refs[:6], refs[6:9]
    x_in, g_in, m_in, st_x, st_d, st_g, send, recv, out_sem, st_sem = refs[9:]
    me = lax.axis_index("ep")
    greet((1, 2, 4))
    own = (x_ref, g_ref, m_ref)
    land = lambda s: (x_in.at[s - 1], g_in.at[s - 1], m_in.at[s - 1])

    def push(srcs, s, bit):
        copies = []
        for k, (src, dst) in enumerate(zip(srcs, land(s))):
            copies.append(pltpu.make_async_remote_copy(src_ref=src, dst_ref=dst, send_sem=send.at[s - 1, k], recv_sem=recv.at[s - 1, k], device_id=device_of(bit), device_id_type=MESH))
        for c in copies:
            c.start()
        return copies

    flights = {2: push(own, 2, 2), 4: push(own, 4, 4), 1: push(own, 1, 1)}
    outs = []

    def arrive(s):
        for c in flights[s]:
            c.wait_recv()
        keep = [pltpu.make_async_copy(x_in.at[s - 1], xs_out.at[s - 1], out_sem.at[s - 1, 0]), pltpu.make_async_copy(m_in.at[s - 1], ms_out.at[s - 1], out_sem.at[s - 1, 1])]
        if s == 2:
            keep.append(pltpu.make_async_copy(g_in.at[s - 1], g2_out, out_sem.at[s - 1, 2]))
        for c in keep:
            c.start()
        outs.extend(keep)

    stage = Stage(per_group * SLOTS, (st_x, st_d, st_g), st_sem, rows_out)

    def gather(s):
        x, g, m = own if s == 0 else land(s)
        stage.gather(s, 3 if s < 4 else 2, me, per_group, m, x, g)

    gather(0)
    arrive(1)
    gather(1)
    arrive(2)
    flights[3] = push(land(2), 3, 1)
    arrive(4)
    flights[5] = push(land(4), 5, 1)
    gather(2)
    arrive(3)
    gather(3)
    gather(4)
    arrive(5)
    gather(5)
    stage.drain(0)
    stage.drain(1)
    for s in flights:
        for c in flights[s]:
            c.wait_send()
    for c in outs:
        c.wait()


def back_kernel(per_group, x6_ref, g6_ref, m6_ref, q_ref, gx_ref, *refs):
    rows_out, (x7_ref, m7_ref, me_ref, peer_ref, q_out) = refs[:4], refs[4:9]
    x7_in, g7_in, m7_in, part_in, q_in, st_x, st_d, send, recv, q_send, q_recv, ld_sem, st_sem = refs[9:]
    me = lax.axis_index("ep")
    n_dev = q_in.shape[0]
    greet(tuple(range(1, n_dev)))

    def push(src, dst, i, bit, s_sem, r_sem):
        c = pltpu.make_async_remote_copy(src_ref=src, dst_ref=dst, send_sem=s_sem.at[i], recv_sem=r_sem.at[i], device_id=device_of(bit), device_id_type=MESH)
        c.start()
        return c

    qs = [push(q_ref, q_in.at[bit], bit, bit, q_send, q_recv) for bit in range(1, n_dev)]
    sevens = [push(src, dst, i, 1, send, recv) for i, (src, dst) in enumerate(((x6_ref, x7_in), (g6_ref, g7_in), (m6_ref, m7_in)))]
    parts = [push(gx_ref.at[2 * h + 1], part_in.at[h], 3 + h, 1, send, recv) for h in range(2)]
    loads = [pltpu.make_async_copy(gx_ref.at[2 * h], dst, ld_sem.at[h]) for h, dst in enumerate((me_ref, peer_ref))]
    for c in loads:
        c.start()
    stage = Stage(per_group * SLOTS, (st_x, st_d), st_sem, rows_out)
    stage.gather(0, 2, me, per_group, m6_ref, x6_ref, g6_ref)
    for c in sevens:
        c.wait_recv()
    stage.gather(1, 2, me, per_group, m7_in, x7_in, g7_in)
    x7_ref[...] = x7_in[...]
    m7_ref[...] = m7_in[...]
    q_out[0] = q_ref[...]
    for bit, c in enumerate(qs):
        c.wait_recv()
        q_out[bit + 1] = q_in[bit + 1]
    for h, dst in enumerate((me_ref, peer_ref)):
        loads[h].wait()
        parts[h].wait_recv()
        dst[...] += part_in[h]
    stage.drain(0)
    stage.drain(1)
    for c in qs + sevens + parts:
        c.wait_send()


def expert_math(x, d, w1, w3, w2):
    z1 = nn_dot(x, w1)
    z3 = nn_dot(x, w3)
    sig = jax.nn.sigmoid(z1)
    silu = z1 * sig
    act = (silu * z3).astype(BF16)
    d_act = nt_dot(d, w2)
    dz1 = (d_act * z3 * sig * (1.0 + z1 * (1.0 - sig))).astype(BF16)
    dz3 = (d_act * silu).astype(BF16)
    return act, dz1, dz3


def flat(ref, first=0, count=None):
    v = ref[first : first + (count or ref.shape[0])]
    return v.reshape(v.shape[0] * v.shape[1], v.shape[2])


def pass1_kernel(n_sh, per_group, hot_ref, ep_ref, w1_ref, w3_ref, w2_ref, x_ref, d_ref, g_ref, xo_ref, do_ref, go_ref, *refs):
    m_refs = refs[:n_sh]
    gx_ref, q_ref, act_ref, dz_ref, r_scr = refs[n_sh:]
    e = pl.program_id(0)
    ff = w1_ref.shape[2]
    w1, w3, w2 = w1_ref[0], w3_ref[0], w2_ref[0]
    base = per_group * SLOTS

    def token_math(x, d, g):
        act, dz1, dz3 = expert_math(x, d, w1, w3, w2)
        q = jnp.sum(nn_dot(act, w2) * g.astype(F32), axis=1, keepdims=True)
        r = (nt_dot(dz1, w1) + nt_dot(dz3, w3)).astype(BF16)
        return act, dz1, dz3, q, r

    @pl.when(e == 0)
    def _():
        r_scr[:, base : base + EXTRA, :] = jnp.zeros((n_sh, EXTRA, r_scr.shape[2]), BF16)
        q_ref[...] = jnp.zeros_like(q_ref)

    act, dz1, dz3, q, r = token_math(flat(x_ref), flat(d_ref), flat(g_ref))
    act_ref[0] = act
    dz_ref[0, :, :ff] = dz1
    dz_ref[0, :, ff:] = dz3
    for j in range(n_sh):
        rank_row = m_refs[j][0, 0, pl.ds(e, 1), :]
        mask = slot_mask(rank_row, SLOTS, 0)
        q_ref[j, pl.ds(e, 1), :] = jnp.sum(jnp.where(mask, q[j * SLOTS : (j + 1) * SLOTS], 0.0), axis=0, keepdims=True)
        r_scr[j, pl.ds(pl.multiple_of(e * SLOTS, SLOTS), SLOTS), :] = r[j * SLOTS : (j + 1) * SLOTS]

    is_hot = [hot_ref[e * n_sh + j] for j in range(n_sh)]

    @pl.when(sum(is_hot) > 0)
    def _():
        d = jnp.concatenate([do_ref[j] * is_hot[j].astype(F32).astype(BF16) for j in range(n_sh)], axis=0)
        _, _, _, q, r = token_math(flat(xo_ref), d, flat(go_ref))
        for j in range(n_sh):

            @pl.when(is_hot[j] > 0)
            def _():
                rank_row = m_refs[j][0, 0, pl.ds(e, 1), :]
                mask = slot_mask(rank_row, EXTRA, SLOTS)
                q_ref[j, pl.ds(e, 1), :] += jnp.sum(jnp.where(mask, q[j * EXTRA : (j + 1) * EXTRA], 0.0), axis=0, keepdims=True)
                r_scr[j, base : base + EXTRA, :] = r[j * EXTRA : (j + 1) * EXTRA]

    @pl.when(e == per_group - 1)
    def _():
        for j in range(n_sh):
            rank = m_refs[j][0, 0]
            masks = [slot_mask(rank[i : i + 1, :], SLOTS, 0) for i in range(per_group)]
            masks.append(slot_mask(extra_rank(rank), EXTRA, SLOTS))
            pick = jnp.concatenate([m.astype(F32).astype(BF16) for m in masks], axis=0)
            gx_ref[j] = tn_dot(pick, r_scr[j])


def pass2_kernel(n_near, hot_ref, w1_ref, w3_ref, w2_ref, act_ref, dz_ref, x_ref, d_ref, xf_ref, df_ref, xo_ref, do_ref, xfo_ref, dfo_ref, g1_ref, g3_ref, g2_ref):
    n_sh = x_ref.shape[0] + xf_ref.shape[0]
    e = pl.program_id(0)
    ff = w1_ref.shape[2]
    w1, w3, w2 = w1_ref[0], w3_ref[0], w2_ref[0]
    n_mid = x_ref.shape[0] - n_near
    x = jnp.concatenate([flat(x_ref), flat(xf_ref)], axis=0)
    d = jnp.concatenate([flat(d_ref), flat(df_ref)], axis=0)
    near = n_near * SLOTS
    act, dz1, dz3 = expert_math(x[near:], d[near:], w1, w3, w2)
    g1_ref[0] = tn_dot(x, jnp.concatenate([dz_ref[0, :, :ff], dz1], axis=0))
    g3_ref[0] = tn_dot(x, jnp.concatenate([dz_ref[0, :, ff:], dz3], axis=0))
    g2_ref[0] = tn_dot(jnp.concatenate([act_ref[0], act], axis=0), d)

    hot = [hot_ref[e * n_sh + j] for j in range(n_sh)]
    for far in range(2):
        is_hot = hot[n_near:] if far else hot[:n_near]

        @pl.when(sum(is_hot) > 0)
        def _():
            if far:
                x = jnp.concatenate([flat(xo_ref, n_near, n_mid), flat(xfo_ref)], axis=0)
                ds = [do_ref[n_near + i] for i in range(n_mid)] + [dfo_ref[i] for i in range(n_near - n_mid)]
            else:
                x = flat(xo_ref, 0, n_near)
                ds = [do_ref[i] for i in range(n_near)]
            d = jnp.concatenate([v * h.astype(F32).astype(BF16) for v, h in zip(ds, is_hot)], axis=0)
            act, dz1, dz3 = expert_math(x, d, w1, w3, w2)
            g1_ref[0] += tn_dot(x, dz1)
            g3_ref[0] += tn_dot(x, dz3)
            g2_ref[0] += tn_dot(act, d)


def finish_kernel(groups, ep_ref, keep_ref, far_ref, wr_ref, x0_ref, xs_ref, x6_ref, x7_ref, m0_ref, ms_ref, m6_ref, m7_ref, q_ref, gx_ref, gr_ref):
    n_sh = q_ref.shape[0]
    x_refs = [x0_ref] + [xs_ref.at[i] for i in range(n_sh - 3)] + [x6_ref, x7_ref]
    m_refs = [m0_ref] + [ms_ref.at[i] for i in range(n_sh - 3)] + [m6_ref, m7_ref]
    ep = ep_ref[0]
    for s in range(n_sh):
        d, j = divmod(s, groups)
        q = jnp.concatenate([q_ref[d * groups + (ep ^ a), (ep ^ a) ^ j] for a in range(groups)], axis=0)
        p = m_refs[s][1].reshape(groups * PAD, q.shape[1])
        dl = p * (q - jnp.sum(p * q, axis=0, keepdims=True))
        dl = dl.astype(BF16)
        term = nn_dot(dl, x_refs[s][...])
        if s == 0:
            du = tn_dot(dl, wr_ref[...])
            gx_ref[...] = (keep_ref[...] + far_ref[...] + du).astype(BF16)
            gr_ref[...] = term
        else:
            gr_ref[...] += term


def solution(mesh):
    dp, ep = mesh.shape["dp"], mesh.shape["ep"]
    n_dev = dp * ep
    tok_spec = P(("dp", "ep"), None)
    exp_spec = P("ep", None, None)

    def swap(v, bit):
        return lax.ppermute(v, ("dp", "ep"), [(s, s ^ bit) for s in range(n_dev)])

    def device_step(x_loc, route_idx, w_router, w_gate, w_up, w_down, dy_loc):
        toks, dim = x_loc.shape
        n_exp = w_router.shape[1]
        n_loc, _, ff = w_gate.shape
        me = lax.axis_index("ep")
        ep_arr = me.reshape(1).astype(jnp.int32)
        vmem = pl.BlockSpec(memory_space=pltpu.VMEM)
        params = pltpu.CompilerParams(vmem_limit_bytes=VMEM_LIMIT)

        wr_rows = jnp.pad(w_router.T.reshape(ep, n_loc, dim), ((0, 0), (0, PAD - n_loc), (0, 0))).reshape(ep * PAD, dim)
        route = pl.pallas_call(
            functools.partial(route_kernel, ep, n_loc),
            out_shape=jax.ShapeDtypeStruct((2, ep, PAD, toks), F32),
            in_specs=[vmem] * 3,
            out_specs=vmem,
            compiler_params=params,
            cost_estimate=pl.CostEstimate(flops=10**9, bytes_accessed=10**6, transcendentals=0),
            name="route",
        )(x_loc, wr_rows, route_idx.T)

        hbm = pl.BlockSpec(memory_space=pl.ANY)
        main = n_loc * SLOTS
        sds = jax.ShapeDtypeStruct
        m_shape = route.shape
        near_out = pl.pallas_call(
            functools.partial(near_kernel, n_loc),
            out_shape=[
                sds((6, main, dim), BF16),
                sds((6, EXTRA, dim), BF16),
                sds((6, main, dim), BF16),
                sds((6, EXTRA, dim), BF16),
                sds((4, main, dim), BF16),
                sds((4, EXTRA, dim), BF16),
                sds((5, toks, dim), BF16),
                sds((5,) + m_shape, F32),
                sds((toks, dim), BF16),
            ],
            in_specs=[vmem] * 3,
            out_specs=[hbm] * 9,
            scratch_shapes=[
                pltpu.VMEM((5, toks, dim), BF16),
                pltpu.VMEM((5, toks, dim), BF16),
                pltpu.VMEM((5,) + m_shape, F32),
                pltpu.VMEM((2, main + EXTRA, dim), BF16),
                pltpu.VMEM((2, main + EXTRA, dim), BF16),
                pltpu.VMEM((2, main + EXTRA, dim), BF16),
                pltpu.SemaphoreType.DMA((5, 3)),
                pltpu.SemaphoreType.DMA((5, 3)),
                pltpu.SemaphoreType.DMA((5, 3)),
                pltpu.SemaphoreType.DMA((2, 6)),
            ],
            compiler_params=pltpu.CompilerParams(collective_id=0, has_side_effects=True, vmem_limit_bytes=VMEM_LIMIT),
            cost_estimate=pl.CostEstimate(flops=2 * 10**10, bytes_accessed=5 * 10**7, transcendentals=0),
            name="near",
        )(x_loc, dy_loc, route)
        x_rows, x_more, d_rows, d_more, g_rows, g_more, xs, ms, g2 = near_out
        x6, g6, m6 = swap(xs[1], 4), swap(g2, 4), swap(ms[1], 4)

        def hot_flags(m_list):
            ranks = jnp.stack([lax.dynamic_index_in_dim(m[0], me, 0, keepdims=False) for m in m_list])
            return (jnp.max(ranks, axis=2) >= SLOTS).astype(jnp.int32)[:, :n_loc].T.reshape(-1)

        m_near = [route] + [ms[i] for i in range(5)]
        w_specs = lambda im: [pl.BlockSpec((1, dim, ff), im), pl.BlockSpec((1, dim, ff), im), pl.BlockSpec((1, ff, dim), im)]

        im3 = lambda e, hot, ep_ref: (e, 0, 0)
        rows_at = lambda e, hot, ep_ref: (0, e, 0)
        fix = lambda shape: pl.BlockSpec(shape, lambda e, hot, ep_ref: (0,) * len(shape), pipeline_mode=pl.Buffered(1))
        n_row = ep * SLOTS
        gx_part, q_loc, act, dz = pl.pallas_call(
            functools.partial(pass1_kernel, ep, n_loc),
            out_shape=[
                jax.ShapeDtypeStruct((ep, toks, dim), F32),
                jax.ShapeDtypeStruct((ep, PAD, toks), F32),
                jax.ShapeDtypeStruct((n_loc, n_row, ff), BF16),
                jax.ShapeDtypeStruct((n_loc, n_row, 2 * ff), BF16),
            ],
            grid_spec=pltpu.PrefetchScalarGridSpec(
                num_scalar_prefetch=2,
                grid=(n_loc,),
                in_specs=w_specs(im3)
                + [pl.BlockSpec((ep, SLOTS, dim), rows_at)] * 3
                + [fix((ep, EXTRA, dim))] * 3
                + [pl.BlockSpec((1, 1, PAD, toks), lambda e, hot, ep_ref: (0, ep_ref[0], 0, 0))] * ep,
                out_specs=[fix((ep, toks, dim)), fix((ep, PAD, toks)), pl.BlockSpec((1, n_row, ff), im3), pl.BlockSpec((1, n_row, 2 * ff), im3)],
                scratch_shapes=[pltpu.VMEM((ep, n_loc * SLOTS + EXTRA, dim), BF16)],
            ),
            compiler_params=params,
            cost_estimate=pl.CostEstimate(flops=4 * 10**10, bytes_accessed=10**8, transcendentals=0),
            name="pass1",
        )(
            hot_flags(m_near[:ep]),
            ep_arr,
            w_gate,
            w_up,
            w_down,
            x_rows,
            d_rows,
            g_rows,
            x_more,
            d_more,
            g_more,
            *m_near[:ep],
        )

        sum_shape = sds((toks, dim), F32)
        back_out = pl.pallas_call(
            functools.partial(back_kernel, n_loc),
            out_shape=[
                sds((2, main, dim), BF16),
                sds((2, EXTRA, dim), BF16),
                sds((2, main, dim), BF16),
                sds((2, EXTRA, dim), BF16),
                sds((toks, dim), BF16),
                sds(m_shape, F32),
                sum_shape,
                sum_shape,
                sds((n_dev, ep, PAD, toks), F32),
            ],
            in_specs=[vmem] * 4 + [hbm],
            out_specs=[hbm] * 4 + [vmem] * 5,
            scratch_shapes=[
                pltpu.VMEM((toks, dim), BF16),
                pltpu.VMEM((toks, dim), BF16),
                pltpu.VMEM(m_shape, F32),
                pltpu.VMEM((2, toks, dim), F32),
                pltpu.VMEM((n_dev, ep, PAD, toks), F32),
                pltpu.VMEM((2, main + EXTRA, dim), BF16),
                pltpu.VMEM((2, main + EXTRA, dim), BF16),
                pltpu.SemaphoreType.DMA((5,)),
                pltpu.SemaphoreType.DMA((5,)),
                pltpu.SemaphoreType.DMA((n_dev,)),
                pltpu.SemaphoreType.DMA((n_dev,)),
                pltpu.SemaphoreType.DMA((2,)),
                pltpu.SemaphoreType.DMA((2, 4)),
            ],
            compiler_params=pltpu.CompilerParams(collective_id=1, has_side_effects=True, vmem_limit_bytes=VMEM_LIMIT),
            cost_estimate=pl.CostEstimate(flops=8 * 10**9, bytes_accessed=5 * 10**7, transcendentals=0),
            name="back",
        )(x6, g6, m6, q_loc, gx_part)
        xf_rows, xf_more, df_rows, df_more, x7, m7, for_me, for_peer, q_all = back_out
        from_peer = swap(for_peer, 2)

        im3 = lambda e, hot: (e, 0, 0)
        rows_at = lambda e, hot: (0, e, 0)
        fix = lambda shape: pl.BlockSpec(shape, lambda e, hot: (0,) * len(shape), pipeline_mode=pl.Buffered(1))
        grad_gate, grad_up, grad_down = pl.pallas_call(
            functools.partial(pass2_kernel, ep),
            out_shape=[
                jax.ShapeDtypeStruct((n_loc, dim, ff), F32),
                jax.ShapeDtypeStruct((n_loc, dim, ff), F32),
                jax.ShapeDtypeStruct((n_loc, ff, dim), F32),
            ],
            grid_spec=pltpu.PrefetchScalarGridSpec(
                num_scalar_prefetch=1,
                grid=(n_loc,),
                in_specs=w_specs(im3)
                + [pl.BlockSpec((1, n_row, ff), im3), pl.BlockSpec((1, n_row, 2 * ff), im3)]
                + [pl.BlockSpec((6, SLOTS, dim), rows_at)] * 2
                + [pl.BlockSpec((2, SLOTS, dim), rows_at)] * 2
                + [fix((6, EXTRA, dim))] * 2
                + [fix((2, EXTRA, dim))] * 2,
                out_specs=w_specs(im3),
            ),
            compiler_params=params,
            cost_estimate=pl.CostEstimate(flops=6 * 10**10, bytes_accessed=2 * 10**8, transcendentals=0),
            name="pass2",
        )(
            hot_flags(m_near + [m6, m7]),
            w_gate,
            w_up,
            w_down,
            act,
            dz,
            x_rows,
            d_rows,
            xf_rows,
            df_rows,
            x_more,
            d_more,
            xf_more,
            df_more,
        )

        fixed = lambda shape: pl.BlockSpec(shape, lambda i, ep_ref: (0,) * len(shape))
        grad_x, grad_rt = pl.pallas_call(
            functools.partial(finish_kernel, ep),
            out_shape=[jax.ShapeDtypeStruct((toks, dim), BF16), jax.ShapeDtypeStruct((ep * PAD, dim), F32)],
            grid_spec=pltpu.PrefetchScalarGridSpec(
                num_scalar_prefetch=1,
                grid=(1,),
                in_specs=[fixed((toks, dim)), fixed((toks, dim)), fixed((ep * PAD, dim))]
                + [fixed(v.shape) for v in (x_loc, xs, x6, x7, route, ms, m6, m7, q_all)],
                out_specs=[fixed((toks, dim)), fixed((ep * PAD, dim))],
            ),
            compiler_params=params,
            cost_estimate=pl.CostEstimate(flops=4 * 10**9, bytes_accessed=10**7, transcendentals=0),
            name="finish",
        )(ep_arr, for_me, from_peer, wr_rows, x_loc, xs, x6, x7, route, ms, m6, m7, q_all)
        grad_router = grad_rt.reshape(ep, PAD, dim)[:, :n_loc].reshape(n_exp, dim).T
        return grad_x, grad_gate, grad_up, grad_down, grad_router

    return jax.shard_map(device_step, mesh=mesh, in_specs=(tok_spec, tok_spec, P(), exp_spec, exp_spec, exp_spec, tok_spec), out_specs=(tok_spec, exp_spec, exp_spec, exp_spec, P()), check_vma=False)
```

```python
import functools

import jax
import jax.numpy as jnp
from jax import lax
from jax.experimental import pallas as pl
from jax.experimental.pallas import tpu as pltpu
from jax.sharding import PartitionSpec as P

SLOTS = 64
EXTRA = 96
PAD = 16
F32 = jnp.float32
BF16 = jnp.bfloat16
VMEM_LIMIT = 67043328
MESH = pl.DeviceIdType.MESH


def nt_dot(a, b):
    return lax.dot_general(a, b, (((1,), (1,)), ((), ())), preferred_element_type=F32)


def tn_dot(a, b):
    return lax.dot_general(a, b, (((0,), (0,)), ((), ())), preferred_element_type=F32)


def nn_dot(a, b):
    return jnp.dot(a, b, preferred_element_type=F32)


def slot_mask(rank_row, rows, first):
    slot = lax.broadcasted_iota(jnp.int32, (rows, rank_row.shape[1]), 0) + first
    return slot.astype(F32) == rank_row


def hot_rows(rank):
    return jnp.max(rank, axis=1, keepdims=True) >= SLOTS


def extra_rank(rank):
    return jnp.max(jnp.where(hot_rows(rank), rank, -1.0), axis=0, keepdims=True)


def route_kernel(groups, per_group, x_ref, wr_ref, idx_ref, out_ref):
    rows, toks = groups * PAD, x_ref.shape[0]
    logits = nt_dot(wr_ref[...], x_ref[...])
    row = lax.broadcasted_iota(jnp.int32, (rows, toks), 0)
    expert = jnp.where(row % PAD < per_group, (row // PAD) * per_group + row % PAD, -1)
    chosen = expert == idx_ref[0:1, :]
    for k in range(1, idx_ref.shape[0]):
        chosen = chosen | (expert == idx_ref[k : k + 1, :])
    before = lax.broadcasted_iota(jnp.int32, (toks, toks), 0) < lax.broadcasted_iota(jnp.int32, (toks, toks), 1)
    rank = nn_dot(chosen.astype(F32).astype(BF16), before.astype(F32).astype(BF16))
    top = jnp.max(jnp.where(chosen, logits, -jnp.inf), axis=0, keepdims=True)
    weight = jnp.where(chosen, jnp.exp(logits - top), 0.0)
    prob = weight / jnp.sum(weight, axis=0, keepdims=True)
    out_ref[0] = jnp.where(chosen, rank, -1.0).reshape(groups, PAD, toks)
    out_ref[1] = prob.reshape(groups, PAD, toks)


def gather_rows(me, per_group, m_ref, x_ref, g_ref, x_out, d_out, g_out):
    step = per_group // 2

    def emit(masks, probs, where):
        pick = jnp.concatenate([m.astype(F32).astype(BF16) for m in masks], axis=0)
        gate = jnp.concatenate([jnp.sum(jnp.where(m, p, 0.0), axis=1, keepdims=True) for m, p in zip(masks, probs)], axis=0)
        x_out[where, :] = nn_dot(pick, x_ref[...]).astype(BF16)
        rows_g = nn_dot(pick, g_ref[...])
        if g_out is not None:
            g_out[where, :] = rows_g.astype(BF16)
        d_out[where, :] = (gate * rows_g).astype(BF16)

    def part(i, carry):
        ranks = [m_ref[0, me, pl.ds(i * step + k, 1), :] for k in range(step)]
        probs = [m_ref[1, me, pl.ds(i * step + k, 1), :] for k in range(step)]
        emit([slot_mask(r, SLOTS, 0) for r in ranks], probs, pl.ds(pl.multiple_of(i * (step * SLOTS), SLOTS), step * SLOTS))
        return carry

    lax.fori_loop(0, 2, part, 0)
    rank, prob = m_ref[0, me], m_ref[1, me]
    prob_hot = jnp.sum(jnp.where(hot_rows(rank), prob, 0.0), axis=0, keepdims=True)
    emit([slot_mask(extra_rank(rank), EXTRA, SLOTS)], [prob_hot], pl.ds(per_group * SLOTS, EXTRA))


class Stage:
    def __init__(self, main, bufs, sems, outs):
        self.main, self.bufs, self.sems, self.outs, self.busy, self.turn = main, bufs, sems, outs, {}, 0

    def gather(self, i, kinds, me, per_group, m_ref, x_ref, g_ref):
        slot, self.turn = self.turn, 1 - self.turn
        self.drain(slot)
        views = [self.bufs[k].at[slot] for k in range(kinds)]
        gather_rows(me, per_group, m_ref, x_ref, g_ref, *(views + [None])[:3])
        copies = []
        for k in range(kinds):
            copies.append(pltpu.make_async_copy(views[k].at[pl.ds(0, self.main)], self.outs[2 * k].at[i], self.sems.at[slot, 2 * k]))
            copies.append(pltpu.make_async_copy(views[k].at[pl.ds(self.main, EXTRA)], self.outs[2 * k + 1].at[i], self.sems.at[slot, 2 * k + 1]))
        for c in copies:
            c.start()
        self.busy[slot] = copies

    def drain(self, slot):
        for c in self.busy.pop(slot, ()):
            c.wait()


def device_of(bit):
    return (lax.axis_index("dp") ^ (bit >> 2), lax.axis_index("ep") ^ (bit & 3))


def greet(bits):
    barrier = pltpu.get_barrier_semaphore()
    for bit in bits:
        pl.semaphore_signal(barrier, inc=1, device_id=device_of(bit), device_id_type=MESH)
    pl.semaphore_wait(barrier, len(bits))


def near_kernel(per_group, x_ref, g_ref, m_ref, *refs):
    rows_out, (xs_out, ms_out, hot_out) = refs[:6], refs[6:9]
    x_in, g_in, m_in, st_x, st_d, st_g, send, recv, out_sem, st_sem = refs[9:]
    me = lax.axis_index("ep")
    greet((1, 2, 4))
    own = (x_ref, g_ref, m_ref)
    land = lambda s: own if s == 0 else (x_in.at[s - 1], g_in.at[s - 1], m_in.at[s - 1])
    flights = {}

    def push(k, source, s, bit):
        c = pltpu.make_async_remote_copy(src_ref=land(source)[k], dst_ref=land(s)[k], send_sem=send.at[s - 1, k], recv_sem=recv.at[s - 1, k], device_id=device_of(bit), device_id_type=MESH)
        c.start()
        flights[s, k] = c

    outs = []

    def keep(k, s):
        out = xs_out if k == 0 else ms_out
        c = pltpu.make_async_copy(land(s)[k], out.at[s - 1], out_sem.at[s - 1, k // 2])
        c.start()
        outs.append(c)

    def arrive(k, s, *onward):
        flights[s, k].wait_recv()
        for to, bit in onward:
            push(k, s, to, bit)
        if k != 1:
            keep(k, s)

    stage = Stage(per_group * SLOTS, (st_x, st_d, st_g), st_sem, rows_out)

    def gather(s):
        x, g, m = land(s)
        stage.gather(s, 3 if s < 4 else 2, me, per_group, m, x, g)
        hot = hot_rows(m[0, me]).astype(jnp.int32)
        shape = (hot.shape[0], hot_out.shape[1])
        diagonal = lax.broadcasted_iota(jnp.int32, shape, 0) == lax.broadcasted_iota(jnp.int32, shape, 1)
        hot_out[s : s + 1, :] = jnp.sum(jnp.where(diagonal, hot, 0), axis=0, keepdims=True)

    X, G, M = range(3)
    for k in (X, G, M):
        push(k, 0, 2, 2)
    for k in (G, X, M):
        push(k, 0, 4, 4)
    for k in (X, G, M):
        push(k, 0, 1, 1)
    gather(0)
    for k in (X, G, M):
        arrive(k, 1)
    gather(1)
    arrive(X, 2, (6, 4), (3, 1))
    arrive(G, 4, (6, 2), (5, 1))
    arrive(G, 2, (3, 1))
    arrive(M, 2, (6, 4), (3, 1))
    arrive(X, 4, (5, 1))
    arrive(M, 4, (5, 1))
    gather(2)
    gather(4)
    for s in (3, 5):
        for k in (X, G, M):
            arrive(k, s)
        gather(s)
    for k in (X, G, M):
        arrive(k, 6, (7, 1))
    gather(6)
    for k in (X, G, M):
        arrive(k, 7)
    gather(7)
    stage.drain(0)
    stage.drain(1)
    for c in flights.values():
        c.wait_send()
    for c in outs:
        c.wait()


def back_kernel(q_ref, gx_ref, me_ref, peer_ref, q_out, part_in, q_in, send, recv, q_send, q_recv, ld_sem):
    n_dev = q_in.shape[0]
    greet(tuple(range(1, n_dev)))

    def push(src, dst, i, bit, s_sem, r_sem):
        c = pltpu.make_async_remote_copy(src_ref=src, dst_ref=dst, send_sem=s_sem.at[i], recv_sem=r_sem.at[i], device_id=device_of(bit), device_id_type=MESH)
        c.start()
        return c

    parts = {h: push(gx_ref.at[2 * h + 1], part_in.at[h], h, 1, send, recv) for h in (1, 0)}
    qs = [push(q_ref, q_in.at[bit], bit, bit, q_send, q_recv) for bit in range(1, n_dev)]
    loads = [pltpu.make_async_copy(gx_ref.at[2 * h], dst, ld_sem.at[h]) for h, dst in enumerate((me_ref, peer_ref))]
    for c in loads:
        c.start()
    q_out[0] = q_ref[...]
    for i, c in enumerate(qs):
        c.wait_recv()
        q_out[i + 1] = q_in[i + 1]
    for h, dst in ((1, peer_ref), (0, me_ref)):
        loads[h].wait()
        parts[h].wait_recv()
        dst[...] += part_in[h]
    for c in qs + list(parts.values()):
        c.wait_send()


def expert_math(x, d, w1, w3, w2):
    z1 = nn_dot(x, w1)
    z3 = nn_dot(x, w3)
    sig = jax.nn.sigmoid(z1)
    silu = z1 * sig
    act = (silu * z3).astype(BF16)
    d_act = nt_dot(d, w2)
    dz1 = (d_act * z3 * sig * (1.0 + z1 * (1.0 - sig))).astype(BF16)
    dz3 = (d_act * silu).astype(BF16)
    return act, dz1, dz3


def flat(ref, first=0, count=None):
    v = ref[first : first + (count or ref.shape[0])]
    return v.reshape(v.shape[0] * v.shape[1], v.shape[2])


def pass1_kernel(per_group, hot_ref, ep_ref, w1_ref, w3_ref, w2_ref, x_ref, d_ref, g_ref, xo_ref, do_ref, go_ref, m0_ref, ms_ref, gx_ref, q_ref, act_ref, dz_ref, acto_ref, dzo_ref, r_scr):
    n_sh, n_all = g_ref.shape[0], x_ref.shape[0]
    e = pl.program_id(0)
    ff = w1_ref.shape[2]
    w1, w3, w2 = w1_ref[0], w3_ref[0], w2_ref[0]
    base = per_group * SLOTS
    m_of = lambda j: m0_ref.at[0, 0] if j == 0 else ms_ref.at[j - 1, 0, 0]

    def token_math(act, dz1, dz3, g):
        q = jnp.sum(nn_dot(act, w2) * g.astype(F32), axis=1, keepdims=True)
        return q, (nt_dot(dz1, w1) + nt_dot(dz3, w3)).astype(BF16)

    @pl.when(e == 0)
    def _():
        r_scr[:, base : base + EXTRA, :] = jnp.zeros((n_sh, EXTRA, r_scr.shape[2]), BF16)
        q_ref[...] = jnp.zeros_like(q_ref)
        acto_ref[...] = jnp.zeros_like(acto_ref)
        dzo_ref[...] = jnp.zeros_like(dzo_ref)

    act, dz1, dz3 = expert_math(flat(x_ref), flat(d_ref), w1, w3, w2)
    act_ref[0] = act
    dz_ref[0, :, :ff] = dz1
    dz_ref[0, :, ff:] = dz3
    near = n_sh * SLOTS
    q, r = token_math(act[:near], dz1[:near], dz3[:near], flat(g_ref))
    for j in range(n_sh):
        mask = slot_mask(m_of(j)[pl.ds(e, 1), :], SLOTS, 0)
        q_ref[j, pl.ds(e, 1), :] = jnp.sum(jnp.where(mask, q[j * SLOTS : (j + 1) * SLOTS], 0.0), axis=0, keepdims=True)
        r_scr[j, pl.ds(pl.multiple_of(e * SLOTS, SLOTS), SLOTS), :] = r[j * SLOTS : (j + 1) * SLOTS]

    for first in range(0, n_all, n_sh):
        is_hot = [hot_ref[first + j, e] for j in range(n_sh)]

        @pl.when(sum(is_hot) > 0)
        def _():
            act, dz1, dz3 = expert_math(flat(xo_ref, first, n_sh), flat(do_ref, first, n_sh), w1, w3, w2)
            if first == 0:
                q, r = token_math(act, dz1, dz3, flat(go_ref))
            for j in range(n_sh):
                rows = slice(j * EXTRA, (j + 1) * EXTRA)

                @pl.when(is_hot[j] > 0)
                def _():
                    acto_ref[first + j] = act[rows]
                    dzo_ref[first + j, :, :ff] = dz1[rows]
                    dzo_ref[first + j, :, ff:] = dz3[rows]
                    if first == 0:
                        mask = slot_mask(m_of(j)[pl.ds(e, 1), :], EXTRA, SLOTS)
                        q_ref[j, pl.ds(e, 1), :] += jnp.sum(jnp.where(mask, q[rows], 0.0), axis=0, keepdims=True)
                        r_scr[j, base : base + EXTRA, :] = r[rows]

    @pl.when(e == per_group - 1)
    def _():
        for j in range(n_sh):
            rank = m_of(j)[...]
            masks = [slot_mask(rank[i : i + 1, :], SLOTS, 0) for i in range(per_group)]
            masks.append(slot_mask(extra_rank(rank), EXTRA, SLOTS))
            pick = jnp.concatenate([m.astype(F32).astype(BF16) for m in masks], axis=0)
            gx_ref[j] = tn_dot(pick, r_scr[j])


def pass2_kernel(hot_ref, act_ref, dz_ref, x_ref, d_ref, xo_ref, do_ref, acto_ref, dzo_ref, g1_ref, g3_ref, g2_ref):
    n_all = x_ref.shape[0]
    e = pl.program_id(0)
    ff = g1_ref.shape[2]
    x = flat(x_ref)
    g1_ref[0] = tn_dot(x, dz_ref[0, :, :ff])
    g3_ref[0] = tn_dot(x, dz_ref[0, :, ff:])
    g2_ref[0] = tn_dot(act_ref[0], flat(d_ref))
    is_hot = [hot_ref[j, e] for j in range(n_all)]

    @pl.when(sum(is_hot) > 0)
    def _():
        keep = [h.astype(F32).astype(BF16) for h in is_hot]
        x = flat(xo_ref)
        dz = jnp.concatenate([dzo_ref[j] * keep[j] for j in range(n_all)], axis=0)
        d = jnp.concatenate([do_ref[j] * keep[j] for j in range(n_all)], axis=0)
        g1_ref[0] += tn_dot(x, dz[:, :ff])
        g3_ref[0] += tn_dot(x, dz[:, ff:])
        g2_ref[0] += tn_dot(flat(acto_ref), d)


def finish_kernel(groups, ep_ref, keep_ref, far_ref, wr_ref, x0_ref, xs_ref, m0_ref, ms_ref, q_ref, gx_ref, gr_ref):
    n_sh = q_ref.shape[0]
    x_refs = [x0_ref] + [xs_ref.at[i] for i in range(n_sh - 1)]
    m_refs = [m0_ref] + [ms_ref.at[i] for i in range(n_sh - 1)]
    ep = ep_ref[0]
    for s in range(n_sh):
        d, j = divmod(s, groups)
        q = jnp.concatenate([q_ref[d * groups + (ep ^ a), (ep ^ a) ^ j] for a in range(groups)], axis=0)
        p = m_refs[s][1].reshape(groups * PAD, q.shape[1])
        dl = p * (q - jnp.sum(p * q, axis=0, keepdims=True))
        dl = dl.astype(BF16)
        term = nn_dot(dl, x_refs[s][...])
        if s == 0:
            du = tn_dot(dl, wr_ref[...])
            gx_ref[...] = (keep_ref[...] + far_ref[...] + du).astype(BF16)
            gr_ref[...] = term
        else:
            gr_ref[...] += term


def solution(mesh):
    dp, ep = mesh.shape["dp"], mesh.shape["ep"]
    n_dev = dp * ep
    tok_spec = P(("dp", "ep"), None)
    exp_spec = P("ep", None, None)

    def swap(v, bit):
        return lax.ppermute(v, ("dp", "ep"), [(s, s ^ bit) for s in range(n_dev)])

    def device_step(x_loc, route_idx, w_router, w_gate, w_up, w_down, dy_loc):
        toks, dim = x_loc.shape
        n_exp = w_router.shape[1]
        n_loc, _, ff = w_gate.shape
        me = lax.axis_index("ep")
        ep_arr = me.reshape(1).astype(jnp.int32)
        vmem = pl.BlockSpec(memory_space=pltpu.VMEM)
        params = pltpu.CompilerParams(vmem_limit_bytes=VMEM_LIMIT)

        wr_rows = jnp.pad(w_router.T.reshape(ep, n_loc, dim), ((0, 0), (0, PAD - n_loc), (0, 0))).reshape(ep * PAD, dim)
        route = pl.pallas_call(
            functools.partial(route_kernel, ep, n_loc),
            out_shape=jax.ShapeDtypeStruct((2, ep, PAD, toks), F32),
            in_specs=[vmem] * 3,
            out_specs=vmem,
            compiler_params=params,
            cost_estimate=pl.CostEstimate(flops=10**9, bytes_accessed=10**6, transcendentals=0),
            name="route",
        )(x_loc, wr_rows, route_idx.T)

        hbm = pl.BlockSpec(memory_space=pl.ANY)
        main = n_loc * SLOTS
        sds = jax.ShapeDtypeStruct
        m_shape = route.shape
        others = n_dev - 1
        x_rows, x_more, d_rows, d_more, g_rows, g_more, xs, ms, hot = pl.pallas_call(
            functools.partial(near_kernel, n_loc),
            out_shape=[
                sds((n_dev, main, dim), BF16),
                sds((n_dev, EXTRA, dim), BF16),
                sds((n_dev, main, dim), BF16),
                sds((n_dev, EXTRA, dim), BF16),
                sds((ep, main, dim), BF16),
                sds((ep, EXTRA, dim), BF16),
                sds((others, toks, dim), BF16),
                sds((others,) + m_shape, F32),
                sds((n_dev, 128), jnp.int32),
            ],
            in_specs=[vmem] * 3,
            out_specs=[hbm] * 8 + [vmem],
            scratch_shapes=[
                pltpu.VMEM((others, toks, dim), BF16),
                pltpu.VMEM((others, toks, dim), BF16),
                pltpu.VMEM((others,) + m_shape, F32),
                pltpu.VMEM((2, main + EXTRA, dim), BF16),
                pltpu.VMEM((2, main + EXTRA, dim), BF16),
                pltpu.VMEM((2, main + EXTRA, dim), BF16),
                pltpu.SemaphoreType.DMA((others, 3)),
                pltpu.SemaphoreType.DMA((others, 3)),
                pltpu.SemaphoreType.DMA((others, 2)),
                pltpu.SemaphoreType.DMA((2, 6)),
            ],
            compiler_params=pltpu.CompilerParams(collective_id=0, has_side_effects=True, vmem_limit_bytes=VMEM_LIMIT),
            cost_estimate=pl.CostEstimate(flops=2 * 10**10, bytes_accessed=5 * 10**7, transcendentals=0),
            name="near",
        )(x_loc, dy_loc, route)

        w_specs = lambda im: [pl.BlockSpec((1, dim, ff), im), pl.BlockSpec((1, dim, ff), im), pl.BlockSpec((1, ff, dim), im)]
        im3 = lambda e, hot, ep_ref: (e, 0, 0)
        rows_at = lambda e, hot, ep_ref: (0, e, 0)
        fix = lambda shape: pl.BlockSpec(shape, lambda e, hot, ep_ref: (0,) * len(shape), pipeline_mode=pl.Buffered(1))
        n_row = n_dev * SLOTS
        gx_part, q_loc, act, dz, act_more, dz_more = pl.pallas_call(
            functools.partial(pass1_kernel, n_loc),
            out_shape=[
                sds((ep, toks, dim), F32),
                sds((ep, PAD, toks), F32),
                sds((n_loc, n_row, ff), BF16),
                sds((n_loc, n_row, 2 * ff), BF16),
                sds((n_dev, EXTRA, ff), BF16),
                sds((n_dev, EXTRA, 2 * ff), BF16),
            ],
            grid_spec=pltpu.PrefetchScalarGridSpec(
                num_scalar_prefetch=2,
                grid=(n_loc,),
                in_specs=w_specs(im3)
                + [pl.BlockSpec((n_dev, SLOTS, dim), rows_at)] * 2
                + [pl.BlockSpec((ep, SLOTS, dim), rows_at)]
                + [fix((n_dev, EXTRA, dim))] * 2
                + [fix((ep, EXTRA, dim))]
                + [pl.BlockSpec((1, 1, PAD, toks), lambda e, hot, ep_ref: (0, ep_ref[0], 0, 0))]
                + [pl.BlockSpec((ep - 1, 1, 1, PAD, toks), lambda e, hot, ep_ref: (0, 0, ep_ref[0], 0, 0))],
                out_specs=[fix((ep, toks, dim)), fix((ep, PAD, toks)), pl.BlockSpec((1, n_row, ff), im3), pl.BlockSpec((1, n_row, 2 * ff), im3)]
                + [fix((n_dev, EXTRA, ff)), fix((n_dev, EXTRA, 2 * ff))],
                scratch_shapes=[pltpu.VMEM((ep, main + EXTRA, dim), BF16)],
            ),
            compiler_params=params,
            cost_estimate=pl.CostEstimate(flops=4 * 10**10, bytes_accessed=10**8, transcendentals=0),
            name="pass1",
        )(hot, ep_arr, w_gate, w_up, w_down, x_rows, d_rows, g_rows, x_more, d_more, g_more, route, ms)

        for_me, for_peer, q_all = pl.pallas_call(
            back_kernel,
            out_shape=[sds((toks, dim), F32), sds((toks, dim), F32), sds((n_dev, ep, PAD, toks), F32)],
            in_specs=[vmem, hbm],
            out_specs=[vmem] * 3,
            scratch_shapes=[
                pltpu.VMEM((2, toks, dim), F32),
                pltpu.VMEM((n_dev, ep, PAD, toks), F32),
                pltpu.SemaphoreType.DMA((2,)),
                pltpu.SemaphoreType.DMA((2,)),
                pltpu.SemaphoreType.DMA((n_dev,)),
                pltpu.SemaphoreType.DMA((n_dev,)),
                pltpu.SemaphoreType.DMA((2,)),
            ],
            compiler_params=pltpu.CompilerParams(collective_id=1, has_side_effects=True, vmem_limit_bytes=VMEM_LIMIT),
            cost_estimate=pl.CostEstimate(flops=8 * 10**9, bytes_accessed=5 * 10**7, transcendentals=0),
            name="back",
        )(q_loc, gx_part)
        from_peer = swap(for_peer, 2)

        im3 = lambda e, hot: (e, 0, 0)
        rows_at = lambda e, hot: (0, e, 0)
        fix = lambda shape: pl.BlockSpec(shape, lambda e, hot: (0,) * len(shape), pipeline_mode=pl.Buffered(1))
        grad_gate, grad_up, grad_down = pl.pallas_call(
            pass2_kernel,
            out_shape=[sds((n_loc, dim, ff), F32), sds((n_loc, dim, ff), F32), sds((n_loc, ff, dim), F32)],
            grid_spec=pltpu.PrefetchScalarGridSpec(
                num_scalar_prefetch=1,
                grid=(n_loc,),
                in_specs=[pl.BlockSpec((1, n_row, ff), im3), pl.BlockSpec((1, n_row, 2 * ff), im3)]
                + [pl.BlockSpec((n_dev, SLOTS, dim), rows_at)] * 2
                + [fix((n_dev, EXTRA, dim))] * 2
                + [fix((n_dev, EXTRA, ff)), fix((n_dev, EXTRA, 2 * ff))],
                out_specs=w_specs(im3),
            ),
            compiler_params=params,
            cost_estimate=pl.CostEstimate(flops=6 * 10**10, bytes_accessed=2 * 10**8, transcendentals=0),
            name="pass2",
        )(hot, act, dz, x_rows, d_rows, x_more, d_more, act_more, dz_more)

        fixed = lambda shape: pl.BlockSpec(shape, lambda i, ep_ref: (0,) * len(shape))
        grad_x, grad_rt = pl.pallas_call(
            functools.partial(finish_kernel, ep),
            out_shape=[jax.ShapeDtypeStruct((toks, dim), BF16), jax.ShapeDtypeStruct((ep * PAD, dim), F32)],
            grid_spec=pltpu.PrefetchScalarGridSpec(
                num_scalar_prefetch=1,
                grid=(1,),
                in_specs=[fixed((toks, dim)), fixed((toks, dim)), fixed((ep * PAD, dim))]
                + [fixed(v.shape) for v in (x_loc, xs, route, ms, q_all)],
                out_specs=[fixed((toks, dim)), fixed((ep * PAD, dim))],
            ),
            compiler_params=params,
            cost_estimate=pl.CostEstimate(flops=4 * 10**9, bytes_accessed=10**7, transcendentals=0),
            name="finish",
        )(ep_arr, for_me, from_peer, wr_rows, x_loc, xs, route, ms, q_all)
        grad_router = grad_rt.reshape(ep, PAD, dim)[:, :n_loc].reshape(n_exp, dim).T
        return grad_x, grad_gate, grad_up, grad_down, grad_router

    return jax.shard_map(device_step, mesh=mesh, in_specs=(tok_spec, tok_spec, P(), exp_spec, exp_spec, exp_spec, tok_spec), out_specs=(tok_spec, exp_spec, exp_spec, exp_spec, P()), check_vma=False)
```

```python
import functools

import jax
import jax.numpy as jnp
from jax import lax
from jax.experimental import pallas as pl
from jax.experimental.pallas import tpu as pltpu
from jax.sharding import PartitionSpec as P

SLOTS = 56
EXTRA = 104
SPAN = 64
TAIL = 112
PAD = 16
F32 = jnp.float32
BF16 = jnp.bfloat16
VMEM_LIMIT = 67043328
MESH = pl.DeviceIdType.MESH


def nt_dot(a, b):
    return lax.dot_general(a, b, (((1,), (1,)), ((), ())), preferred_element_type=F32)


def tn_dot(a, b):
    return lax.dot_general(a, b, (((0,), (0,)), ((), ())), preferred_element_type=F32)


def nn_dot(a, b):
    return jnp.dot(a, b, preferred_element_type=F32)


def slot_mask(rank_row, rows, first):
    slot = lax.broadcasted_iota(jnp.int32, (rows, rank_row.shape[1]), 0) + first
    return slot.astype(F32) == rank_row


def hot_rows(rank):
    return jnp.max(rank, axis=1, keepdims=True) >= SLOTS


def extra_rank(rank):
    return jnp.max(jnp.where(hot_rows(rank), rank, -1.0), axis=0, keepdims=True)


def route(per_group, x_ref, idx_ref, wr_ref, out_ref):
    groups, toks = out_ref.shape[1], x_ref.shape[0]
    logits = nn_dot(x_ref[...], wr_ref[...]).T
    expert = lax.broadcasted_iota(jnp.int32, logits.shape, 0)
    chosen = expert == idx_ref[0:1, :]
    for k in range(1, idx_ref.shape[0]):
        chosen = chosen | (expert == idx_ref[k : k + 1, :])
    before = lax.broadcasted_iota(jnp.int32, (toks, toks), 0) < lax.broadcasted_iota(jnp.int32, (toks, toks), 1)
    rank = nn_dot(chosen.astype(F32).astype(BF16), before.astype(F32).astype(BF16))
    top = jnp.max(jnp.where(chosen, logits, -jnp.inf), axis=0, keepdims=True)
    weight = jnp.where(chosen, jnp.exp(logits - top), 0.0)
    prob = weight / jnp.sum(weight, axis=0, keepdims=True)
    rank = jnp.where(chosen, rank, -1.0)
    for a in range(groups):
        rows = slice(a * per_group, (a + 1) * per_group)
        out_ref[0, a, :per_group, :] = rank[rows]
        out_ref[0, a, per_group:, :] = jnp.full((PAD - per_group, toks), -1.0, F32)
        out_ref[1, a, :per_group, :] = prob[rows]
        out_ref[1, a, per_group:, :] = jnp.zeros((PAD - per_group, toks), F32)


def gather_rows(me, per_group, m_refs, x_refs, g_refs, x_out, d_out, g_out):
    step = per_group // 2

    def emit(masks, probs, size, first):
        def put(out, pair):
            for k in range(len(masks[0])):
                rows = jnp.concatenate([v[k * size : (k + 1) * size] for v in pair], axis=0)
                start = first + k * (2 * size)
                out[pl.ds(start if isinstance(start, int) else pl.multiple_of(start, 16), 2 * size), :] = rows.astype(BF16)

        picks = [jnp.concatenate([m.astype(F32) for m in ms], axis=0).astype(BF16) for ms in masks]
        put(x_out, [nn_dot(pick, x[...]) for pick, x in zip(picks, x_refs)])
        rows_g = [nn_dot(pick, g[...]) for pick, g in zip(picks, g_refs)]
        if g_out is not None:
            put(g_out, rows_g)
        gates = [jnp.concatenate([jnp.sum(jnp.where(m, p, 0.0), axis=1, keepdims=True) for m, p in zip(*mp)], axis=0) for mp in zip(masks, probs)]
        put(d_out, [gate * v for gate, v in zip(gates, rows_g)])

    def part(i, carry):
        masks = [[slot_mask(m[0, me, pl.ds(i * step + k, 1), :], SLOTS, 0) for k in range(step)] for m in m_refs]
        probs = [[m[1, me, pl.ds(i * step + k, 1), :] for k in range(step)] for m in m_refs]
        emit(masks, probs, SLOTS, i * (step * 2 * SLOTS))
        return carry

    lax.fori_loop(0, 2, part, 0)
    masks, probs = [], []
    for m in m_refs:
        rank, prob = m[0, me], m[1, me]
        masks.append([slot_mask(extra_rank(rank), EXTRA, SLOTS)])
        probs.append([jnp.sum(jnp.where(hot_rows(rank), prob, 0.0), axis=0, keepdims=True)])
    emit(masks, probs, EXTRA, per_group * 2 * SLOTS)


class Stage:
    def __init__(self, main, bufs, sems, outs):
        self.main, self.bufs, self.sems, self.outs, self.busy, self.turn = main, bufs, sems, outs, {}, 0

    def gather(self, i, kinds, *args):
        slot, self.turn = self.turn, 1 - self.turn
        self.drain(slot)
        views = [self.bufs[k].at[slot] for k in range(kinds)]
        gather_rows(*args, *(views + [None])[:3])
        copies = []
        for k in range(kinds):
            copies.append(pltpu.make_async_copy(views[k].at[pl.ds(0, self.main)], self.outs[2 * k].at[i], self.sems.at[slot, 2 * k]))
            copies.append(pltpu.make_async_copy(views[k].at[pl.ds(self.main, 2 * EXTRA)], self.outs[2 * k + 1].at[i], self.sems.at[slot, 2 * k + 1]))
        for c in copies:
            c.start()
        self.busy[slot] = copies

    def drain(self, slot):
        for c in self.busy.pop(slot, ()):
            c.wait()


def device_of(bit):
    return (lax.axis_index("dp") ^ (bit >> 2), lax.axis_index("ep") ^ (bit & 3))


def greet(bits):
    barrier = pltpu.get_barrier_semaphore()
    for bit in bits:
        pl.semaphore_signal(barrier, inc=1, device_id=device_of(bit), device_id_type=MESH)
    pl.semaphore_wait(barrier, len(bits))


def near_kernel(per_group, x_ref, g_ref, idx_ref, wr_ref, *refs):
    rows_out, (xs_out, ms_out, hot_out) = refs[:6], refs[6:9]
    x_in, g_in, i_in, st_x, st_d, st_g, send, recv, out_sem, st_sem = refs[9:]
    me = lax.axis_index("ep")
    greet((1, 2, 4))
    own = (x_ref, g_ref, idx_ref)
    land = lambda s: own if s == 0 else (x_in.at[s - 1], g_in.at[s - 1], i_in.at[s - 1])
    flights = {}

    def push(k, source, s, bit):
        c = pltpu.make_async_remote_copy(src_ref=land(source)[k], dst_ref=land(s)[k], send_sem=send.at[s - 1, k], recv_sem=recv.at[s - 1, k], device_id=device_of(bit), device_id_type=MESH)
        c.start()
        flights[s, k] = c

    outs = []

    def arrive(k, s, *onward):
        flights[s, k].wait_recv()
        for to, bit in onward:
            push(k, s, to, bit)
        if k == 0:
            c = pltpu.make_async_copy(land(s)[k], xs_out.at[s - 1], out_sem.at[s - 1])
            c.start()
            outs.append(c)

    stage = Stage(per_group * 2 * SLOTS, (st_x, st_d, st_g), st_sem, rows_out)

    def routing(s):
        x, _, idx = land(s)
        route(per_group, x, idx, wr_ref, ms_out.at[s])
        hot = hot_rows(ms_out[s, 0, me]).astype(jnp.int32)
        shape = (hot.shape[0], hot_out.shape[1])
        diagonal = lax.broadcasted_iota(jnp.int32, shape, 0) == lax.broadcasted_iota(jnp.int32, shape, 1)
        hot_out[s : s + 1, :] = jnp.sum(jnp.where(diagonal, hot, 0), axis=0, keepdims=True)

    def gather(s):
        pair = (s, s + 1)
        stage.gather(s // 2, 3 if s < 4 else 2, me, per_group, [ms_out.at[i] for i in pair], [land(i)[0] for i in pair], [land(i)[1] for i in pair])

    X, G, I = range(3)
    for k in (X, I, G):
        push(k, 0, 2, 2)
    for k in (G, I, X):
        push(k, 0, 4, 4)
    for k in (X, I, G):
        push(k, 0, 1, 1)
    routing(0)
    for k in (X, G, I):
        arrive(k, 1)
    routing(1)
    gather(0)
    arrive(X, 2, (6, 4), (3, 1))
    arrive(I, 2, (6, 4), (3, 1))
    arrive(G, 4, (6, 2), (5, 1))
    arrive(I, 4, (5, 1))
    routing(2)
    arrive(X, 3)
    arrive(I, 3)
    routing(3)
    arrive(G, 2, (3, 1))
    arrive(X, 4, (5, 1))
    routing(4)
    arrive(G, 3)
    gather(2)
    for k in (X, G, I):
        arrive(k, 5)
    routing(5)
    gather(4)
    for k in (X, I, G):
        arrive(k, 6, (7, 1))
    routing(6)
    for k in (X, I, G):
        arrive(k, 7)
    routing(7)
    gather(6)
    stage.drain(0)
    stage.drain(1)
    for c in flights.values():
        c.wait_send()
    for c in outs:
        c.wait()


def back_kernel(q_ref, keep_ref, give_ref, peer_ref, q_out, part_in, q_in, send, recv, q_send, q_recv, ld_sem):
    n_dev = q_in.shape[0]
    greet(tuple(range(1, n_dev)))

    def push(src, dst, bit, s_sem, r_sem):
        c = pltpu.make_async_remote_copy(src_ref=src, dst_ref=dst, send_sem=s_sem, recv_sem=r_sem, device_id=device_of(bit), device_id_type=MESH)
        c.start()
        return c

    part = push(give_ref, part_in, 1, send.at[0], recv.at[0])
    load = pltpu.make_async_copy(keep_ref, peer_ref, ld_sem.at[0])
    load.start()
    qs = [push(q_ref, q_in.at[bit], bit, q_send.at[bit], q_recv.at[bit]) for bit in range(1, n_dev)]
    q_out[0] = q_ref[...]
    load.wait()
    part.wait_recv()
    peer_ref[...] += part_in[...]
    for i, c in enumerate(qs):
        c.wait_recv()
        q_out[i + 1] = q_in[i + 1]
    for c in qs + [part]:
        c.wait_send()


def expert_math(x, d, w1, w3, w2):
    z1 = nn_dot(x, w1)
    z3 = nn_dot(x, w3)
    sig = jax.nn.sigmoid(z1)
    silu = z1 * sig
    act = (silu * z3).astype(BF16)
    d_act = nt_dot(d, w2)
    dz1 = (d_act * z3 * sig * (1.0 + z1 * (1.0 - sig))).astype(BF16)
    dz3 = (d_act * silu).astype(BF16)
    return act, dz1, dz3


def flat(ref, first=0, count=None):
    v = ref[first : first + (count or ref.shape[0])]
    return v.reshape(v.shape[0] * v.shape[1], v.shape[2])


def hot_column(is_hot):
    return jnp.concatenate([jnp.full((EXTRA, 1), 1.0, F32) * h.astype(F32) for h in is_hot], axis=0) > 0.0


def masked(column, v):
    return jnp.where(column, v.astype(F32), 0.0).astype(BF16)


def pass1_kernel(per_group, hot_ref, ep_ref, w1_ref, w3_ref, w2_ref, x_ref, d_ref, g_ref, xo_ref, do_ref, go_ref, ms_ref, *refs):
    n_pair = g_ref.shape[0]
    n_sh, n_all = 2 * n_pair, hot_ref.shape[0]
    gx_refs, (q_ref, act_ref, dz_ref, acto_ref, dzo_ref, r_scr) = refs[:n_sh], refs[n_sh:]
    e = pl.program_id(0)
    ff = w1_ref.shape[2]
    w1, w3, w2 = w1_ref[0], w3_ref[0], w2_ref[0]
    base = per_group * SPAN
    m_of = lambda j: ms_ref.at[j, 0, 0]

    def token_math(act, dz1, dz3, g):
        q = jnp.sum(nn_dot(act, w2) * g.astype(F32), axis=1, keepdims=True)
        return q, nt_dot(dz1, w1) + nt_dot(dz3, w3)

    @pl.when(e == 0)
    def _():
        r_scr[:, base:, :] = jnp.zeros((n_sh, TAIL, r_scr.shape[2]), BF16)
        for i in range(per_group):
            r_scr[:, i * SPAN + SPAN - 16 : (i + 1) * SPAN, :] = jnp.zeros((n_sh, 16, r_scr.shape[2]), BF16)
        acto_ref[...] = jnp.zeros_like(acto_ref)
        dzo_ref[...] = jnp.zeros_like(dzo_ref)

    act, dz1, dz3 = expert_math(flat(x_ref), flat(d_ref), w1, w3, w2)
    act_ref[0] = act
    dz_ref[0, :, :ff] = dz1
    dz_ref[0, :, ff:] = dz3
    near = n_sh * SLOTS
    q, r = token_math(act[:near], dz1[:near], dz3[:near], flat(g_ref))
    for j in range(n_sh):
        rows = slice(j * SLOTS, (j + 1) * SLOTS)
        mask = slot_mask(m_of(j)[pl.ds(e, 1), :], SLOTS, 0)
        q_ref[pl.ds(j * per_group + e, 1), :] = jnp.sum(jnp.where(mask, q[rows], 0.0), axis=0, keepdims=True)
        r_scr[j, pl.ds(pl.multiple_of(e * SPAN, SPAN), SLOTS), :] = r[rows].astype(BF16)

    for first in range(0, n_all, n_sh):
        is_hot = [hot_ref[first + j, e] for j in range(n_sh)]

        @pl.when(sum(is_hot) > 0)
        def _():
            part = first // 2
            column = hot_column(is_hot)
            d = masked(column, flat(do_ref, part, n_pair))
            act, dz1, dz3 = expert_math(flat(xo_ref, part, n_pair), d, w1, w3, w2)
            shape = (n_pair, 2 * EXTRA, ff)
            acto_ref[part : part + n_pair] += masked(column, act).reshape(shape)
            dzo_ref[part : part + n_pair, :, :ff] += dz1.reshape(shape)
            dzo_ref[part : part + n_pair, :, ff:] += dz3.reshape(shape)
            if first == 0:
                q, r = token_math(act, dz1, dz3, flat(go_ref))
                for j in range(n_sh):
                    rows = slice(j * EXTRA, (j + 1) * EXTRA)

                    @pl.when(is_hot[j] > 0)
                    def _():
                        mask = slot_mask(m_of(j)[pl.ds(e, 1), :], EXTRA, SLOTS)
                        q_ref[pl.ds(j * per_group + e, 1), :] += jnp.sum(jnp.where(mask, q[rows], 0.0), axis=0, keepdims=True)
                        r_scr[j, base : base + EXTRA, :] = r[rows].astype(BF16)

    @pl.when(e == per_group - 1)
    def _():
        for j in range(n_sh):
            rank = m_of(j)[...]
            low = jnp.where(rank < SLOTS, rank, -1.0)
            masks = [slot_mask(low[i : i + 1, :], SPAN, 0) for i in range(per_group)]
            masks.append(slot_mask(extra_rank(rank), TAIL, SLOTS))
            pick = jnp.concatenate([m.astype(F32) for m in masks], axis=0).astype(BF16)
            gx_refs[j][...] = tn_dot(pick, r_scr[j])


def pass2_kernel(hot_ref, act_ref, dz_ref, x_ref, d_ref, xo_ref, do_ref, acto_ref, dzo_ref, g1_ref, g3_ref, g2_ref):
    e = pl.program_id(0)
    ff = g1_ref.shape[2]
    x = flat(x_ref)
    g1_ref[0] = tn_dot(x, dz_ref[0, :, :ff])
    g3_ref[0] = tn_dot(x, dz_ref[0, :, ff:])
    g2_ref[0] = tn_dot(act_ref[0], flat(d_ref))
    is_hot = [hot_ref[j, e] for j in range(hot_ref.shape[0])]

    @pl.when(sum(is_hot) > 0)
    def _():
        column = hot_column(is_hot)
        x = flat(xo_ref)
        dz = masked(column, flat(dzo_ref))
        g1_ref[0] += tn_dot(x, dz[:, :ff])
        g3_ref[0] += tn_dot(x, dz[:, ff:])
        g2_ref[0] += tn_dot(flat(acto_ref), masked(column, flat(do_ref)))


def finish_kernel(per_group, ep_ref, own_ref, near_ref, far_ref, wr_ref, x0_ref, xs_ref, ms_ref, q_ref, gx_ref, gr_ref, acc):
    n_sh, groups = q_ref.shape[0], wr_ref.shape[0]
    ep = ep_ref[0]
    for s in range(n_sh):
        d, j = divmod(s, groups)
        rows = lambda m: slice((m ^ j) * per_group, ((m ^ j) + 1) * per_group)
        q = [q_ref[d * groups + m, rows(m), :] for m in range(groups)]
        p = [ms_ref[s, 0, ep ^ m][:per_group] for m in range(groups)]
        mean = sum(jnp.sum(a * b, axis=0, keepdims=True) for a, b in zip(p, q))
        gap = jnp.zeros((PAD - per_group, q[0].shape[1]), F32)
        dl = jnp.concatenate([v for a, b in zip(p, q) for v in (a * (b - mean), gap)], axis=0).astype(BF16)
        term = nn_dot(dl, x0_ref[...] if s == 0 else xs_ref[s - 1])
        if s == 0:
            wr = jnp.concatenate([wr_ref[ep ^ m] for m in range(groups)], axis=0)
            gx_ref[...] = (own_ref[...] + near_ref[...] + far_ref[...] + tn_dot(dl, wr)).astype(BF16)
            acc[...] = term
        else:
            acc[...] += term
    for m in range(groups):
        gr_ref[ep ^ m] = acc[m * PAD : (m + 1) * PAD, :]


def solution(mesh):
    dp, ep = mesh.shape["dp"], mesh.shape["ep"]
    n_dev = dp * ep
    tok_spec = P(("dp", "ep"), None)
    exp_spec = P("ep", None, None)

    def swap(v, bit):
        return lax.ppermute(v, ("dp", "ep"), [(s, s ^ bit) for s in range(n_dev)])

    def device_step(x_loc, route_idx, w_router, w_gate, w_up, w_down, dy_loc):
        toks, dim = x_loc.shape
        top_k = route_idx.shape[1]
        n_exp = w_router.shape[1]
        n_loc, _, ff = w_gate.shape
        me = lax.axis_index("ep")
        ep_arr = me.reshape(1).astype(jnp.int32)
        vmem = pl.BlockSpec(memory_space=pltpu.VMEM)
        params = pltpu.CompilerParams(vmem_limit_bytes=VMEM_LIMIT)

        wr_rows = jnp.pad(w_router.T.reshape(ep, n_loc, dim), ((0, 0), (0, PAD - n_loc), (0, 0)))
        m_shape = (2, ep, PAD, toks)
        hbm = pl.BlockSpec(memory_space=pl.ANY)
        main = n_loc * 2 * SLOTS
        pairs = n_dev // 2
        sds = jax.ShapeDtypeStruct
        others = n_dev - 1
        x_rows, x_more, d_rows, d_more, g_rows, g_more, xs, ms, hot = pl.pallas_call(
            functools.partial(near_kernel, n_loc),
            out_shape=[
                sds((pairs, main, dim), BF16),
                sds((pairs, 2 * EXTRA, dim), BF16),
                sds((pairs, main, dim), BF16),
                sds((pairs, 2 * EXTRA, dim), BF16),
                sds((ep // 2, main, dim), BF16),
                sds((ep // 2, 2 * EXTRA, dim), BF16),
                sds((others, toks, dim), BF16),
                sds((n_dev,) + m_shape, F32),
                sds((n_dev, 128), jnp.int32),
            ],
            in_specs=[vmem] * 4,
            out_specs=[hbm] * 7 + [vmem] * 2,
            scratch_shapes=[
                pltpu.VMEM((others, toks, dim), BF16),
                pltpu.VMEM((others, toks, dim), BF16),
                pltpu.VMEM((others, top_k, toks), jnp.int32),
                pltpu.VMEM((2, main + 2 * EXTRA, dim), BF16),
                pltpu.VMEM((2, main + 2 * EXTRA, dim), BF16),
                pltpu.VMEM((2, main + 2 * EXTRA, dim), BF16),
                pltpu.SemaphoreType.DMA((others, 3)),
                pltpu.SemaphoreType.DMA((others, 3)),
                pltpu.SemaphoreType.DMA((others,)),
                pltpu.SemaphoreType.DMA((2, 6)),
            ],
            compiler_params=pltpu.CompilerParams(collective_id=0, has_side_effects=True, vmem_limit_bytes=VMEM_LIMIT),
            cost_estimate=pl.CostEstimate(flops=2 * 10**10, bytes_accessed=5 * 10**7, transcendentals=0),
            name="near",
        )(x_loc, dy_loc, route_idx.T, w_router)

        w_specs = lambda im: [pl.BlockSpec((1, dim, ff), im), pl.BlockSpec((1, dim, ff), im), pl.BlockSpec((1, ff, dim), im)]
        im3 = lambda e, hot, ep_ref: (e, 0, 0)
        rows_at = lambda e, hot, ep_ref: (0, e, 0)
        fix = lambda shape: pl.BlockSpec(shape, lambda e, hot, ep_ref: (0,) * len(shape), pipeline_mode=pl.Buffered(1))
        n_row = n_dev * SLOTS
        *gx_part, q_loc, act, dz, act_more, dz_more = pl.pallas_call(
            functools.partial(pass1_kernel, n_loc),
            out_shape=[sds((toks, dim), F32)] * ep
            + [
                sds((ep * n_loc, toks), F32),
                sds((n_loc, n_row, ff), BF16),
                sds((n_loc, n_row, 2 * ff), BF16),
                sds((pairs, 2 * EXTRA, ff), BF16),
                sds((pairs, 2 * EXTRA, 2 * ff), BF16),
            ],
            grid_spec=pltpu.PrefetchScalarGridSpec(
                num_scalar_prefetch=2,
                grid=(n_loc,),
                in_specs=w_specs(im3)
                + [pl.BlockSpec((pairs, 2 * SLOTS, dim), rows_at)] * 2
                + [pl.BlockSpec((ep // 2, 2 * SLOTS, dim), rows_at)]
                + [fix((pairs, 2 * EXTRA, dim))] * 2
                + [fix((ep // 2, 2 * EXTRA, dim))]
                + [pl.BlockSpec((ep, 1, 1, PAD, toks), lambda e, hot, ep_ref: (0, 0, ep_ref[0], 0, 0))],
                out_specs=[fix((toks, dim))] * ep
                + [fix((ep * n_loc, toks)), pl.BlockSpec((1, n_row, ff), im3), pl.BlockSpec((1, n_row, 2 * ff), im3)]
                + [fix((pairs, 2 * EXTRA, ff)), fix((pairs, 2 * EXTRA, 2 * ff))],
                scratch_shapes=[pltpu.VMEM((ep, n_loc * SPAN + TAIL, dim), BF16)],
            ),
            compiler_params=params,
            cost_estimate=pl.CostEstimate(flops=4 * 10**10, bytes_accessed=10**8, transcendentals=0),
            name="pass1",
        )(hot, ep_arr, w_gate, w_up, w_down, x_rows, d_rows, g_rows, x_more, d_more, g_more, ms)

        from_core = swap(gx_part[1], 1)
        for_peer, q_all = pl.pallas_call(
            back_kernel,
            out_shape=[sds((toks, dim), F32), sds((n_dev, ep * n_loc, toks), F32)],
            in_specs=[vmem, hbm, hbm],
            out_specs=[vmem] * 2,
            scratch_shapes=[
                pltpu.VMEM((toks, dim), F32),
                pltpu.VMEM((n_dev, ep * n_loc, toks), F32),
                pltpu.SemaphoreType.DMA((1,)),
                pltpu.SemaphoreType.DMA((1,)),
                pltpu.SemaphoreType.DMA((n_dev,)),
                pltpu.SemaphoreType.DMA((n_dev,)),
                pltpu.SemaphoreType.DMA((1,)),
            ],
            compiler_params=pltpu.CompilerParams(collective_id=1, has_side_effects=True, vmem_limit_bytes=VMEM_LIMIT),
            cost_estimate=pl.CostEstimate(flops=8 * 10**9, bytes_accessed=5 * 10**7, transcendentals=0),
            name="back",
        )(q_loc, gx_part[2], gx_part[3])
        from_peer = swap(for_peer, 2)

        im3 = lambda e, hot: (e, 0, 0)
        rows_at = lambda e, hot: (0, e, 0)
        fix = lambda shape: pl.BlockSpec(shape, lambda e, hot: (0,) * len(shape), pipeline_mode=pl.Buffered(1))
        grad_gate, grad_up, grad_down = pl.pallas_call(
            pass2_kernel,
            out_shape=[sds((n_loc, dim, ff), F32), sds((n_loc, dim, ff), F32), sds((n_loc, ff, dim), F32)],
            grid_spec=pltpu.PrefetchScalarGridSpec(
                num_scalar_prefetch=1,
                grid=(n_loc,),
                in_specs=[pl.BlockSpec((1, n_row, ff), im3), pl.BlockSpec((1, n_row, 2 * ff), im3)]
                + [pl.BlockSpec((pairs, 2 * SLOTS, dim), rows_at)] * 2
                + [fix((pairs, 2 * EXTRA, dim))] * 2
                + [fix((pairs, 2 * EXTRA, ff)), fix((pairs, 2 * EXTRA, 2 * ff))],
                out_specs=w_specs(im3),
            ),
            compiler_params=params,
            cost_estimate=pl.CostEstimate(flops=6 * 10**10, bytes_accessed=2 * 10**8, transcendentals=0),
            name="pass2",
        )(hot, act, dz, x_rows, d_rows, x_more, d_more, act_more, dz_more)

        fixed = lambda shape: pl.BlockSpec(shape, lambda i, ep_ref: (0,) * len(shape))
        grad_x, grad_rt = pl.pallas_call(
            functools.partial(finish_kernel, n_loc),
            out_shape=[sds((toks, dim), BF16), sds((ep, PAD, dim), F32)],
            grid_spec=pltpu.PrefetchScalarGridSpec(
                num_scalar_prefetch=1,
                grid=(1,),
                in_specs=[fixed(v.shape) for v in (gx_part[0], from_core, from_peer, wr_rows, x_loc, xs)]
                + [pl.BlockSpec((n_dev, 1, ep, PAD, toks), lambda i, ep_ref: (0, 1, 0, 0, 0)), fixed(q_all.shape)],
                out_specs=[fixed((toks, dim)), fixed((ep, PAD, dim))],
                scratch_shapes=[pltpu.VMEM((ep * PAD, dim), F32)],
            ),
            compiler_params=params,
            cost_estimate=pl.CostEstimate(flops=4 * 10**9, bytes_accessed=10**7, transcendentals=0),
            name="finish",
        )(ep_arr, gx_part[0], from_core, from_peer, wr_rows, x_loc, xs, ms, q_all)
        grad_router = grad_rt[:, :n_loc].reshape(n_exp, dim).T
        return grad_x, grad_gate, grad_up, grad_down, grad_router

    return jax.shard_map(device_step, mesh=mesh, in_specs=(tok_spec, tok_spec, P(), exp_spec, exp_spec, exp_spec, tok_spec), out_specs=(tok_spec, exp_spec, exp_spec, exp_spec, P()), check_vma=False)
```

```python
import functools

import jax
import jax.numpy as jnp
from jax import lax
from jax.experimental import pallas as pl
from jax.experimental.pallas import tpu as pltpu
from jax.sharding import PartitionSpec as P

SLOTS = 56
EXTRA = 104
SPAN = 64
TAIL = 112
PAD = 16
F32 = jnp.float32
BF16 = jnp.bfloat16
VMEM_LIMIT = 67043328
MESH = pl.DeviceIdType.MESH


def nt_dot(a, b):
    return lax.dot_general(a, b, (((1,), (1,)), ((), ())), preferred_element_type=F32)


def tn_dot(a, b):
    return lax.dot_general(a, b, (((0,), (0,)), ((), ())), preferred_element_type=F32)


def nn_dot(a, b):
    return jnp.dot(a, b, preferred_element_type=F32)


def slot_mask(rank_row, rows, first):
    slot = lax.broadcasted_iota(jnp.int32, (rows, rank_row.shape[1]), 0) + first
    return slot.astype(F32) == rank_row


def hot_rows(rank):
    return jnp.max(rank, axis=1, keepdims=True) >= SLOTS


def extra_rank(rank):
    return jnp.max(jnp.where(hot_rows(rank), rank, -1.0), axis=0, keepdims=True)


def route(per_group, x_ref, idx_ref, wr_ref, out_ref):
    groups, toks = out_ref.shape[1], x_ref.shape[0]
    logits = nt_dot(wr_ref[...], x_ref[...])
    expert = lax.broadcasted_iota(jnp.int32, logits.shape, 0)
    chosen = expert == idx_ref[0:1, :]
    for k in range(1, idx_ref.shape[0]):
        chosen = chosen | (expert == idx_ref[k : k + 1, :])
    before = lax.broadcasted_iota(jnp.int32, (toks, toks), 0) < lax.broadcasted_iota(jnp.int32, (toks, toks), 1)
    rank = nn_dot(chosen.astype(F32).astype(BF16), before.astype(F32).astype(BF16))
    top = jnp.max(jnp.where(chosen, logits, -jnp.inf), axis=0, keepdims=True)
    weight = jnp.where(chosen, jnp.exp(logits - top), 0.0)
    prob = weight / jnp.sum(weight, axis=0, keepdims=True)
    rank = jnp.where(chosen, rank, -1.0)
    for a in range(groups):
        rows = slice(a * per_group, (a + 1) * per_group)
        out_ref[0, a, :per_group, :] = rank[rows]
        out_ref[0, a, per_group:, :] = jnp.full((PAD - per_group, toks), -1.0, F32)
        out_ref[1, a, :per_group, :] = prob[rows]
        out_ref[1, a, per_group:, :] = jnp.zeros((PAD - per_group, toks), F32)


def gather_rows(me, per_group, m_refs, x_refs, g_refs, x_out, d_out, g_out):
    step = per_group // 2

    def emit(masks, probs, size, first):
        def put(out, pair):
            for k in range(len(masks[0])):
                rows = jnp.concatenate([v[k * size : (k + 1) * size] for v in pair], axis=0)
                start = first + k * (2 * size)
                out[pl.ds(start if isinstance(start, int) else pl.multiple_of(start, 16), 2 * size), :] = rows.astype(BF16)

        picks = [jnp.concatenate([m.astype(F32) for m in ms], axis=0).astype(BF16) for ms in masks]
        put(x_out, [nn_dot(pick, x[...]) for pick, x in zip(picks, x_refs)])
        rows_g = [nn_dot(pick, g[...]) for pick, g in zip(picks, g_refs)]
        if g_out is not None:
            put(g_out, rows_g)
        gates = [jnp.concatenate([jnp.sum(jnp.where(m, p, 0.0), axis=1, keepdims=True) for m, p in zip(*mp)], axis=0) for mp in zip(masks, probs)]
        put(d_out, [gate * v for gate, v in zip(gates, rows_g)])

    def part(i, carry):
        masks = [[slot_mask(m[0, me, pl.ds(i * step + k, 1), :], SLOTS, 0) for k in range(step)] for m in m_refs]
        probs = [[m[1, me, pl.ds(i * step + k, 1), :] for k in range(step)] for m in m_refs]
        emit(masks, probs, SLOTS, i * (step * 2 * SLOTS))
        return carry

    lax.fori_loop(0, 2, part, 0)
    masks, probs = [], []
    for m in m_refs:
        rank, prob = m[0, me], m[1, me]
        masks.append([slot_mask(extra_rank(rank), EXTRA, SLOTS)])
        probs.append([jnp.sum(jnp.where(hot_rows(rank), prob, 0.0), axis=0, keepdims=True)])
    emit(masks, probs, EXTRA, per_group * 2 * SLOTS)


class Stage:
    def __init__(self, main, bufs, sems, outs):
        self.main, self.bufs, self.sems, self.outs, self.busy, self.turn = main, bufs, sems, outs, {}, 0

    def gather(self, i, kinds, *args):
        slot, self.turn = self.turn, 1 - self.turn
        self.drain(slot)
        views = [self.bufs[k].at[slot] for k in range(kinds)]
        gather_rows(*args, *(views + [None])[:3])
        copies = []
        for k in range(kinds):
            copies.append(pltpu.make_async_copy(views[k].at[pl.ds(0, self.main)], self.outs[2 * k].at[i], self.sems.at[slot, 2 * k]))
            copies.append(pltpu.make_async_copy(views[k].at[pl.ds(self.main, 2 * EXTRA)], self.outs[2 * k + 1].at[i], self.sems.at[slot, 2 * k + 1]))
        for c in copies:
            c.start()
        self.busy[slot] = copies

    def drain(self, slot):
        for c in self.busy.pop(slot, ()):
            c.wait()


def device_of(bit):
    return (lax.axis_index("dp") ^ (bit >> 2), lax.axis_index("ep") ^ (bit & 3))


def greet(bits):
    barrier = pltpu.get_barrier_semaphore()
    for bit in bits:
        pl.semaphore_signal(barrier, inc=1, device_id=device_of(bit), device_id_type=MESH)
    pl.semaphore_wait(barrier, len(bits))


def near_kernel(per_group, x_ref, g_ref, idx_ref, wr_ref, *refs):
    rows_out, (xs_out, ms_out, hot_out) = refs[:6], refs[6:9]
    x_in, g_in, i_in, st_x, st_d, st_g, send, recv, out_sem, st_sem = refs[9:]
    me = lax.axis_index("ep")
    greet((1, 2, 4))
    own = (x_ref, g_ref, idx_ref)
    land = lambda s: own if s == 0 else (x_in.at[s - 1], g_in.at[s - 1], i_in.at[s - 1])
    flights = {}

    def push(k, source, s, bit):
        c = pltpu.make_async_remote_copy(src_ref=land(source)[k], dst_ref=land(s)[k], send_sem=send.at[s - 1, k], recv_sem=recv.at[s - 1, k], device_id=device_of(bit), device_id_type=MESH)
        c.start()
        flights[s, k] = c

    outs = []

    def arrive(k, s, *onward):
        flights[s, k].wait_recv()
        for to, bit in onward:
            push(k, s, to, bit)
        if k == 0:
            c = pltpu.make_async_copy(land(s)[k], xs_out.at[s - 1], out_sem.at[s - 1])
            c.start()
            outs.append(c)

    stage = Stage(per_group * 2 * SLOTS, (st_x, st_d, st_g), st_sem, rows_out)

    def routing(s):
        x, _, idx = land(s)
        route(per_group, x, idx, wr_ref, ms_out.at[s])
        hot = hot_rows(ms_out[s, 0, me]).astype(jnp.int32)
        shape = (hot.shape[0], hot_out.shape[1])
        diagonal = lax.broadcasted_iota(jnp.int32, shape, 0) == lax.broadcasted_iota(jnp.int32, shape, 1)
        hot_out[s : s + 1, :] = jnp.sum(jnp.where(diagonal, hot, 0), axis=0, keepdims=True)

    def gather(s):
        pair = (s, s + 1)
        stage.gather(s // 2, 3 if s < 4 else 2, me, per_group, [ms_out.at[i] for i in pair], [land(i)[0] for i in pair], [land(i)[1] for i in pair])

    X, G, I = range(3)
    for k in (X, I, G):
        push(k, 0, 2, 2)
    for k in (G, I, X):
        push(k, 0, 4, 4)
    for k in (X, I, G):
        push(k, 0, 1, 1)
    routing(0)
    for k in (X, G, I):
        arrive(k, 1)
    routing(1)
    gather(0)
    arrive(X, 2, (6, 4), (3, 1))
    arrive(I, 2, (6, 4), (3, 1))
    arrive(G, 4, (6, 2), (5, 1))
    arrive(I, 4, (5, 1))
    routing(2)
    arrive(X, 3)
    arrive(I, 3)
    routing(3)
    arrive(G, 2, (3, 1))
    arrive(X, 4, (5, 1))
    routing(4)
    arrive(G, 3)
    gather(2)
    for k in (X, G, I):
        arrive(k, 5)
    routing(5)
    gather(4)
    for k in (X, I, G):
        arrive(k, 6, (7, 1))
    routing(6)
    for k in (X, I, G):
        arrive(k, 7)
    routing(7)
    gather(6)
    stage.drain(0)
    stage.drain(1)
    for c in flights.values():
        c.wait_send()
    for c in outs:
        c.wait()


def back_kernel(q_ref, keep_ref, give_ref, peer_ref, q_out, part_in, q_in, send, recv, q_send, q_recv, ld_sem):
    n_dev = q_in.shape[0]
    greet(tuple(range(1, n_dev)))

    def push(src, dst, bit, s_sem, r_sem):
        c = pltpu.make_async_remote_copy(src_ref=src, dst_ref=dst, send_sem=s_sem, recv_sem=r_sem, device_id=device_of(bit), device_id_type=MESH)
        c.start()
        return c

    part = push(give_ref, part_in, 1, send.at[0], recv.at[0])
    load = pltpu.make_async_copy(keep_ref, peer_ref, ld_sem.at[0])
    load.start()
    qs = [push(q_ref, q_in.at[bit], bit, q_send.at[bit], q_recv.at[bit]) for bit in range(1, n_dev)]
    q_out[0] = q_ref[...]
    load.wait()
    part.wait_recv()
    peer_ref[...] += part_in[...]
    for i, c in enumerate(qs):
        c.wait_recv()
        q_out[i + 1] = q_in[i + 1]
    for c in qs + [part]:
        c.wait_send()


def expert_math(x, d, w1, w3, w2):
    z1 = nn_dot(x, w1)
    z3 = nn_dot(x, w3)
    sig = jax.nn.sigmoid(z1)
    silu = z1 * sig
    act = (silu * z3).astype(BF16)
    d_act = nt_dot(d, w2)
    dz1 = (d_act * z3 * sig * (1.0 + z1 * (1.0 - sig))).astype(BF16)
    dz3 = (d_act * silu).astype(BF16)
    return act, dz1, dz3


def flat(ref, first=0, count=None):
    v = ref[first : first + (count or ref.shape[0])]
    return v.reshape(v.shape[0] * v.shape[1], v.shape[2])


def hot_column(is_hot):
    return jnp.concatenate([jnp.full((EXTRA, 1), 1.0, F32) * h.astype(F32) for h in is_hot], axis=0) > 0.0


def masked(column, v):
    return jnp.where(column, v.astype(F32), 0.0).astype(BF16)


def pass1_kernel(per_group, hot_ref, ep_ref, w1_ref, w3_ref, w2_ref, x_ref, d_ref, g_ref, xo_hbm, do_hbm, go_hbm, ms_ref, *refs):
    n_pair = g_ref.shape[0]
    n_sh, n_all = 2 * n_pair, hot_ref.shape[0]
    gx_hbms, (q_ref, act_ref, dz_ref, acto_ref, dzo_ref, r_scr, gx_scr, xo_ref, do_ref, go_ref, gx_sem, more_sem) = refs[:n_sh], refs[n_sh:]
    more = [pltpu.make_async_copy(src, dst, more_sem.at[i]) for i, (src, dst) in enumerate(((xo_hbm, xo_ref), (do_hbm, do_ref), (go_hbm, go_ref)))]
    e = pl.program_id(0)
    ff = w1_ref.shape[2]
    w1, w3, w2 = w1_ref[0], w3_ref[0], w2_ref[0]
    base = per_group * SPAN
    m_of = lambda j: ms_ref.at[j, 0, 0]

    def token_math(act, dz1, dz3, g):
        q = jnp.sum(nn_dot(act, w2) * g.astype(F32), axis=1, keepdims=True)
        return q, nt_dot(dz1, w1) + nt_dot(dz3, w3)

    @pl.when(e == 0)
    def _():
        for c in more:
            c.start()
        r_scr[:, base:, :] = jnp.zeros((n_sh, TAIL, r_scr.shape[2]), BF16)
        for i in range(per_group):
            r_scr[:, i * SPAN + SPAN - 16 : (i + 1) * SPAN, :] = jnp.zeros((n_sh, 16, r_scr.shape[2]), BF16)
        acto_ref[...] = jnp.zeros_like(acto_ref)
        dzo_ref[...] = jnp.zeros_like(dzo_ref)

    act, dz1, dz3 = expert_math(flat(x_ref), flat(d_ref), w1, w3, w2)
    act_ref[0] = act
    dz_ref[0, :, :ff] = dz1
    dz_ref[0, :, ff:] = dz3
    near = n_sh * SLOTS
    q, r = token_math(act[:near], dz1[:near], dz3[:near], flat(g_ref))
    for j in range(n_sh):
        rows = slice(j * SLOTS, (j + 1) * SLOTS)
        mask = slot_mask(m_of(j)[pl.ds(e, 1), :], SLOTS, 0)
        q_ref[pl.ds(j * per_group + e, 1), :] = jnp.sum(jnp.where(mask, q[rows], 0.0), axis=0, keepdims=True)
        r_scr[j, pl.ds(pl.multiple_of(e * SPAN, SPAN), SLOTS), :] = r[rows].astype(BF16)

    @pl.when(e == 0)
    def _():
        for c in more:
            c.wait()

    for first in range(0, n_all, n_sh):
        is_hot = [hot_ref[first + j, e] for j in range(n_sh)]

        @pl.when(sum(is_hot) > 0)
        def _():
            part = first // 2
            column = hot_column(is_hot)
            d = masked(column, flat(do_ref, part, n_pair))
            act, dz1, dz3 = expert_math(flat(xo_ref, part, n_pair), d, w1, w3, w2)
            shape = (n_pair, 2 * EXTRA, ff)
            acto_ref[part : part + n_pair] += masked(column, act).reshape(shape)
            dzo_ref[part : part + n_pair, :, :ff] += dz1.reshape(shape)
            dzo_ref[part : part + n_pair, :, ff:] += dz3.reshape(shape)
            if first == 0:
                q, r = token_math(act, dz1, dz3, flat(go_ref))
                for j in range(n_sh):
                    rows = slice(j * EXTRA, (j + 1) * EXTRA)

                    @pl.when(is_hot[j] > 0)
                    def _():
                        mask = slot_mask(m_of(j)[pl.ds(e, 1), :], EXTRA, SLOTS)
                        q_ref[pl.ds(j * per_group + e, 1), :] += jnp.sum(jnp.where(mask, q[rows], 0.0), axis=0, keepdims=True)
                        r_scr[j, base : base + EXTRA, :] = r[rows].astype(BF16)

    @pl.when(e == per_group - 1)
    def _():
        outs = []
        for j in range(n_sh):
            rank = m_of(j)[...]
            low = jnp.where(rank < SLOTS, rank, -1.0)
            masks = [slot_mask(low[i : i + 1, :], SPAN, 0) for i in range(per_group)]
            masks.append(slot_mask(extra_rank(rank), TAIL, SLOTS))
            pick = jnp.concatenate([m.astype(F32) for m in masks], axis=0).astype(BF16)
            gx_scr[j] = tn_dot(pick, r_scr[j])
            outs.append(pltpu.make_async_copy(gx_scr.at[j], gx_hbms[j], gx_sem.at[j]))
            outs[j].start()
        for c in outs:
            c.wait()


def pass2_kernel(hot_ref, act_ref, dz_ref, x_ref, d_ref, xo_hbm, do_hbm, acto_hbm, dzo_hbm, g1_ref, g3_ref, g2_ref, xo_ref, do_ref, acto_ref, dzo_ref, more_sem):
    e = pl.program_id(0)
    pieces = ((xo_hbm, xo_ref), (do_hbm, do_ref), (acto_hbm, acto_ref), (dzo_hbm, dzo_ref))
    more = [pltpu.make_async_copy(src, dst, more_sem.at[i]) for i, (src, dst) in enumerate(pieces)]

    @pl.when(e == 0)
    def _():
        for c in more:
            c.start()

    ff = g1_ref.shape[2]
    x = flat(x_ref)
    g1_ref[0] = tn_dot(x, dz_ref[0, :, :ff])
    g3_ref[0] = tn_dot(x, dz_ref[0, :, ff:])
    g2_ref[0] = tn_dot(act_ref[0], flat(d_ref))

    @pl.when(e == 0)
    def _():
        for c in more:
            c.wait()

    is_hot = [hot_ref[j, e] for j in range(hot_ref.shape[0])]

    @pl.when(sum(is_hot) > 0)
    def _():
        column = hot_column(is_hot)
        x = flat(xo_ref)
        dz = masked(column, flat(dzo_ref))
        g1_ref[0] += tn_dot(x, dz[:, :ff])
        g3_ref[0] += tn_dot(x, dz[:, ff:])
        g2_ref[0] += tn_dot(flat(acto_ref), masked(column, flat(do_ref)))


def finish_kernel(per_group, groups, ep_ref, own_ref, near_ref, far_ref, wr_ref, x0_ref, xs_ref, ms_ref, q_ref, gx_ref, gr_ref, wr_scr, acc):
    n_sh = q_ref.shape[0]
    ep = ep_ref[0]
    span = lambda m: slice(m * per_group, (m + 1) * per_group)
    for a in range(groups):

        @pl.when(ep == a)
        def _():
            for m in range(groups):
                wr_scr[span(m), :] = wr_ref[span(a ^ m), :]

    for s in range(n_sh):
        d, j = divmod(s, groups)
        q = [q_ref[d * groups + m, span(m ^ j), :] for m in range(groups)]
        p = [ms_ref[s, 0, ep ^ m][:per_group] for m in range(groups)]
        mean = sum(jnp.sum(a * b, axis=0, keepdims=True) for a, b in zip(p, q))
        dl = jnp.concatenate([a * (b - mean) for a, b in zip(p, q)], axis=0).astype(BF16)
        term = nn_dot(dl, x0_ref[...] if s == 0 else xs_ref[s - 1])
        if s == 0:
            gx_ref[...] = (own_ref[...] + near_ref[...] + far_ref[...] + tn_dot(dl, wr_scr[...])).astype(BF16)
            acc[...] = term
        else:
            acc[...] += term
    for a in range(groups):

        @pl.when(ep == a)
        def _():
            for m in range(groups):
                gr_ref[span(a ^ m), :] = acc[span(m), :]


def solution(mesh):
    dp, ep = mesh.shape["dp"], mesh.shape["ep"]
    n_dev = dp * ep
    tok_spec = P(("dp", "ep"), None)
    exp_spec = P("ep", None, None)

    def swap(v, bit):
        return lax.ppermute(v, ("dp", "ep"), [(s, s ^ bit) for s in range(n_dev)])

    def device_step(x_loc, route_idx, w_router, w_gate, w_up, w_down, dy_loc):
        toks, dim = x_loc.shape
        top_k = route_idx.shape[1]
        n_exp = w_router.shape[1]
        n_loc, _, ff = w_gate.shape
        me = lax.axis_index("ep")
        ep_arr = me.reshape(1).astype(jnp.int32)
        vmem = pl.BlockSpec(memory_space=pltpu.VMEM)
        params = pltpu.CompilerParams(vmem_limit_bytes=VMEM_LIMIT)

        m_shape = (2, ep, PAD, toks)
        hbm = pl.BlockSpec(memory_space=pl.ANY)
        main = n_loc * 2 * SLOTS
        pairs = n_dev // 2
        sds = jax.ShapeDtypeStruct
        others = n_dev - 1
        x_rows, x_more, d_rows, d_more, g_rows, g_more, xs, ms, hot = pl.pallas_call(
            functools.partial(near_kernel, n_loc),
            out_shape=[
                sds((pairs, main, dim), BF16),
                sds((pairs, 2 * EXTRA, dim), BF16),
                sds((pairs, main, dim), BF16),
                sds((pairs, 2 * EXTRA, dim), BF16),
                sds((ep // 2, main, dim), BF16),
                sds((ep // 2, 2 * EXTRA, dim), BF16),
                sds((others, toks, dim), BF16),
                sds((n_dev,) + m_shape, F32),
                sds((n_dev, 128), jnp.int32),
            ],
            in_specs=[vmem] * 4,
            out_specs=[hbm] * 7 + [vmem] * 2,
            scratch_shapes=[
                pltpu.VMEM((others, toks, dim), BF16),
                pltpu.VMEM((others, toks, dim), BF16),
                pltpu.VMEM((others, top_k, toks), jnp.int32),
                pltpu.VMEM((2, main + 2 * EXTRA, dim), BF16),
                pltpu.VMEM((2, main + 2 * EXTRA, dim), BF16),
                pltpu.VMEM((2, main + 2 * EXTRA, dim), BF16),
                pltpu.SemaphoreType.DMA((others, 3)),
                pltpu.SemaphoreType.DMA((others, 3)),
                pltpu.SemaphoreType.DMA((others,)),
                pltpu.SemaphoreType.DMA((2, 6)),
            ],
            compiler_params=pltpu.CompilerParams(collective_id=0, has_side_effects=True, vmem_limit_bytes=VMEM_LIMIT),
            cost_estimate=pl.CostEstimate(flops=2 * 10**10, bytes_accessed=5 * 10**7, transcendentals=0),
            name="near",
        )(x_loc, dy_loc, route_idx.T, w_router.T)

        w_specs = lambda im: [pl.BlockSpec((1, dim, ff), im), pl.BlockSpec((1, dim, ff), im), pl.BlockSpec((1, ff, dim), im)]
        im3 = lambda e, hot, ep_ref: (e, 0, 0)
        rows_at = lambda e, hot, ep_ref: (0, e, 0)
        fix = lambda shape: pl.BlockSpec(shape, lambda e, hot, ep_ref: (0,) * len(shape), pipeline_mode=pl.Buffered(1))
        n_row = n_dev * SLOTS
        *gx_part, q_loc, act, dz, act_more, dz_more = pl.pallas_call(
            functools.partial(pass1_kernel, n_loc),
            out_shape=[sds((toks, dim), F32)] * ep
            + [
                sds((ep * n_loc, toks), F32),
                sds((n_loc, n_row, ff), BF16),
                sds((n_loc, n_row, 2 * ff), BF16),
                sds((pairs, 2 * EXTRA, ff), BF16),
                sds((pairs, 2 * EXTRA, 2 * ff), BF16),
            ],
            grid_spec=pltpu.PrefetchScalarGridSpec(
                num_scalar_prefetch=2,
                grid=(n_loc,),
                in_specs=w_specs(im3)
                + [pl.BlockSpec((pairs, 2 * SLOTS, dim), rows_at)] * 2
                + [pl.BlockSpec((ep // 2, 2 * SLOTS, dim), rows_at)]
                + [hbm] * 3
                + [pl.BlockSpec((ep, 1, 1, PAD, toks), lambda e, hot, ep_ref: (0, 0, ep_ref[0], 0, 0))],
                out_specs=[hbm] * ep
                + [fix((ep * n_loc, toks)), pl.BlockSpec((1, n_row, ff), im3), pl.BlockSpec((1, n_row, 2 * ff), im3)]
                + [fix((pairs, 2 * EXTRA, ff)), fix((pairs, 2 * EXTRA, 2 * ff))],
                scratch_shapes=[
                    pltpu.VMEM((ep, n_loc * SPAN + TAIL, dim), BF16),
                    pltpu.VMEM((ep, toks, dim), F32),
                    pltpu.VMEM((pairs, 2 * EXTRA, dim), BF16),
                    pltpu.VMEM((pairs, 2 * EXTRA, dim), BF16),
                    pltpu.VMEM((ep // 2, 2 * EXTRA, dim), BF16),
                    pltpu.SemaphoreType.DMA((ep,)),
                    pltpu.SemaphoreType.DMA((3,)),
                ],
            ),
            compiler_params=params,
            cost_estimate=pl.CostEstimate(flops=4 * 10**10, bytes_accessed=10**8, transcendentals=0),
            name="pass1",
        )(hot, ep_arr, w_gate, w_up, w_down, x_rows, d_rows, g_rows, x_more, d_more, g_more, ms)

        for_peer, q_all = pl.pallas_call(
            back_kernel,
            out_shape=[sds((toks, dim), F32), sds((n_dev, ep * n_loc, toks), F32)],
            in_specs=[vmem, hbm, hbm],
            out_specs=[vmem] * 2,
            scratch_shapes=[
                pltpu.VMEM((toks, dim), F32),
                pltpu.VMEM((n_dev, ep * n_loc, toks), F32),
                pltpu.SemaphoreType.DMA((1,)),
                pltpu.SemaphoreType.DMA((1,)),
                pltpu.SemaphoreType.DMA((n_dev,)),
                pltpu.SemaphoreType.DMA((n_dev,)),
                pltpu.SemaphoreType.DMA((1,)),
            ],
            compiler_params=pltpu.CompilerParams(collective_id=1, has_side_effects=True, vmem_limit_bytes=VMEM_LIMIT),
            cost_estimate=pl.CostEstimate(flops=8 * 10**9, bytes_accessed=5 * 10**7, transcendentals=0),
            name="back",
        )(q_loc, gx_part[2], gx_part[3])
        for_peer, for_core = lax.optimization_barrier((for_peer, gx_part[1]))
        from_peer = swap(for_peer, 2)
        from_core = swap(for_core, 1)

        im3 = lambda e, hot: (e, 0, 0)
        rows_at = lambda e, hot: (0, e, 0)
        fix = lambda shape: pl.BlockSpec(shape, lambda e, hot: (0,) * len(shape), pipeline_mode=pl.Buffered(1))
        grad_gate, grad_up, grad_down = pl.pallas_call(
            pass2_kernel,
            out_shape=[sds((n_loc, dim, ff), F32), sds((n_loc, dim, ff), F32), sds((n_loc, ff, dim), F32)],
            grid_spec=pltpu.PrefetchScalarGridSpec(
                num_scalar_prefetch=1,
                grid=(n_loc,),
                in_specs=[pl.BlockSpec((1, n_row, ff), im3), pl.BlockSpec((1, n_row, 2 * ff), im3)]
                + [pl.BlockSpec((pairs, 2 * SLOTS, dim), rows_at)] * 2
                + [hbm] * 4,
                out_specs=w_specs(im3),
                scratch_shapes=[
                    pltpu.VMEM((pairs, 2 * EXTRA, dim), BF16),
                    pltpu.VMEM((pairs, 2 * EXTRA, dim), BF16),
                    pltpu.VMEM((pairs, 2 * EXTRA, ff), BF16),
                    pltpu.VMEM((pairs, 2 * EXTRA, 2 * ff), BF16),
                    pltpu.SemaphoreType.DMA((4,)),
                ],
            ),
            compiler_params=params,
            cost_estimate=pl.CostEstimate(flops=6 * 10**10, bytes_accessed=2 * 10**8, transcendentals=0),
            name="pass2",
        )(hot, act, dz, x_rows, d_rows, x_more, d_more, act_more, dz_more)

        fixed = lambda shape: pl.BlockSpec(shape, lambda i, ep_ref: (0,) * len(shape))
        grad_x, grad_rt = pl.pallas_call(
            functools.partial(finish_kernel, n_loc, ep),
            out_shape=[sds((toks, dim), BF16), sds((n_exp, dim), F32)],
            grid_spec=pltpu.PrefetchScalarGridSpec(
                num_scalar_prefetch=1,
                grid=(1,),
                in_specs=[fixed(v.shape) for v in (gx_part[0], from_core, from_peer, w_router.T, x_loc, xs)]
                + [pl.BlockSpec((n_dev, 1, ep, PAD, toks), lambda i, ep_ref: (0, 1, 0, 0, 0)), fixed(q_all.shape)],
                out_specs=[fixed((toks, dim)), fixed((n_exp, dim))],
                scratch_shapes=[pltpu.VMEM((n_exp, dim), BF16), pltpu.VMEM((n_exp, dim), F32)],
            ),
            compiler_params=params,
            cost_estimate=pl.CostEstimate(flops=4 * 10**9, bytes_accessed=10**7, transcendentals=0),
            name="finish",
        )(ep_arr, gx_part[0], from_core, from_peer, w_router.T, x_loc, xs, ms, q_all)
        grad_router = grad_rt.T
        return grad_x, grad_gate, grad_up, grad_down, grad_router

    return jax.shard_map(device_step, mesh=mesh, in_specs=(tok_spec, tok_spec, P(), exp_spec, exp_spec, exp_spec, tok_spec), out_specs=(tok_spec, exp_spec, exp_spec, exp_spec, P()), check_vma=False)
```

```python
import functools

import jax
import jax.numpy as jnp
from jax import lax
from jax.experimental import pallas as pl
from jax.experimental.pallas import tpu as pltpu
from jax.sharding import PartitionSpec as P

SLOTS = 56
EXTRA = 104
SPAN = 64
TAIL = 112
PAD = 16
F32 = jnp.float32
BF16 = jnp.bfloat16
VMEM_LIMIT = 67043328
MESH = pl.DeviceIdType.MESH


def nt_dot(a, b):
    return lax.dot_general(a, b, (((1,), (1,)), ((), ())), preferred_element_type=F32)


def tn_dot(a, b):
    return lax.dot_general(a, b, (((0,), (0,)), ((), ())), preferred_element_type=F32)


def nn_dot(a, b):
    return jnp.dot(a, b, preferred_element_type=F32)


def slot_mask(rank_row, rows, first):
    slot = lax.broadcasted_iota(jnp.int32, (rows, rank_row.shape[1]), 0) + first
    return slot.astype(F32) == rank_row


def hot_rows(rank):
    return jnp.max(rank, axis=1, keepdims=True) >= SLOTS


def extra_rank(rank):
    return jnp.max(jnp.where(hot_rows(rank), rank, -1.0), axis=0, keepdims=True)


def route(per_group, x_ref, idx_ref, wr_ref, out_ref):
    groups, toks = out_ref.shape[1], x_ref.shape[0]
    logits = nt_dot(wr_ref[...], x_ref[...])
    expert = lax.broadcasted_iota(jnp.int32, logits.shape, 0)
    chosen = expert == idx_ref[0:1, :]
    for k in range(1, idx_ref.shape[0]):
        chosen = chosen | (expert == idx_ref[k : k + 1, :])
    before = lax.broadcasted_iota(jnp.int32, (toks, toks), 0) < lax.broadcasted_iota(jnp.int32, (toks, toks), 1)
    rank = nn_dot(chosen.astype(F32).astype(BF16), before.astype(F32).astype(BF16))
    top = jnp.max(jnp.where(chosen, logits, -jnp.inf), axis=0, keepdims=True)
    weight = jnp.where(chosen, jnp.exp(logits - top), 0.0)
    prob = weight / jnp.sum(weight, axis=0, keepdims=True)
    rank = jnp.where(chosen, rank, -1.0)
    for a in range(groups):
        rows = slice(a * per_group, (a + 1) * per_group)
        out_ref[0, a, :per_group, :] = rank[rows]
        out_ref[0, a, per_group:, :] = jnp.full((PAD - per_group, toks), -1.0, F32)
        out_ref[1, a, :per_group, :] = prob[rows]
        out_ref[1, a, per_group:, :] = jnp.zeros((PAD - per_group, toks), F32)


def gather_rows(me, per_group, m_refs, x_refs, g_refs, x_out, d_out, g_out):
    step = per_group // 2

    def emit(masks, probs, size, first):
        def put(out, pair):
            for k in range(len(masks[0])):
                rows = jnp.concatenate([v[k * size : (k + 1) * size] for v in pair], axis=0)
                start = first + k * (2 * size)
                out[pl.ds(start if isinstance(start, int) else pl.multiple_of(start, 16), 2 * size), :] = rows.astype(BF16)

        picks = [jnp.concatenate([m.astype(F32) for m in ms], axis=0).astype(BF16) for ms in masks]
        put(x_out, [nn_dot(pick, x[...]) for pick, x in zip(picks, x_refs)])
        rows_g = [nn_dot(pick, g[...]) for pick, g in zip(picks, g_refs)]
        if g_out is not None:
            put(g_out, rows_g)
        gates = [jnp.concatenate([jnp.sum(jnp.where(m, p, 0.0), axis=1, keepdims=True) for m, p in zip(*mp)], axis=0) for mp in zip(masks, probs)]
        put(d_out, [gate * v for gate, v in zip(gates, rows_g)])

    def part(i, carry):
        masks = [[slot_mask(m[0, me, pl.ds(i * step + k, 1), :], SLOTS, 0) for k in range(step)] for m in m_refs]
        probs = [[m[1, me, pl.ds(i * step + k, 1), :] for k in range(step)] for m in m_refs]
        emit(masks, probs, SLOTS, i * (step * 2 * SLOTS))
        return carry

    lax.fori_loop(0, 2, part, 0)
    masks, probs = [], []
    for m in m_refs:
        rank, prob = m[0, me], m[1, me]
        masks.append([slot_mask(extra_rank(rank), EXTRA, SLOTS)])
        probs.append([jnp.sum(jnp.where(hot_rows(rank), prob, 0.0), axis=0, keepdims=True)])
    emit(masks, probs, EXTRA, per_group * 2 * SLOTS)


class Stage:
    def __init__(self, main, bufs, sems, outs):
        self.main, self.bufs, self.sems, self.outs, self.busy, self.turn = main, bufs, sems, outs, {}, 0

    def gather(self, index, *args):
        kinds = len(index)
        slot, self.turn = self.turn, 1 - self.turn
        self.drain(slot)
        views = [self.bufs[k].at[slot] for k in range(kinds)]
        gather_rows(*args, *(views + [None])[:3])
        copies = []
        for k in range(kinds):
            copies.append(pltpu.make_async_copy(views[k].at[pl.ds(0, self.main)], self.outs[2 * k].at[index[k]], self.sems.at[slot, 2 * k]))
            copies.append(pltpu.make_async_copy(views[k].at[pl.ds(self.main, 2 * EXTRA)], self.outs[2 * k + 1].at[index[k]], self.sems.at[slot, 2 * k + 1]))
        for c in copies:
            c.start()
        self.busy[slot] = copies

    def drain(self, slot):
        for c in self.busy.pop(slot, ()):
            c.wait()


def device_of(bit):
    return (lax.axis_index("dp") ^ (bit >> 2), lax.axis_index("ep") ^ (bit & 3))


def greet(bits):
    barrier = pltpu.get_barrier_semaphore()
    for bit in bits:
        pl.semaphore_signal(barrier, inc=1, device_id=device_of(bit), device_id_type=MESH)
    pl.semaphore_wait(barrier, len(bits))


def near_kernel(per_group, x_ref, g_ref, idx_ref, wr_ref, w1_hbm, w3_hbm, w2_hbm, *refs):
    rows_out, (xs_out, act_out, dz_out, ms_out, hot_out, q_out) = refs[:6], refs[6:12]
    x_in, g_in, i_in, st_x, st_d, st_g, w1_buf, w3_buf, w2_buf, act_scr, dz_scr, send, recv, out_sem, st_sem, w_sem = refs[12:]
    me = lax.axis_index("ep")
    n_dev = hot_out.shape[0]

    def weights(e, slot):
        pairs = ((w1_hbm, w1_buf), (w3_hbm, w3_buf), (w2_hbm, w2_buf))
        return [pltpu.make_async_copy(src.at[e], dst.at[slot], w_sem.at[slot, i]) for i, (src, dst) in enumerate(pairs)]

    for c in weights(0, 0):
        c.start()
    greet((1, 2, 4))
    own = (x_ref, g_ref, idx_ref)
    land = lambda s: own if s == 0 else (x_in.at[s - 1], g_in.at[s - 1], i_in.at[s - 1])
    flights = {}

    def push(k, source, s, bit):
        c = pltpu.make_async_remote_copy(src_ref=land(source)[k], dst_ref=land(s)[k], send_sem=send.at[s - 1, k], recv_sem=recv.at[s - 1, k], device_id=device_of(bit), device_id_type=MESH)
        c.start()
        flights[s, k] = c

    outs = []

    def arrive(k, s, *onward):
        flights[s, k].wait_recv()
        for to, bit in onward:
            push(k, s, to, bit)
        if k == 0:
            c = pltpu.make_async_copy(land(s)[k], xs_out.at[s - 1], out_sem.at[s - 1])
            c.start()
            outs.append(c)

    stage = Stage(per_group * 2 * SLOTS, (st_x, st_d, st_g), st_sem, rows_out)

    def routing(s):
        x, _, idx = land(s)
        route(per_group, x, idx, wr_ref, ms_out.at[s])
        hot = hot_rows(ms_out[s, 0, me]).astype(jnp.int32)
        shape = (hot.shape[0], hot_out.shape[1])
        diagonal = lax.broadcasted_iota(jnp.int32, shape, 0) == lax.broadcasted_iota(jnp.int32, shape, 1)
        row = (s - 2) % n_dev
        hot_out[row : row + 1, :] = jnp.sum(jnp.where(diagonal, hot, 0), axis=0, keepdims=True)

    def gather(s):
        pair = (s, s + 1)
        place = (s // 2 - 1) % (n_dev // 2)
        index = (place, place, 1 - s // 2) if s < 4 else (place, place)
        stage.gather(index, me, per_group, [ms_out.at[i] for i in pair], [land(i)[0] for i in pair], [land(i)[1] for i in pair])

    def own_chip(e, carry):
        slot = lax.rem(e, 2)
        for c in weights(e, slot):
            c.wait()

        @pl.when(e + 1 < per_group)
        def _():
            for c in weights(e + 1, 1 - slot):
                c.start()

        ff = act_scr.shape[2]
        rows = pl.ds(pl.multiple_of(e * (2 * SLOTS), 16), 2 * SLOTS)
        w2 = w2_buf[slot]
        act, dz1, dz3 = expert_math(st_x[0, rows, :], st_d[0, rows, :], w1_buf[slot], w3_buf[slot], w2)
        act_scr[e] = act
        dz_scr[e, :, :ff] = dz1
        dz_scr[e, :, ff:] = dz3
        q = jnp.sum(nn_dot(act, w2) * st_g[0, rows, :].astype(F32), axis=1, keepdims=True)
        for j in range(2):
            mask = slot_mask(ms_out[j, 0, me, pl.ds(e, 1), :], SLOTS, 0)
            q_out[pl.ds(j * per_group + e, 1), :] = jnp.sum(jnp.where(mask, q[j * SLOTS : (j + 1) * SLOTS], 0.0), axis=0, keepdims=True)
        return carry

    X, G, I = range(3)
    for k in (X, I, G):
        push(k, 0, 2, 2)
    for k in (G, I, X):
        push(k, 0, 4, 4)
    for k in (X, I, G):
        push(k, 0, 1, 1)
    routing(0)
    for k in (X, G, I):
        arrive(k, 1)
    routing(1)
    gather(0)
    lax.fori_loop(0, per_group, own_chip, 0)
    for i, (src, dst) in enumerate(((act_scr, act_out), (dz_scr, dz_out))):
        c = pltpu.make_async_copy(src, dst, out_sem.at[n_dev - 1 + i])
        c.start()
        outs.append(c)
    arrive(X, 2, (6, 4), (3, 1))
    arrive(I, 2, (6, 4), (3, 1))
    arrive(G, 4, (6, 2), (5, 1))
    arrive(I, 4, (5, 1))
    routing(2)
    arrive(X, 3)
    arrive(I, 3)
    routing(3)
    arrive(G, 2, (3, 1))
    arrive(X, 4, (5, 1))
    routing(4)
    arrive(G, 3)
    gather(2)
    for k in (X, G, I):
        arrive(k, 5)
    routing(5)
    gather(4)
    for k in (X, I, G):
        arrive(k, 6, (7, 1))
    routing(6)
    for k in (X, I, G):
        arrive(k, 7)
    routing(7)
    gather(6)
    stage.drain(0)
    stage.drain(1)
    for c in flights.values():
        c.wait_send()
    for c in outs:
        c.wait()


def back_kernel(q_ref, keep_ref, give_ref, peer_ref, q_out, part_in, q_in, send, recv, q_send, q_recv, ld_sem):
    n_dev = q_in.shape[0]
    greet(tuple(range(1, n_dev)))

    def push(src, dst, bit, s_sem, r_sem):
        c = pltpu.make_async_remote_copy(src_ref=src, dst_ref=dst, send_sem=s_sem, recv_sem=r_sem, device_id=device_of(bit), device_id_type=MESH)
        c.start()
        return c

    part = push(give_ref, part_in, 1, send.at[0], recv.at[0])
    load = pltpu.make_async_copy(keep_ref, peer_ref, ld_sem.at[0])
    load.start()
    qs = [push(q_ref, q_in.at[bit], bit, q_send.at[bit], q_recv.at[bit]) for bit in range(1, n_dev)]
    q_out[0] = q_ref[...]
    load.wait()
    part.wait_recv()
    peer_ref[...] += part_in[...]
    for i, c in enumerate(qs):
        c.wait_recv()
        q_out[i + 1] = q_in[i + 1]
    for c in qs + [part]:
        c.wait_send()


def expert_math(x, d, w1, w3, w2):
    z1 = nn_dot(x, w1)
    z3 = nn_dot(x, w3)
    sig = jax.nn.sigmoid(z1)
    silu = z1 * sig
    act = (silu * z3).astype(BF16)
    d_act = nt_dot(d, w2)
    dz1 = (d_act * z3 * sig * (1.0 + z1 * (1.0 - sig))).astype(BF16)
    dz3 = (d_act * silu).astype(BF16)
    return act, dz1, dz3


def flat(ref, first=0, count=None):
    v = ref[first : first + (count or ref.shape[0])]
    return v.reshape(v.shape[0] * v.shape[1], v.shape[2])


def hot_column(is_hot):
    return jnp.concatenate([jnp.full((EXTRA, 1), 1.0, F32) * h.astype(F32) for h in is_hot], axis=0) > 0.0


def masked(column, v):
    return jnp.where(column, v.astype(F32), 0.0).astype(BF16)


def pass1_kernel(per_group, order, hot_ref, ep_ref, w1_ref, w3_ref, w2_ref, x_ref, d_ref, g_ref, dz01_ref, q01_ref, xo_hbm, do_hbm, go_hbm, ms_ref, *refs):
    n_sh, n_all = len(order), hot_ref.shape[0]
    gx_hbms, (q_ref, act_ref, dz_ref, acto_ref, dzo_ref, r_scr, gx_scr, xo_ref, do_ref, go_ref, gx_sem, more_sem) = refs[:n_sh], refs[n_sh:]
    more = [pltpu.make_async_copy(src, dst, more_sem.at[i]) for i, (src, dst) in enumerate(((xo_hbm, xo_ref), (do_hbm, do_ref), (go_hbm, go_ref)))]
    e = pl.program_id(0)
    ff = w1_ref.shape[2]
    w1, w3, w2 = w1_ref[0], w3_ref[0], w2_ref[0]
    base = per_group * SPAN
    m_of = lambda i: ms_ref.at[order[i], 0, 0]
    q_row = lambda i: pl.ds(order[i] * per_group + e, 1)

    def q_math(act, g):
        return jnp.sum(nn_dot(act, w2) * g.astype(F32), axis=1, keepdims=True)

    def r_math(dz1, dz3):
        return nt_dot(dz1, w1) + nt_dot(dz3, w3)

    @pl.when(e == 0)
    def _():
        for c in more:
            c.start()
        r_scr[:, base:, :] = jnp.zeros((n_sh, TAIL, r_scr.shape[2]), BF16)
        for i in range(per_group):
            r_scr[:, i * SPAN + SPAN - 16 : (i + 1) * SPAN, :] = jnp.zeros((n_sh, 16, r_scr.shape[2]), BF16)
        acto_ref[...] = jnp.zeros_like(acto_ref)
        dzo_ref[...] = jnp.zeros_like(dzo_ref)
        q_ref[: 2 * per_group, :] = q01_ref[...]

    act, dz1, dz3 = expert_math(flat(x_ref), flat(d_ref), w1, w3, w2)
    act_ref[0] = act
    dz_ref[0, :, :ff] = dz1
    dz_ref[0, :, ff:] = dz3
    near = 2 * SLOTS
    q = q_math(act[:near], flat(g_ref))
    r = r_math(jnp.concatenate([dz1[:near], dz01_ref[0, :, :ff]], axis=0), jnp.concatenate([dz3[:near], dz01_ref[0, :, ff:]], axis=0))
    for i in range(n_sh):
        rows = slice(i * SLOTS, (i + 1) * SLOTS)
        if i < 2:
            mask = slot_mask(m_of(i)[pl.ds(e, 1), :], SLOTS, 0)
            q_ref[q_row(i), :] = jnp.sum(jnp.where(mask, q[rows], 0.0), axis=0, keepdims=True)
        r_scr[i, pl.ds(pl.multiple_of(e * SPAN, SPAN), SLOTS), :] = r[rows].astype(BF16)

    @pl.when(e == 0)
    def _():
        for c in more:
            c.wait()

    last = n_all // 2 - 1
    for near_part in (True, False):
        places = (0, last) if near_part else tuple(range(1, last))
        is_hot = [hot_ref[2 * place + k, e] for place in places for k in range(2)]

        @pl.when(sum(is_hot) > 0)
        def _():
            column = hot_column(is_hot)
            take = lambda ref: jnp.concatenate([ref[place] for place in places], axis=0)
            act, dz1, dz3 = expert_math(take(xo_ref), masked(column, take(do_ref)), w1, w3, w2)
            kept = masked(column, act)
            for i, place in enumerate(places):
                rows = slice(i * 2 * EXTRA, (i + 1) * 2 * EXTRA)
                acto_ref[place] += kept[rows]
                dzo_ref[place, :, :ff] += dz1[rows]
                dzo_ref[place, :, ff:] += dz3[rows]
            if near_part:
                q, r = q_math(act, flat(go_ref)), r_math(dz1, dz3)
                for i in range(n_sh):
                    rows = slice(i * EXTRA, (i + 1) * EXTRA)

                    @pl.when(is_hot[i] > 0)
                    def _():
                        mask = slot_mask(m_of(i)[pl.ds(e, 1), :], EXTRA, SLOTS)
                        q_ref[q_row(i), :] += jnp.sum(jnp.where(mask, q[rows], 0.0), axis=0, keepdims=True)
                        r_scr[i, base : base + EXTRA, :] = r[rows].astype(BF16)

    @pl.when(e == per_group - 1)
    def _():
        outs = []
        for i in range(n_sh - 1, -1, -1):
            rank = m_of(i)[...]
            low = jnp.where(rank < SLOTS, rank, -1.0)
            masks = [slot_mask(low[k : k + 1, :], SPAN, 0) for k in range(per_group)]
            masks.append(slot_mask(extra_rank(rank), TAIL, SLOTS))
            pick = jnp.concatenate([m.astype(F32) for m in masks], axis=0).astype(BF16)
            gx_scr[i] = tn_dot(pick, r_scr[i])
            outs.append(pltpu.make_async_copy(gx_scr.at[i], gx_hbms[order[i]], gx_sem.at[i]))
            outs[-1].start()
        for c in outs:
            c.wait()


def pass2_kernel(hot_ref, act_ref, dz_ref, act01_ref, dz01_ref, x_ref, d_ref, xo_hbm, do_hbm, acto_hbm, dzo_hbm, g1_ref, g3_ref, g2_ref, xo_ref, do_ref, acto_ref, dzo_ref, more_sem):
    e = pl.program_id(0)
    pieces = ((xo_hbm, xo_ref), (do_hbm, do_ref), (acto_hbm, acto_ref), (dzo_hbm, dzo_ref))
    more = [pltpu.make_async_copy(src, dst, more_sem.at[i]) for i, (src, dst) in enumerate(pieces)]

    @pl.when(e == 0)
    def _():
        for c in more:
            c.start()

    ff = g1_ref.shape[2]
    x = flat(x_ref)
    g1_ref[0] = tn_dot(x, jnp.concatenate([dz_ref[0, :, :ff], dz01_ref[0, :, :ff]], axis=0))
    g3_ref[0] = tn_dot(x, jnp.concatenate([dz_ref[0, :, ff:], dz01_ref[0, :, ff:]], axis=0))
    g2_ref[0] = tn_dot(jnp.concatenate([act_ref[0], act01_ref[0]], axis=0), flat(d_ref))

    @pl.when(e == 0)
    def _():
        for c in more:
            c.wait()

    is_hot = [hot_ref[j, e] for j in range(hot_ref.shape[0])]

    @pl.when(sum(is_hot) > 0)
    def _():
        column = hot_column(is_hot)
        x = flat(xo_ref)
        dz = masked(column, flat(dzo_ref))
        g1_ref[0] += tn_dot(x, dz[:, :ff])
        g3_ref[0] += tn_dot(x, dz[:, ff:])
        g2_ref[0] += tn_dot(flat(acto_ref), masked(column, flat(do_ref)))


def finish_kernel(per_group, groups, ep_ref, own_ref, near_ref, far_ref, wr_ref, x0_ref, xs_ref, ms_ref, q_ref, gx_ref, gr_ref, wr_scr, acc):
    n_sh = q_ref.shape[0]
    ep = ep_ref[0]
    span = lambda m: slice(m * per_group, (m + 1) * per_group)
    for a in range(groups):

        @pl.when(ep == a)
        def _():
            for m in range(groups):
                wr_scr[span(m), :] = wr_ref[span(a ^ m), :]

    for s in range(n_sh):
        d, j = divmod(s, groups)
        q = [q_ref[d * groups + m, span(m ^ j), :] for m in range(groups)]
        p = [ms_ref[s, 0, ep ^ m][:per_group] for m in range(groups)]
        mean = sum(jnp.sum(a * b, axis=0, keepdims=True) for a, b in zip(p, q))
        dl = jnp.concatenate([a * (b - mean) for a, b in zip(p, q)], axis=0).astype(BF16)
        term = nn_dot(dl, x0_ref[...] if s == 0 else xs_ref[s - 1])
        if s == 0:
            gx_ref[...] = (own_ref[...] + near_ref[...] + far_ref[...] + tn_dot(dl, wr_scr[...])).astype(BF16)
            acc[...] = term
        else:
            acc[...] += term
    for a in range(groups):

        @pl.when(ep == a)
        def _():
            for m in range(groups):
                gr_ref[span(a ^ m), :] = acc[span(m), :]


def solution(mesh):
    dp, ep = mesh.shape["dp"], mesh.shape["ep"]
    n_dev = dp * ep
    tok_spec = P(("dp", "ep"), None)
    exp_spec = P("ep", None, None)

    def swap(v, bit):
        return lax.ppermute(v, ("dp", "ep"), [(s, s ^ bit) for s in range(n_dev)])

    def device_step(x_loc, route_idx, w_router, w_gate, w_up, w_down, dy_loc):
        toks, dim = x_loc.shape
        top_k = route_idx.shape[1]
        n_exp = w_router.shape[1]
        n_loc, _, ff = w_gate.shape
        me = lax.axis_index("ep")
        ep_arr = me.reshape(1).astype(jnp.int32)
        vmem = pl.BlockSpec(memory_space=pltpu.VMEM)
        params = pltpu.CompilerParams(vmem_limit_bytes=VMEM_LIMIT)

        m_shape = (2, ep, PAD, toks)
        hbm = pl.BlockSpec(memory_space=pl.ANY)
        main = n_loc * 2 * SLOTS
        pairs = n_dev // 2
        sds = jax.ShapeDtypeStruct
        others = n_dev - 1
        x_rows, x_more, d_rows, d_more, g_rows, g_more, xs, act01, dz01, ms, hot, q01 = pl.pallas_call(
            functools.partial(near_kernel, n_loc),
            out_shape=[
                sds((pairs, main, dim), BF16),
                sds((pairs, 2 * EXTRA, dim), BF16),
                sds((pairs, main, dim), BF16),
                sds((pairs, 2 * EXTRA, dim), BF16),
                sds((ep // 2, main, dim), BF16),
                sds((ep // 2, 2 * EXTRA, dim), BF16),
                sds((others, toks, dim), BF16),
                sds((n_loc, 2 * SLOTS, ff), BF16),
                sds((n_loc, 2 * SLOTS, 2 * ff), BF16),
                sds((n_dev,) + m_shape, F32),
                sds((n_dev, 128), jnp.int32),
                sds((2 * n_loc, toks), F32),
            ],
            in_specs=[vmem] * 4 + [hbm] * 3,
            out_specs=[hbm] * 9 + [vmem] * 3,
            scratch_shapes=[
                pltpu.VMEM((others, toks, dim), BF16),
                pltpu.VMEM((others, toks, dim), BF16),
                pltpu.VMEM((others, top_k, toks), jnp.int32),
                pltpu.VMEM((2, main + 2 * EXTRA, dim), BF16),
                pltpu.VMEM((2, main + 2 * EXTRA, dim), BF16),
                pltpu.VMEM((2, main + 2 * EXTRA, dim), BF16),
                pltpu.VMEM((2, dim, ff), BF16),
                pltpu.VMEM((2, dim, ff), BF16),
                pltpu.VMEM((2, ff, dim), BF16),
                pltpu.VMEM((n_loc, 2 * SLOTS, ff), BF16),
                pltpu.VMEM((n_loc, 2 * SLOTS, 2 * ff), BF16),
                pltpu.SemaphoreType.DMA((others, 3)),
                pltpu.SemaphoreType.DMA((others, 3)),
                pltpu.SemaphoreType.DMA((others + 2,)),
                pltpu.SemaphoreType.DMA((2, 6)),
                pltpu.SemaphoreType.DMA((2, 3)),
            ],
            compiler_params=pltpu.CompilerParams(collective_id=0, has_side_effects=True, vmem_limit_bytes=VMEM_LIMIT),
            cost_estimate=pl.CostEstimate(flops=2 * 10**10, bytes_accessed=5 * 10**7, transcendentals=0),
            name="near",
        )(x_loc, dy_loc, route_idx.T, w_router.T, w_gate, w_up, w_down)

        w_specs = lambda im: [pl.BlockSpec((1, dim, ff), im), pl.BlockSpec((1, dim, ff), im), pl.BlockSpec((1, ff, dim), im)]
        im3 = lambda e, hot, ep_ref: (e, 0, 0)
        rows_at = lambda e, hot, ep_ref: (0, e, 0)
        fix = lambda shape: pl.BlockSpec(shape, lambda e, hot, ep_ref: (0,) * len(shape), pipeline_mode=pl.Buffered(1))
        n_row = (n_dev - 2) * SLOTS
        *gx_part, q_loc, act, dz, act_more, dz_more = pl.pallas_call(
            functools.partial(pass1_kernel, n_loc, (2, 3, 0, 1)),
            out_shape=[sds((toks, dim), F32)] * ep
            + [
                sds((ep * n_loc, toks), F32),
                sds((n_loc, n_row, ff), BF16),
                sds((n_loc, n_row, 2 * ff), BF16),
                sds((pairs, 2 * EXTRA, ff), BF16),
                sds((pairs, 2 * EXTRA, 2 * ff), BF16),
            ],
            grid_spec=pltpu.PrefetchScalarGridSpec(
                num_scalar_prefetch=2,
                grid=(n_loc,),
                in_specs=w_specs(im3)
                + [pl.BlockSpec((pairs - 1, 2 * SLOTS, dim), rows_at)] * 2
                + [pl.BlockSpec((1, 2 * SLOTS, dim), rows_at), pl.BlockSpec((1, 2 * SLOTS, 2 * ff), im3), fix((2 * n_loc, toks))]
                + [hbm] * 3
                + [pl.BlockSpec((ep, 1, 1, PAD, toks), lambda e, hot, ep_ref: (0, 0, ep_ref[0], 0, 0))],
                out_specs=[hbm] * ep
                + [fix((ep * n_loc, toks)), pl.BlockSpec((1, n_row, ff), im3), pl.BlockSpec((1, n_row, 2 * ff), im3)]
                + [fix((pairs, 2 * EXTRA, ff)), fix((pairs, 2 * EXTRA, 2 * ff))],
                scratch_shapes=[
                    pltpu.VMEM((ep, n_loc * SPAN + TAIL, dim), BF16),
                    pltpu.VMEM((ep, toks, dim), F32),
                    pltpu.VMEM((pairs, 2 * EXTRA, dim), BF16),
                    pltpu.VMEM((pairs, 2 * EXTRA, dim), BF16),
                    pltpu.VMEM((ep // 2, 2 * EXTRA, dim), BF16),
                    pltpu.SemaphoreType.DMA((ep,)),
                    pltpu.SemaphoreType.DMA((3,)),
                ],
            ),
            compiler_params=params,
            cost_estimate=pl.CostEstimate(flops=4 * 10**10, bytes_accessed=10**8, transcendentals=0),
            name="pass1",
        )(hot, ep_arr, w_gate, w_up, w_down, x_rows, d_rows, g_rows, dz01, q01, x_more, d_more, g_more, ms)

        for_peer, q_all = pl.pallas_call(
            back_kernel,
            out_shape=[sds((toks, dim), F32), sds((n_dev, ep * n_loc, toks), F32)],
            in_specs=[vmem, hbm, hbm],
            out_specs=[vmem] * 2,
            scratch_shapes=[
                pltpu.VMEM((toks, dim), F32),
                pltpu.VMEM((n_dev, ep * n_loc, toks), F32),
                pltpu.SemaphoreType.DMA((1,)),
                pltpu.SemaphoreType.DMA((1,)),
                pltpu.SemaphoreType.DMA((n_dev,)),
                pltpu.SemaphoreType.DMA((n_dev,)),
                pltpu.SemaphoreType.DMA((1,)),
            ],
            compiler_params=pltpu.CompilerParams(collective_id=1, has_side_effects=True, vmem_limit_bytes=VMEM_LIMIT),
            cost_estimate=pl.CostEstimate(flops=8 * 10**9, bytes_accessed=5 * 10**7, transcendentals=0),
            name="back",
        )(q_loc, gx_part[2], gx_part[3])
        for_peer, for_core = lax.optimization_barrier((for_peer, gx_part[1]))
        from_peer = swap(for_peer, 2)
        from_core = swap(for_core, 1)

        im3 = lambda e, hot: (e, 0, 0)
        rows_at = lambda e, hot: (0, e, 0)
        fix = lambda shape: pl.BlockSpec(shape, lambda e, hot: (0,) * len(shape), pipeline_mode=pl.Buffered(1))
        grad_gate, grad_up, grad_down = pl.pallas_call(
            pass2_kernel,
            out_shape=[sds((n_loc, dim, ff), F32), sds((n_loc, dim, ff), F32), sds((n_loc, ff, dim), F32)],
            grid_spec=pltpu.PrefetchScalarGridSpec(
                num_scalar_prefetch=1,
                grid=(n_loc,),
                in_specs=[pl.BlockSpec((1, n_row, ff), im3), pl.BlockSpec((1, n_row, 2 * ff), im3)]
                + [pl.BlockSpec((1, 2 * SLOTS, ff), im3), pl.BlockSpec((1, 2 * SLOTS, 2 * ff), im3)]
                + [pl.BlockSpec((pairs, 2 * SLOTS, dim), rows_at)] * 2
                + [hbm] * 4,
                out_specs=w_specs(im3),
                scratch_shapes=[
                    pltpu.VMEM((pairs, 2 * EXTRA, dim), BF16),
                    pltpu.VMEM((pairs, 2 * EXTRA, dim), BF16),
                    pltpu.VMEM((pairs, 2 * EXTRA, ff), BF16),
                    pltpu.VMEM((pairs, 2 * EXTRA, 2 * ff), BF16),
                    pltpu.SemaphoreType.DMA((4,)),
                ],
            ),
            compiler_params=params,
            cost_estimate=pl.CostEstimate(flops=6 * 10**10, bytes_accessed=2 * 10**8, transcendentals=0),
            name="pass2",
        )(hot, act, dz, act01, dz01, x_rows, d_rows, x_more, d_more, act_more, dz_more)

        fixed = lambda shape: pl.BlockSpec(shape, lambda i, ep_ref: (0,) * len(shape))
        grad_x, grad_rt = pl.pallas_call(
            functools.partial(finish_kernel, n_loc, ep),
            out_shape=[sds((toks, dim), BF16), sds((n_exp, dim), F32)],
            grid_spec=pltpu.PrefetchScalarGridSpec(
                num_scalar_prefetch=1,
                grid=(1,),
                in_specs=[fixed(v.shape) for v in (gx_part[0], from_core, from_peer, w_router.T, x_loc, xs)]
                + [pl.BlockSpec((n_dev, 1, ep, PAD, toks), lambda i, ep_ref: (0, 1, 0, 0, 0)), fixed(q_all.shape)],
                out_specs=[fixed((toks, dim)), fixed((n_exp, dim))],
                scratch_shapes=[pltpu.VMEM((n_exp, dim), BF16), pltpu.VMEM((n_exp, dim), F32)],
            ),
            compiler_params=params,
            cost_estimate=pl.CostEstimate(flops=4 * 10**9, bytes_accessed=10**7, transcendentals=0),
            name="finish",
        )(ep_arr, gx_part[0], from_core, from_peer, w_router.T, x_loc, xs, ms, q_all)
        grad_router = grad_rt.T
        return grad_x, grad_gate, grad_up, grad_down, grad_router

    return jax.shard_map(device_step, mesh=mesh, in_specs=(tok_spec, tok_spec, P(), exp_spec, exp_spec, exp_spec, tok_spec), out_specs=(tok_spec, exp_spec, exp_spec, exp_spec, P()), check_vma=False)
```

```python
import functools

import jax
import jax.numpy as jnp
from jax import lax
from jax.experimental import pallas as pl
from jax.experimental.pallas import tpu as pltpu
from jax.sharding import PartitionSpec as P

SLOTS = 56
EXTRA = 104
SPAN = 64
TAIL = 112
PAD = 16
F32 = jnp.float32
BF16 = jnp.bfloat16
VMEM_LIMIT = 67043328
MESH = pl.DeviceIdType.MESH


def nt_dot(a, b):
    return lax.dot_general(a, b, (((1,), (1,)), ((), ())), preferred_element_type=F32)


def tn_dot(a, b):
    return lax.dot_general(a, b, (((0,), (0,)), ((), ())), preferred_element_type=F32)


def nn_dot(a, b):
    return jnp.dot(a, b, preferred_element_type=F32)


def slot_mask(rank_row, rows, first):
    slot = lax.broadcasted_iota(jnp.int32, (rows, rank_row.shape[1]), 0) + first
    return slot.astype(F32) == rank_row


def hot_rows(rank):
    return jnp.max(rank, axis=1, keepdims=True) >= SLOTS


def extra_rank(rank):
    return jnp.max(jnp.where(hot_rows(rank), rank, -1.0), axis=0, keepdims=True)


def route(per_group, x_ref, idx_ref, wr_ref, out_ref):
    groups, toks = out_ref.shape[1], x_ref.shape[0]
    logits = nt_dot(wr_ref[...], x_ref[...])
    expert = lax.broadcasted_iota(jnp.int32, logits.shape, 0)
    chosen = expert == idx_ref[0:1, :]
    for k in range(1, idx_ref.shape[0]):
        chosen = chosen | (expert == idx_ref[k : k + 1, :])
    before = lax.broadcasted_iota(jnp.int32, (toks, toks), 0) < lax.broadcasted_iota(jnp.int32, (toks, toks), 1)
    rank = nn_dot(chosen.astype(F32).astype(BF16), before.astype(F32).astype(BF16))
    top = jnp.max(jnp.where(chosen, logits, -jnp.inf), axis=0, keepdims=True)
    weight = jnp.where(chosen, jnp.exp(logits - top), 0.0)
    prob = weight / jnp.sum(weight, axis=0, keepdims=True)
    rank = jnp.where(chosen, rank, -1.0)
    for a in range(groups):
        rows = slice(a * per_group, (a + 1) * per_group)
        out_ref[0, a, :per_group, :] = rank[rows]
        out_ref[0, a, per_group:, :] = jnp.full((PAD - per_group, toks), -1.0, F32)
        out_ref[1, a, :per_group, :] = prob[rows]
        out_ref[1, a, per_group:, :] = jnp.zeros((PAD - per_group, toks), F32)


def gather_rows(me, per_group, m_refs, x_refs, g_refs, x_out, d_out, g_out):
    step = per_group // 2

    def emit(masks, probs, size, first):
        def put(out, pair):
            for k in range(len(masks[0])):
                rows = jnp.concatenate([v[k * size : (k + 1) * size] for v in pair], axis=0)
                start = first + k * (2 * size)
                out[pl.ds(start if isinstance(start, int) else pl.multiple_of(start, 16), 2 * size), :] = rows.astype(BF16)

        picks = [jnp.concatenate([m.astype(F32) for m in ms], axis=0).astype(BF16) for ms in masks]
        put(x_out, [nn_dot(pick, x[...]) for pick, x in zip(picks, x_refs)])
        rows_g = [nn_dot(pick, g[...]) for pick, g in zip(picks, g_refs)]
        if g_out is not None:
            put(g_out, rows_g)
        gates = [jnp.concatenate([jnp.sum(jnp.where(m, p, 0.0), axis=1, keepdims=True) for m, p in zip(*mp)], axis=0) for mp in zip(masks, probs)]
        put(d_out, [gate * v for gate, v in zip(gates, rows_g)])

    def part(i, carry):
        masks = [[slot_mask(m[0, me, pl.ds(i * step + k, 1), :], SLOTS, 0) for k in range(step)] for m in m_refs]
        probs = [[m[1, me, pl.ds(i * step + k, 1), :] for k in range(step)] for m in m_refs]
        emit(masks, probs, SLOTS, i * (step * 2 * SLOTS))
        return carry

    lax.fori_loop(0, 2, part, 0)
    masks, probs = [], []
    for m in m_refs:
        rank, prob = m[0, me], m[1, me]
        masks.append([slot_mask(extra_rank(rank), EXTRA, SLOTS)])
        probs.append([jnp.sum(jnp.where(hot_rows(rank), prob, 0.0), axis=0, keepdims=True)])
    emit(masks, probs, EXTRA, per_group * 2 * SLOTS)


class Stage:
    def __init__(self, main, bufs, sems, outs):
        self.main, self.bufs, self.sems, self.outs, self.busy, self.turn = main, bufs, sems, outs, {}, 0

    def gather(self, index, *args):
        kinds = len(index)
        slot, self.turn = self.turn, 1 - self.turn
        self.drain(slot)
        views = [self.bufs[k].at[slot] for k in range(kinds)]
        gather_rows(*args, *(views + [None])[:3])
        copies = []
        for k in range(kinds):
            copies.append(pltpu.make_async_copy(views[k].at[pl.ds(0, self.main)], self.outs[2 * k].at[index[k]], self.sems.at[slot, 2 * k]))
            copies.append(pltpu.make_async_copy(views[k].at[pl.ds(self.main, 2 * EXTRA)], self.outs[2 * k + 1].at[index[k]], self.sems.at[slot, 2 * k + 1]))
        for c in copies:
            c.start()
        self.busy[slot] = copies

    def drain(self, slot):
        for c in self.busy.pop(slot, ()):
            c.wait()


def device_of(bit):
    return (lax.axis_index("dp") ^ (bit >> 2), lax.axis_index("ep") ^ (bit & 3))


def greet(bits):
    barrier = pltpu.get_barrier_semaphore()
    for bit in bits:
        pl.semaphore_signal(barrier, inc=1, device_id=device_of(bit), device_id_type=MESH)
    pl.semaphore_wait(barrier, len(bits))


def near_kernel(per_group, x_ref, g_ref, idx_ref, wr_ref, w1_hbm, w3_hbm, w2_hbm, *refs):
    rows_out, (xs_out, act_out, dz_out, ms_out, hot_out, q_out) = refs[:6], refs[6:12]
    x_in, g_in, i_in, st_x, st_d, st_g, w1_buf, w3_buf, w2_buf, act_scr, dz_scr, send, recv, out_sem, st_sem, w_sem = refs[12:]
    me = lax.axis_index("ep")
    n_dev = hot_out.shape[0]

    def weights(e, slot):
        pairs = ((w1_hbm, w1_buf), (w3_hbm, w3_buf), (w2_hbm, w2_buf))
        return [pltpu.make_async_copy(src.at[e], dst.at[slot], w_sem.at[slot, i]) for i, (src, dst) in enumerate(pairs)]

    for c in weights(0, 0):
        c.start()
    greet((1, 2, 4))
    own = (x_ref, g_ref, idx_ref)
    land = lambda s: own if s == 0 else (x_in.at[s - 1], g_in.at[s - 1], i_in.at[s - 1])
    flights = {}

    def push(k, source, s, bit):
        c = pltpu.make_async_remote_copy(src_ref=land(source)[k], dst_ref=land(s)[k], send_sem=send.at[s - 1, k], recv_sem=recv.at[s - 1, k], device_id=device_of(bit), device_id_type=MESH)
        c.start()
        flights[s, k] = c

    outs = []

    def arrive(k, s, *onward):
        flights[s, k].wait_recv()
        for to, bit in onward:
            push(k, s, to, bit)
        if k == 0:
            c = pltpu.make_async_copy(land(s)[k], xs_out.at[s - 1], out_sem.at[s - 1])
            c.start()
            outs.append(c)

    stage = Stage(per_group * 2 * SLOTS, (st_x, st_d, st_g), st_sem, rows_out)

    def routing(s):
        x, _, idx = land(s)
        route(per_group, x, idx, wr_ref, ms_out.at[s])
        hot = hot_rows(ms_out[s, 0, me]).astype(jnp.int32)
        shape = (hot.shape[0], hot_out.shape[1])
        diagonal = lax.broadcasted_iota(jnp.int32, shape, 0) == lax.broadcasted_iota(jnp.int32, shape, 1)
        row = (s - 2) % n_dev
        hot_out[row : row + 1, :] = jnp.sum(jnp.where(diagonal, hot, 0), axis=0, keepdims=True)

    def gather(s):
        pair = (s, s + 1)
        place = (s // 2 - 1) % (n_dev // 2)
        index = (place, place, 1 - s // 2) if s < 4 else (place, place)
        stage.gather(index, me, per_group, [ms_out.at[i] for i in pair], [land(i)[0] for i in pair], [land(i)[1] for i in pair])

    def own_chip(e, carry):
        slot = lax.rem(e, 2)
        for c in weights(e, slot):
            c.wait()

        @pl.when(e + 1 < per_group)
        def _():
            for c in weights(e + 1, 1 - slot):
                c.start()

        ff = act_scr.shape[2]
        rows = pl.ds(pl.multiple_of(e * (2 * SLOTS), 16), 2 * SLOTS)
        w2 = w2_buf[slot]
        act, dz1, dz3 = expert_math(st_x[0, rows, :], st_d[0, rows, :], w1_buf[slot], w3_buf[slot], w2)
        act_scr[e] = act
        dz_scr[e, :, :ff] = dz1
        dz_scr[e, :, ff:] = dz3
        q = jnp.sum(nn_dot(act, w2) * st_g[0, rows, :].astype(F32), axis=1, keepdims=True)
        for j in range(2):
            mask = slot_mask(ms_out[j, 0, me, pl.ds(e, 1), :], SLOTS, 0)
            q_out[pl.ds(j * per_group + e, 1), :] = jnp.sum(jnp.where(mask, q[j * SLOTS : (j + 1) * SLOTS], 0.0), axis=0, keepdims=True)
        return carry

    X, G, I = range(3)
    for k in (X, I, G):
        push(k, 0, 2, 2)
    for k in (G, I, X):
        push(k, 0, 4, 4)
    for k in (X, I, G):
        push(k, 0, 1, 1)
    routing(0)
    for k in (X, G, I):
        arrive(k, 1)
    routing(1)
    gather(0)
    lax.fori_loop(0, per_group, own_chip, 0)
    for i, (src, dst) in enumerate(((act_scr, act_out), (dz_scr, dz_out))):
        c = pltpu.make_async_copy(src, dst, out_sem.at[n_dev - 1 + i])
        c.start()
        outs.append(c)
    arrive(X, 2, (6, 4), (3, 1))
    arrive(I, 2, (6, 4), (3, 1))
    arrive(G, 4, (6, 2), (5, 1))
    arrive(I, 4, (5, 1))
    routing(2)
    arrive(X, 3)
    arrive(I, 3)
    routing(3)
    arrive(G, 2, (3, 1))
    arrive(X, 4, (5, 1))
    routing(4)
    arrive(G, 3)
    gather(2)
    for k in (X, G, I):
        arrive(k, 5)
    routing(5)
    gather(4)
    for k in (X, I):
        arrive(k, 6, (7, 1))
    routing(6)
    arrive(G, 6, (7, 1))
    for k in (X, I):
        arrive(k, 7)
    routing(7)
    arrive(G, 7)
    gather(6)
    stage.drain(0)
    stage.drain(1)
    for c in flights.values():
        c.wait_send()
    for c in outs:
        c.wait()


def back_kernel(q_ref, keep_ref, give_ref, peer_ref, q_out, part_in, q_in, send, recv, q_send, q_recv, ld_sem):
    n_dev = q_in.shape[0]
    greet(tuple(range(1, n_dev)))

    def push(src, dst, bit, s_sem, r_sem):
        c = pltpu.make_async_remote_copy(src_ref=src, dst_ref=dst, send_sem=s_sem, recv_sem=r_sem, device_id=device_of(bit), device_id_type=MESH)
        c.start()
        return c

    part = push(give_ref, part_in, 1, send.at[0], recv.at[0])
    load = pltpu.make_async_copy(keep_ref, peer_ref, ld_sem.at[0])
    load.start()
    qs = [push(q_ref, q_in.at[bit], bit, q_send.at[bit], q_recv.at[bit]) for bit in range(1, n_dev)]
    q_out[0] = q_ref[...]
    load.wait()
    part.wait_recv()
    peer_ref[...] += part_in[...]
    for i, c in enumerate(qs):
        c.wait_recv()
        q_out[i + 1] = q_in[i + 1]
    for c in qs + [part]:
        c.wait_send()


def expert_math(x, d, w1, w3, w2):
    z1 = nn_dot(x, w1)
    z3 = nn_dot(x, w3)
    sig = jax.nn.sigmoid(z1)
    silu = z1 * sig
    act = (silu * z3).astype(BF16)
    d_act = nt_dot(d, w2)
    dz1 = (d_act * z3 * sig * (1.0 + z1 * (1.0 - sig))).astype(BF16)
    dz3 = (d_act * silu).astype(BF16)
    return act, dz1, dz3


def flat(ref, first=0, count=None):
    v = ref[first : first + (count or ref.shape[0])]
    return v.reshape(v.shape[0] * v.shape[1], v.shape[2])


def hot_column(is_hot):
    return jnp.concatenate([jnp.full((EXTRA, 1), 1.0, F32) * h.astype(F32) for h in is_hot], axis=0) > 0.0


def masked(column, v):
    return jnp.where(column, v.astype(F32), 0.0).astype(BF16)


def pass1_kernel(per_group, order, hot_ref, ep_ref, w1_ref, w3_ref, w2_ref, x_ref, d_ref, g_ref, act01_ref, dz01_ref, q01_ref, xo_hbm, do_hbm, go_hbm, ms_ref, *refs):
    n_sh, n_all = len(order), hot_ref.shape[0]
    gx_hbms, (q_ref, g2_ref, dz_ref, dzo_ref, r_scr, gx_scr, xo_ref, do_ref, go_ref, gx_sem, more_sem) = refs[:n_sh], refs[n_sh:]
    more = [pltpu.make_async_copy(src, dst, more_sem.at[i]) for i, (src, dst) in enumerate(((xo_hbm, xo_ref), (do_hbm, do_ref), (go_hbm, go_ref)))]
    e = pl.program_id(0)
    ff = w1_ref.shape[2]
    w1, w3, w2 = w1_ref[0], w3_ref[0], w2_ref[0]
    base = per_group * SPAN
    m_of = lambda i: ms_ref.at[order[i], 0, 0]
    q_row = lambda i: pl.ds(order[i] * per_group + e, 1)

    def q_math(act, g):
        return jnp.sum(nn_dot(act, w2) * g.astype(F32), axis=1, keepdims=True)

    def r_math(dz1, dz3):
        return nt_dot(dz1, w1) + nt_dot(dz3, w3)

    @pl.when(e == 0)
    def _():
        for c in more:
            c.start()
        r_scr[:, base:, :] = jnp.zeros((n_sh, TAIL, r_scr.shape[2]), BF16)
        for i in range(per_group):
            r_scr[:, i * SPAN + SPAN - 16 : (i + 1) * SPAN, :] = jnp.zeros((n_sh, 16, r_scr.shape[2]), BF16)
        dzo_ref[...] = jnp.zeros_like(dzo_ref)
        q_ref[: 2 * per_group, :] = q01_ref[...]

    d = flat(d_ref)
    act, dz1, dz3 = expert_math(flat(x_ref), d[: x_ref.shape[0] * x_ref.shape[1]], w1, w3, w2)
    g2_ref[0] = tn_dot(jnp.concatenate([act, act01_ref[0]], axis=0), d)
    dz_ref[0, :, :ff] = dz1
    dz_ref[0, :, ff:] = dz3
    near = 2 * SLOTS
    q = q_math(act[:near], flat(g_ref))
    r = r_math(jnp.concatenate([dz1[:near], dz01_ref[0, :, :ff]], axis=0), jnp.concatenate([dz3[:near], dz01_ref[0, :, ff:]], axis=0))
    for i in range(n_sh):
        rows = slice(i * SLOTS, (i + 1) * SLOTS)
        if i < 2:
            mask = slot_mask(m_of(i)[pl.ds(e, 1), :], SLOTS, 0)
            q_ref[q_row(i), :] = jnp.sum(jnp.where(mask, q[rows], 0.0), axis=0, keepdims=True)
        r_scr[i, pl.ds(pl.multiple_of(e * SPAN, SPAN), SLOTS), :] = r[rows].astype(BF16)

    @pl.when(e == 0)
    def _():
        for c in more:
            c.wait()

    last = n_all // 2 - 1
    for near_part in (True, False):
        places = (0, last) if near_part else tuple(range(1, last))
        is_hot = [hot_ref[2 * place + k, e] for place in places for k in range(2)]

        @pl.when(sum(is_hot) > 0)
        def _():
            column = hot_column(is_hot)
            take = lambda ref: jnp.concatenate([ref[place] for place in places], axis=0)
            d = masked(column, take(do_ref))
            act, dz1, dz3 = expert_math(take(xo_ref), d, w1, w3, w2)
            g2_ref[0] += tn_dot(act, d)
            for i, place in enumerate(places):
                rows = slice(i * 2 * EXTRA, (i + 1) * 2 * EXTRA)
                dzo_ref[place, :, :ff] += dz1[rows]
                dzo_ref[place, :, ff:] += dz3[rows]
            if near_part:
                q, r = q_math(act, flat(go_ref)), r_math(dz1, dz3)
                for i in range(n_sh):
                    rows = slice(i * EXTRA, (i + 1) * EXTRA)

                    @pl.when(is_hot[i] > 0)
                    def _():
                        mask = slot_mask(m_of(i)[pl.ds(e, 1), :], EXTRA, SLOTS)
                        q_ref[q_row(i), :] += jnp.sum(jnp.where(mask, q[rows], 0.0), axis=0, keepdims=True)
                        r_scr[i, base : base + EXTRA, :] = r[rows].astype(BF16)

    @pl.when(e == per_group - 1)
    def _():
        outs = []
        for i in range(n_sh - 1, -1, -1):
            rank = m_of(i)[...]
            low = jnp.where(rank < SLOTS, rank, -1.0)
            masks = [slot_mask(low[k : k + 1, :], SPAN, 0) for k in range(per_group)]
            masks.append(slot_mask(extra_rank(rank), TAIL, SLOTS))
            pick = jnp.concatenate([m.astype(F32) for m in masks], axis=0).astype(BF16)
            gx_scr[i] = tn_dot(pick, r_scr[i])
            outs.append(pltpu.make_async_copy(gx_scr.at[i], gx_hbms[order[i]], gx_sem.at[i]))
            outs[-1].start()
        for c in outs:
            c.wait()


def pass2_kernel(hot_ref, dz_ref, dz01_ref, x_ref, xo_hbm, dzo_hbm, g1_ref, g3_ref, xo_ref, dzo_ref, more_sem):
    e = pl.program_id(0)
    pieces = ((xo_hbm, xo_ref), (dzo_hbm, dzo_ref))
    more = [pltpu.make_async_copy(src, dst, more_sem.at[i]) for i, (src, dst) in enumerate(pieces)]

    @pl.when(e == 0)
    def _():
        for c in more:
            c.start()

    ff = g1_ref.shape[2]
    x = flat(x_ref)
    g1_ref[0] = tn_dot(x, jnp.concatenate([dz_ref[0, :, :ff], dz01_ref[0, :, :ff]], axis=0))
    g3_ref[0] = tn_dot(x, jnp.concatenate([dz_ref[0, :, ff:], dz01_ref[0, :, ff:]], axis=0))

    @pl.when(e == 0)
    def _():
        for c in more:
            c.wait()

    is_hot = [hot_ref[j, e] for j in range(hot_ref.shape[0])]

    @pl.when(sum(is_hot) > 0)
    def _():
        column = hot_column(is_hot)
        x = flat(xo_ref)
        dz = masked(column, flat(dzo_ref))
        g1_ref[0] += tn_dot(x, dz[:, :ff])
        g3_ref[0] += tn_dot(x, dz[:, ff:])


def finish_kernel(per_group, groups, ep_ref, own_ref, near_ref, far_ref, wr_ref, x0_ref, xs_ref, ms_ref, q_ref, gx_ref, gr_ref, wr_scr, acc):
    n_sh = q_ref.shape[0]
    ep = ep_ref[0]
    span = lambda m: slice(m * per_group, (m + 1) * per_group)
    for a in range(groups):

        @pl.when(ep == a)
        def _():
            for m in range(groups):
                wr_scr[span(m), :] = wr_ref[span(a ^ m), :]

    for s in range(n_sh):
        d, j = divmod(s, groups)
        q = [q_ref[d * groups + m, span(m ^ j), :] for m in range(groups)]
        p = [ms_ref[s, 0, ep ^ m][:per_group] for m in range(groups)]
        mean = sum(jnp.sum(a * b, axis=0, keepdims=True) for a, b in zip(p, q))
        dl = jnp.concatenate([a * (b - mean) for a, b in zip(p, q)], axis=0).astype(BF16)
        term = nn_dot(dl, x0_ref[...] if s == 0 else xs_ref[s - 1])
        if s == 0:
            gx_ref[...] = (own_ref[...] + near_ref[...] + far_ref[...] + tn_dot(dl, wr_scr[...])).astype(BF16)
            acc[...] = term
        else:
            acc[...] += term
    for a in range(groups):

        @pl.when(ep == a)
        def _():
            for m in range(groups):
                gr_ref[span(a ^ m), :] = acc[span(m), :]


def solution(mesh):
    dp, ep = mesh.shape["dp"], mesh.shape["ep"]
    n_dev = dp * ep
    tok_spec = P(("dp", "ep"), None)
    exp_spec = P("ep", None, None)

    def swap(v, bit):
        return lax.ppermute(v, ("dp", "ep"), [(s, s ^ bit) for s in range(n_dev)])

    def device_step(x_loc, route_idx, w_router, w_gate, w_up, w_down, dy_loc):
        toks, dim = x_loc.shape
        top_k = route_idx.shape[1]
        n_exp = w_router.shape[1]
        n_loc, _, ff = w_gate.shape
        me = lax.axis_index("ep")
        ep_arr = me.reshape(1).astype(jnp.int32)
        vmem = pl.BlockSpec(memory_space=pltpu.VMEM)
        params = pltpu.CompilerParams(vmem_limit_bytes=VMEM_LIMIT)

        m_shape = (2, ep, PAD, toks)
        hbm = pl.BlockSpec(memory_space=pl.ANY)
        main = n_loc * 2 * SLOTS
        pairs = n_dev // 2
        sds = jax.ShapeDtypeStruct
        others = n_dev - 1
        x_rows, x_more, d_rows, d_more, g_rows, g_more, xs, act01, dz01, ms, hot, q01 = pl.pallas_call(
            functools.partial(near_kernel, n_loc),
            out_shape=[
                sds((pairs, main, dim), BF16),
                sds((pairs, 2 * EXTRA, dim), BF16),
                sds((pairs, main, dim), BF16),
                sds((pairs, 2 * EXTRA, dim), BF16),
                sds((ep // 2, main, dim), BF16),
                sds((ep // 2, 2 * EXTRA, dim), BF16),
                sds((others, toks, dim), BF16),
                sds((n_loc, 2 * SLOTS, ff), BF16),
                sds((n_loc, 2 * SLOTS, 2 * ff), BF16),
                sds((n_dev,) + m_shape, F32),
                sds((n_dev, 128), jnp.int32),
                sds((2 * n_loc, toks), F32),
            ],
            in_specs=[vmem] * 4 + [hbm] * 3,
            out_specs=[hbm] * 9 + [vmem] * 3,
            scratch_shapes=[
                pltpu.VMEM((others, toks, dim), BF16),
                pltpu.VMEM((others, toks, dim), BF16),
                pltpu.VMEM((others, top_k, toks), jnp.int32),
                pltpu.VMEM((2, main + 2 * EXTRA, dim), BF16),
                pltpu.VMEM((2, main + 2 * EXTRA, dim), BF16),
                pltpu.VMEM((2, main + 2 * EXTRA, dim), BF16),
                pltpu.VMEM((2, dim, ff), BF16),
                pltpu.VMEM((2, dim, ff), BF16),
                pltpu.VMEM((2, ff, dim), BF16),
                pltpu.VMEM((n_loc, 2 * SLOTS, ff), BF16),
                pltpu.VMEM((n_loc, 2 * SLOTS, 2 * ff), BF16),
                pltpu.SemaphoreType.DMA((others, 3)),
                pltpu.SemaphoreType.DMA((others, 3)),
                pltpu.SemaphoreType.DMA((others + 2,)),
                pltpu.SemaphoreType.DMA((2, 6)),
                pltpu.SemaphoreType.DMA((2, 3)),
            ],
            compiler_params=pltpu.CompilerParams(collective_id=0, has_side_effects=True, vmem_limit_bytes=VMEM_LIMIT),
            cost_estimate=pl.CostEstimate(flops=2 * 10**10, bytes_accessed=5 * 10**7, transcendentals=0),
            name="near",
        )(x_loc, dy_loc, route_idx.T, w_router.T, w_gate, w_up, w_down)

        w_specs = lambda im: [pl.BlockSpec((1, dim, ff), im), pl.BlockSpec((1, dim, ff), im), pl.BlockSpec((1, ff, dim), im)]
        im3 = lambda e, hot, ep_ref: (e, 0, 0)
        rows_at = lambda e, hot, ep_ref: (0, e, 0)
        fix = lambda shape: pl.BlockSpec(shape, lambda e, hot, ep_ref: (0,) * len(shape), pipeline_mode=pl.Buffered(1))
        n_row = (n_dev - 2) * SLOTS
        *gx_part, q_loc, grad_down, dz, dz_more = pl.pallas_call(
            functools.partial(pass1_kernel, n_loc, (2, 3, 0, 1)),
            out_shape=[sds((toks, dim), F32)] * ep
            + [
                sds((ep * n_loc, toks), F32),
                sds((n_loc, ff, dim), F32),
                sds((n_loc, n_row, 2 * ff), BF16),
                sds((pairs, 2 * EXTRA, 2 * ff), BF16),
            ],
            grid_spec=pltpu.PrefetchScalarGridSpec(
                num_scalar_prefetch=2,
                grid=(n_loc,),
                in_specs=w_specs(im3)
                + [pl.BlockSpec((pairs - 1, 2 * SLOTS, dim), rows_at), pl.BlockSpec((pairs, 2 * SLOTS, dim), rows_at)]
                + [pl.BlockSpec((1, 2 * SLOTS, dim), rows_at), pl.BlockSpec((1, 2 * SLOTS, ff), im3), pl.BlockSpec((1, 2 * SLOTS, 2 * ff), im3), fix((2 * n_loc, toks))]
                + [hbm] * 3
                + [pl.BlockSpec((ep, 1, 1, PAD, toks), lambda e, hot, ep_ref: (0, 0, ep_ref[0], 0, 0))],
                out_specs=[hbm] * ep
                + [fix((ep * n_loc, toks)), pl.BlockSpec((1, ff, dim), im3), pl.BlockSpec((1, n_row, 2 * ff), im3)]
                + [fix((pairs, 2 * EXTRA, 2 * ff))],
                scratch_shapes=[
                    pltpu.VMEM((ep, n_loc * SPAN + TAIL, dim), BF16),
                    pltpu.VMEM((ep, toks, dim), F32),
                    pltpu.VMEM((pairs, 2 * EXTRA, dim), BF16),
                    pltpu.VMEM((pairs, 2 * EXTRA, dim), BF16),
                    pltpu.VMEM((ep // 2, 2 * EXTRA, dim), BF16),
                    pltpu.SemaphoreType.DMA((ep,)),
                    pltpu.SemaphoreType.DMA((3,)),
                ],
            ),
            compiler_params=params,
            cost_estimate=pl.CostEstimate(flops=4 * 10**10, bytes_accessed=10**8, transcendentals=0),
            name="pass1",
        )(hot, ep_arr, w_gate, w_up, w_down, x_rows, d_rows, g_rows, act01, dz01, q01, x_more, d_more, g_more, ms)

        for_peer, q_all = pl.pallas_call(
            back_kernel,
            out_shape=[sds((toks, dim), F32), sds((n_dev, ep * n_loc, toks), F32)],
            in_specs=[vmem, hbm, hbm],
            out_specs=[vmem] * 2,
            scratch_shapes=[
                pltpu.VMEM((toks, dim), F32),
                pltpu.VMEM((n_dev, ep * n_loc, toks), F32),
                pltpu.SemaphoreType.DMA((1,)),
                pltpu.SemaphoreType.DMA((1,)),
                pltpu.SemaphoreType.DMA((n_dev,)),
                pltpu.SemaphoreType.DMA((n_dev,)),
                pltpu.SemaphoreType.DMA((1,)),
            ],
            compiler_params=pltpu.CompilerParams(collective_id=1, has_side_effects=True, vmem_limit_bytes=VMEM_LIMIT),
            cost_estimate=pl.CostEstimate(flops=8 * 10**9, bytes_accessed=5 * 10**7, transcendentals=0),
            name="back",
        )(q_loc, gx_part[2], gx_part[3])
        for_peer, for_core = lax.optimization_barrier((for_peer, gx_part[1]))
        from_peer = swap(for_peer, 2)
        from_core = swap(for_core, 1)

        im3 = lambda e, hot: (e, 0, 0)
        rows_at = lambda e, hot: (0, e, 0)
        fix = lambda shape: pl.BlockSpec(shape, lambda e, hot: (0,) * len(shape), pipeline_mode=pl.Buffered(1))
        grad_gate, grad_up = pl.pallas_call(
            pass2_kernel,
            out_shape=[sds((n_loc, dim, ff), F32)] * 2,
            grid_spec=pltpu.PrefetchScalarGridSpec(
                num_scalar_prefetch=1,
                grid=(n_loc,),
                in_specs=[pl.BlockSpec((1, n_row, 2 * ff), im3), pl.BlockSpec((1, 2 * SLOTS, 2 * ff), im3)]
                + [pl.BlockSpec((pairs, 2 * SLOTS, dim), rows_at)]
                + [hbm] * 2,
                out_specs=[pl.BlockSpec((1, dim, ff), im3)] * 2,
                scratch_shapes=[
                    pltpu.VMEM((pairs, 2 * EXTRA, dim), BF16),
                    pltpu.VMEM((pairs, 2 * EXTRA, 2 * ff), BF16),
                    pltpu.SemaphoreType.DMA((2,)),
                ],
            ),
            compiler_params=params,
            cost_estimate=pl.CostEstimate(flops=6 * 10**10, bytes_accessed=2 * 10**8, transcendentals=0),
            name="pass2",
        )(hot, dz, dz01, x_rows, x_more, dz_more)

        fixed = lambda shape: pl.BlockSpec(shape, lambda i, ep_ref: (0,) * len(shape))
        grad_x, grad_rt = pl.pallas_call(
            functools.partial(finish_kernel, n_loc, ep),
            out_shape=[sds((toks, dim), BF16), sds((n_exp, dim), F32)],
            grid_spec=pltpu.PrefetchScalarGridSpec(
                num_scalar_prefetch=1,
                grid=(1,),
                in_specs=[fixed(v.shape) for v in (gx_part[0], from_core, from_peer, w_router.T, x_loc, xs)]
                + [pl.BlockSpec((n_dev, 1, ep, PAD, toks), lambda i, ep_ref: (0, 1, 0, 0, 0)), fixed(q_all.shape)],
                out_specs=[fixed((toks, dim)), fixed((n_exp, dim))],
                scratch_shapes=[pltpu.VMEM((n_exp, dim), BF16), pltpu.VMEM((n_exp, dim), F32)],
            ),
            compiler_params=params,
            cost_estimate=pl.CostEstimate(flops=4 * 10**9, bytes_accessed=10**7, transcendentals=0),
            name="finish",
        )(ep_arr, gx_part[0], from_core, from_peer, w_router.T, x_loc, xs, ms, q_all)
        grad_router = grad_rt.T
        return grad_x, grad_gate, grad_up, grad_down, grad_router

    return jax.shard_map(device_step, mesh=mesh, in_specs=(tok_spec, tok_spec, P(), exp_spec, exp_spec, exp_spec, tok_spec), out_specs=(tok_spec, exp_spec, exp_spec, exp_spec, P()), check_vma=False)
```

```python
import functools

import jax
import jax.numpy as jnp
from jax import lax
from jax.experimental import pallas as pl
from jax.experimental.pallas import tpu as pltpu
from jax.sharding import PartitionSpec as P

SLOTS = 56
EXTRA = 104
SPAN = 64
TAIL = 112
PAD = 16
F32 = jnp.float32
BF16 = jnp.bfloat16
VMEM_LIMIT = 67043328
MESH = pl.DeviceIdType.MESH


def nt_dot(a, b):
    return lax.dot_general(a, b, (((1,), (1,)), ((), ())), preferred_element_type=F32)


def tn_dot(a, b):
    return lax.dot_general(a, b, (((0,), (0,)), ((), ())), preferred_element_type=F32)


def nn_dot(a, b):
    return jnp.dot(a, b, preferred_element_type=F32)


def slot_mask(rank_row, rows, first):
    slot = lax.broadcasted_iota(jnp.int32, (rows, rank_row.shape[1]), 0) + first
    return slot.astype(F32) == rank_row


def hot_rows(rank):
    return jnp.max(rank, axis=1, keepdims=True) >= SLOTS


def extra_rank(rank):
    return jnp.max(jnp.where(hot_rows(rank), rank, -1.0), axis=0, keepdims=True)


def route(per_group, x_ref, idx_ref, wr_ref, out_ref):
    groups, toks = out_ref.shape[1], x_ref.shape[0]
    logits = nt_dot(wr_ref[...], x_ref[...])
    expert = lax.broadcasted_iota(jnp.int32, logits.shape, 0)
    chosen = expert == idx_ref[0:1, :]
    for k in range(1, idx_ref.shape[0]):
        chosen = chosen | (expert == idx_ref[k : k + 1, :])
    before = lax.broadcasted_iota(jnp.int32, (toks, toks), 0) < lax.broadcasted_iota(jnp.int32, (toks, toks), 1)
    rank = nn_dot(chosen.astype(F32).astype(BF16), before.astype(F32).astype(BF16))
    top = jnp.max(jnp.where(chosen, logits, -jnp.inf), axis=0, keepdims=True)
    weight = jnp.where(chosen, jnp.exp(logits - top), 0.0)
    prob = weight / jnp.sum(weight, axis=0, keepdims=True)
    rank = jnp.where(chosen, rank, -1.0)
    for a in range(groups):
        rows = slice(a * per_group, (a + 1) * per_group)
        out_ref[0, a, :per_group, :] = rank[rows]
        out_ref[0, a, per_group:, :] = jnp.full((PAD - per_group, toks), -1.0, F32)
        out_ref[1, a, :per_group, :] = prob[rows]
        out_ref[1, a, per_group:, :] = jnp.zeros((PAD - per_group, toks), F32)


def gather_rows(send, me, per_group, m_refs, x_refs, g_refs, x_out, d_out, g_out):
    step = per_group // 2

    def emit(masks, probs, size, first):
        def put(out, pair):
            for k in range(len(masks[0])):
                rows = jnp.concatenate([v[k * size : (k + 1) * size] for v in pair], axis=0)
                start = first + k * (2 * size)
                out[pl.ds(start if isinstance(start, int) else pl.multiple_of(start, 16), 2 * size), :] = rows.astype(BF16)

        picks = [jnp.concatenate([m.astype(F32) for m in ms], axis=0).astype(BF16) for ms in masks]
        put(x_out, [nn_dot(pick, x[...]) for pick, x in zip(picks, x_refs)])
        rows_g = [nn_dot(pick, g[...]) for pick, g in zip(picks, g_refs)]
        if g_out is not None:
            put(g_out, rows_g)
        gates = [jnp.concatenate([jnp.sum(jnp.where(m, p, 0.0), axis=1, keepdims=True) for m, p in zip(*mp)], axis=0) for mp in zip(masks, probs)]
        put(d_out, [gate * v for gate, v in zip(gates, rows_g)])

    def part(i, carry):
        masks = [[slot_mask(m[0, me, pl.ds(i * step + k, 1), :], SLOTS, 0) for k in range(step)] for m in m_refs]
        probs = [[m[1, me, pl.ds(i * step + k, 1), :] for k in range(step)] for m in m_refs]
        emit(masks, probs, SLOTS, i * (step * 2 * SLOTS))
        send(pl.ds(pl.multiple_of(i * (step * 2 * SLOTS), 16), step * 2 * SLOTS))
        return carry

    lax.fori_loop(0, 2, part, 0)
    masks, probs = [], []
    for m in m_refs:
        rank, prob = m[0, me], m[1, me]
        masks.append([slot_mask(extra_rank(rank), EXTRA, SLOTS)])
        probs.append([jnp.sum(jnp.where(hot_rows(rank), prob, 0.0), axis=0, keepdims=True)])
    emit(masks, probs, EXTRA, per_group * 2 * SLOTS)


class Stage:
    def __init__(self, main, bufs, sems, outs):
        self.main, self.bufs, self.sems, self.outs, self.busy, self.turn = main, bufs, sems, outs, {}, 0

    def gather(self, index, *args):
        kinds = len(index)
        slot, self.turn = self.turn, 1 - self.turn
        self.drain(slot)
        views = [self.bufs[k].at[slot] for k in range(kinds)]

        def main_copies(rows):
            return [pltpu.make_async_copy(views[k].at[rows], self.outs[2 * k].at[index[k], rows], self.sems.at[slot, 2 * k]) for k in range(kinds)]

        def send(rows):
            for c in main_copies(rows):
                c.start()

        gather_rows(send, *args, *(views + [None])[:3])
        extra = [pltpu.make_async_copy(views[k].at[pl.ds(self.main, 2 * EXTRA)], self.outs[2 * k + 1].at[index[k]], self.sems.at[slot, 2 * k + 1]) for k in range(kinds)]
        for c in extra:
            c.start()
        copies = main_copies(pl.ds(0, self.main)) + extra
        self.busy[slot] = copies

    def drain(self, slot):
        for c in self.busy.pop(slot, ()):
            c.wait()


def device_of(bit):
    return (lax.axis_index("dp") ^ (bit >> 2), lax.axis_index("ep") ^ (bit & 3))


def greet(bits):
    barrier = pltpu.get_barrier_semaphore()
    for bit in bits:
        pl.semaphore_signal(barrier, inc=1, device_id=device_of(bit), device_id_type=MESH)
    pl.semaphore_wait(barrier, len(bits))


def near_kernel(per_group, x_ref, g_ref, idx_ref, wr_ref, w1_hbm, w3_hbm, w2_hbm, *refs):
    rows_out, (xs_out, act_out, dz_out, ms_out, hot_out, q_out) = refs[:6], refs[6:12]
    x_in, g_in, i_in, st_x, st_d, st_g, w1_buf, w3_buf, w2_buf, act_scr, dz_scr, send, recv, out_sem, st_sem, w_sem = refs[12:]
    me = lax.axis_index("ep")
    n_dev = hot_out.shape[0]

    def weights(e, slot):
        pairs = ((w1_hbm, w1_buf), (w3_hbm, w3_buf), (w2_hbm, w2_buf))
        return [pltpu.make_async_copy(src.at[e], dst.at[slot], w_sem.at[slot, i]) for i, (src, dst) in enumerate(pairs)]

    for c in weights(0, 0):
        c.start()
    greet((1, 2, 4))
    own = (x_ref, g_ref, idx_ref)
    land = lambda s: own if s == 0 else (x_in.at[s - 1], g_in.at[s - 1], i_in.at[s - 1])
    flights = {}

    def push(k, source, s, bit):
        c = pltpu.make_async_remote_copy(src_ref=land(source)[k], dst_ref=land(s)[k], send_sem=send.at[s - 1, k], recv_sem=recv.at[s - 1, k], device_id=device_of(bit), device_id_type=MESH)
        c.start()
        flights[s, k] = c

    outs = []

    def arrive(k, s, *onward):
        flights[s, k].wait_recv()
        for to, bit in onward:
            push(k, s, to, bit)
        if k == 0:
            c = pltpu.make_async_copy(land(s)[k], xs_out.at[s - 1], out_sem.at[s - 1])
            c.start()
            outs.append(c)

    stage = Stage(per_group * 2 * SLOTS, (st_x, st_d, st_g), st_sem, rows_out)

    def routing(s):
        x, _, idx = land(s)
        route(per_group, x, idx, wr_ref, ms_out.at[s])
        hot = hot_rows(ms_out[s, 0, me]).astype(jnp.int32)
        shape = (hot.shape[0], hot_out.shape[1])
        diagonal = lax.broadcasted_iota(jnp.int32, shape, 0) == lax.broadcasted_iota(jnp.int32, shape, 1)
        row = (s - 2) % n_dev
        hot_out[row : row + 1, :] = jnp.sum(jnp.where(diagonal, hot, 0), axis=0, keepdims=True)

    def gather(s):
        pair = (s, s + 1)
        place = (s // 2 - 1) % (n_dev // 2)
        index = (place, place, 1 - s // 2) if s < 4 else (place, place)
        stage.gather(index, me, per_group, [ms_out.at[i] for i in pair], [land(i)[0] for i in pair], [land(i)[1] for i in pair])

    def own_chip(e, carry):
        slot = lax.rem(e, 2)
        for c in weights(e, slot):
            c.wait()

        @pl.when(e + 1 < per_group)
        def _():
            for c in weights(e + 1, 1 - slot):
                c.start()

        ff = act_scr.shape[2]
        rows = pl.ds(pl.multiple_of(e * (2 * SLOTS), 16), 2 * SLOTS)
        w2 = w2_buf[slot]
        act, dz1, dz3 = expert_math(st_x[0, rows, :], st_d[0, rows, :], w1_buf[slot], w3_buf[slot], w2)
        act_scr[e] = act
        dz_scr[e, :, :ff] = dz1
        dz_scr[e, :, ff:] = dz3
        q = jnp.sum(nn_dot(act, w2) * st_g[0, rows, :].astype(F32), axis=1, keepdims=True)
        for j in range(2):
            mask = slot_mask(ms_out[j, 0, me, pl.ds(e, 1), :], SLOTS, 0)
            q_out[pl.ds(j * per_group + e, 1), :] = jnp.sum(jnp.where(mask, q[j * SLOTS : (j + 1) * SLOTS], 0.0), axis=0, keepdims=True)
        return carry

    X, G, I = range(3)
    for k in (X, I, G):
        push(k, 0, 2, 2)
    for k in (G, I, X):
        push(k, 0, 4, 4)
    for k in (X, I, G):
        push(k, 0, 1, 1)
    routing(0)
    for k in (X, G, I):
        arrive(k, 1)
    routing(1)
    gather(0)
    lax.fori_loop(0, per_group, own_chip, 0)
    for i, (src, dst) in enumerate(((act_scr, act_out), (dz_scr, dz_out))):
        c = pltpu.make_async_copy(src, dst, out_sem.at[n_dev - 1 + i])
        c.start()
        outs.append(c)
    arrive(X, 2, (6, 4), (3, 1))
    arrive(I, 2, (6, 4), (3, 1))
    arrive(G, 4, (6, 2), (5, 1))
    arrive(I, 4, (5, 1))
    routing(2)
    arrive(X, 3)
    arrive(I, 3)
    routing(3)
    arrive(G, 2, (3, 1))
    arrive(X, 4, (5, 1))
    routing(4)
    arrive(G, 3)
    gather(2)
    for k in (X, G, I):
        arrive(k, 5)
    routing(5)
    gather(4)
    for k in (X, I):
        arrive(k, 6, (7, 1))
    routing(6)
    arrive(G, 6, (7, 1))
    for k in (X, I):
        arrive(k, 7)
    routing(7)
    arrive(G, 7)
    gather(6)
    stage.drain(0)
    stage.drain(1)
    for c in flights.values():
        c.wait_send()
    for c in outs:
        c.wait()


def back_kernel(q_ref, keep_ref, give_ref, peer_ref, q_out, part_in, q_in, send, recv, q_send, q_recv, ld_sem):
    n_dev = q_in.shape[0]
    greet(tuple(range(1, n_dev)))

    def push(src, dst, bit, s_sem, r_sem):
        c = pltpu.make_async_remote_copy(src_ref=src, dst_ref=dst, send_sem=s_sem, recv_sem=r_sem, device_id=device_of(bit), device_id_type=MESH)
        c.start()
        return c

    part = push(give_ref, part_in, 1, send.at[0], recv.at[0])
    load = pltpu.make_async_copy(keep_ref, peer_ref, ld_sem.at[0])
    load.start()
    qs = [push(q_ref, q_in.at[bit], bit, q_send.at[bit], q_recv.at[bit]) for bit in range(1, n_dev)]
    q_out[0] = q_ref[...]
    load.wait()
    part.wait_recv()
    peer_ref[...] += part_in[...]
    for i, c in enumerate(qs):
        c.wait_recv()
        q_out[i + 1] = q_in[i + 1]
    for c in qs + [part]:
        c.wait_send()


def expert_math(x, d, w1, w3, w2):
    z1 = nn_dot(x, w1)
    z3 = nn_dot(x, w3)
    sig = jax.nn.sigmoid(z1)
    silu = z1 * sig
    act = (silu * z3).astype(BF16)
    d_act = nt_dot(d, w2)
    dz1 = (d_act * z3 * sig * (1.0 + z1 * (1.0 - sig))).astype(BF16)
    dz3 = (d_act * silu).astype(BF16)
    return act, dz1, dz3


def flat(ref, first=0, count=None):
    v = ref[first : first + (count or ref.shape[0])]
    return v.reshape(v.shape[0] * v.shape[1], v.shape[2])


def hot_column(is_hot):
    return jnp.concatenate([jnp.full((EXTRA, 1), 1.0, F32) * h.astype(F32) for h in is_hot], axis=0) > 0.0


def masked(column, v):
    return jnp.where(column, v.astype(F32), 0.0).astype(BF16)


def pass1_kernel(per_group, order, hot_ref, ep_ref, w1_ref, w3_ref, w2_ref, x_ref, d_ref, g_ref, act01_ref, dz01_ref, q01_ref, xo_hbm, do_hbm, go_hbm, ms_ref, *refs):
    n_sh, n_all = len(order), hot_ref.shape[0]
    gx_hbms, (q_ref, g2_ref, dz_ref, dzo_ref, r_scr, gx_scr, xo_ref, do_ref, go_ref, gx_sem, more_sem) = refs[:n_sh], refs[n_sh:]
    more = [pltpu.make_async_copy(src, dst, more_sem.at[i]) for i, (src, dst) in enumerate(((xo_hbm, xo_ref), (do_hbm, do_ref), (go_hbm, go_ref)))]
    e = pl.program_id(0)
    ff = w1_ref.shape[2]
    w1, w3, w2 = w1_ref[0], w3_ref[0], w2_ref[0]
    base = per_group * SPAN
    m_of = lambda i: ms_ref.at[order[i], 0, 0]
    q_row = lambda i: pl.ds(order[i] * per_group + e, 1)

    def q_math(act, g):
        return jnp.sum(nn_dot(act, w2) * g.astype(F32), axis=1, keepdims=True)

    def r_math(dz1, dz3):
        return nt_dot(dz1, w1) + nt_dot(dz3, w3)

    @pl.when(e == 0)
    def _():
        for c in more:
            c.start()
        r_scr[:, base:, :] = jnp.zeros((n_sh, TAIL, r_scr.shape[2]), BF16)
        for i in range(per_group):
            r_scr[:, i * SPAN + SPAN - 16 : (i + 1) * SPAN, :] = jnp.zeros((n_sh, 16, r_scr.shape[2]), BF16)
        dzo_ref[...] = jnp.zeros_like(dzo_ref)
        q_ref[: 2 * per_group, :] = q01_ref[...]

    d = flat(d_ref)
    act, dz1, dz3 = expert_math(flat(x_ref), d[: x_ref.shape[0] * x_ref.shape[1]], w1, w3, w2)
    g2_ref[0] = tn_dot(jnp.concatenate([act, act01_ref[0]], axis=0), d)
    dz_ref[0, :, :ff] = dz1
    dz_ref[0, :, ff:] = dz3
    near = 2 * SLOTS
    q = q_math(act[:near], flat(g_ref))
    r = r_math(jnp.concatenate([dz1[:near], dz01_ref[0, :, :ff]], axis=0), jnp.concatenate([dz3[:near], dz01_ref[0, :, ff:]], axis=0))
    for i in range(n_sh):
        rows = slice(i * SLOTS, (i + 1) * SLOTS)
        if i < 2:
            mask = slot_mask(m_of(i)[pl.ds(e, 1), :], SLOTS, 0)
            q_ref[q_row(i), :] = jnp.sum(jnp.where(mask, q[rows], 0.0), axis=0, keepdims=True)
        r_scr[i, pl.ds(pl.multiple_of(e * SPAN, SPAN), SLOTS), :] = r[rows].astype(BF16)

    @pl.when(e == 0)
    def _():
        for c in more:
            c.wait()

    last = n_all // 2 - 1
    for near_part in (True, False):
        places = (0, last) if near_part else tuple(range(1, last))
        is_hot = [hot_ref[2 * place + k, e] for place in places for k in range(2)]

        @pl.when(sum(is_hot) > 0)
        def _():
            column = hot_column(is_hot)
            take = lambda ref: jnp.concatenate([ref[place] for place in places], axis=0)
            d = masked(column, take(do_ref))
            act, dz1, dz3 = expert_math(take(xo_ref), d, w1, w3, w2)
            g2_ref[0] += tn_dot(act, d)
            for i, place in enumerate(places):
                rows = slice(i * 2 * EXTRA, (i + 1) * 2 * EXTRA)
                dzo_ref[place, :, :ff] += dz1[rows]
                dzo_ref[place, :, ff:] += dz3[rows]
            if near_part:
                q, r = q_math(act, flat(go_ref)), r_math(dz1, dz3)
                for i in range(n_sh):
                    rows = slice(i * EXTRA, (i + 1) * EXTRA)

                    @pl.when(is_hot[i] > 0)
                    def _():
                        mask = slot_mask(m_of(i)[pl.ds(e, 1), :], EXTRA, SLOTS)
                        q_ref[q_row(i), :] += jnp.sum(jnp.where(mask, q[rows], 0.0), axis=0, keepdims=True)
                        r_scr[i, base : base + EXTRA, :] = r[rows].astype(BF16)

    @pl.when(e == per_group - 1)
    def _():
        outs = []
        for i in range(n_sh - 1, -1, -1):
            rank = m_of(i)[...]
            low = jnp.where(rank < SLOTS, rank, -1.0)
            masks = [slot_mask(low[k : k + 1, :], SPAN, 0) for k in range(per_group)]
            masks.append(slot_mask(extra_rank(rank), TAIL, SLOTS))
            pick = jnp.concatenate([m.astype(F32) for m in masks], axis=0).astype(BF16)
            gx_scr[i] = tn_dot(pick, r_scr[i])
            outs.append(pltpu.make_async_copy(gx_scr.at[i], gx_hbms[order[i]], gx_sem.at[i]))
            outs[-1].start()
        for c in outs:
            c.wait()


def pass2_kernel(hot_ref, dz_ref, dz01_ref, x_ref, xo_hbm, dzo_hbm, g1_ref, g3_ref, xo_ref, dzo_ref, more_sem):
    e = pl.program_id(0)
    pieces = ((xo_hbm, xo_ref), (dzo_hbm, dzo_ref))
    more = [pltpu.make_async_copy(src, dst, more_sem.at[i]) for i, (src, dst) in enumerate(pieces)]

    @pl.when(e == 0)
    def _():
        for c in more:
            c.start()

    ff = g1_ref.shape[2]
    x = flat(x_ref)
    g1_ref[0] = tn_dot(x, jnp.concatenate([dz_ref[0, :, :ff], dz01_ref[0, :, :ff]], axis=0))
    g3_ref[0] = tn_dot(x, jnp.concatenate([dz_ref[0, :, ff:], dz01_ref[0, :, ff:]], axis=0))

    @pl.when(e == 0)
    def _():
        for c in more:
            c.wait()

    is_hot = [hot_ref[j, e] for j in range(hot_ref.shape[0])]

    @pl.when(sum(is_hot) > 0)
    def _():
        column = hot_column(is_hot)
        x = flat(xo_ref)
        dz = masked(column, flat(dzo_ref))
        g1_ref[0] += tn_dot(x, dz[:, :ff])
        g3_ref[0] += tn_dot(x, dz[:, ff:])


def finish_kernel(per_group, groups, ep_ref, own_ref, near_ref, far_ref, wr_ref, x0_ref, xs_ref, ms_ref, q_ref, gx_ref, gr_ref, wr_scr, acc):
    n_sh = q_ref.shape[0]
    ep = ep_ref[0]
    span = lambda m: slice(m * per_group, (m + 1) * per_group)
    for a in range(groups):

        @pl.when(ep == a)
        def _():
            for m in range(groups):
                wr_scr[span(m), :] = wr_ref[span(a ^ m), :]

    for s in range(n_sh):
        d, j = divmod(s, groups)
        q = [q_ref[d * groups + m, span(m ^ j), :] for m in range(groups)]
        p = [ms_ref[s, 0, ep ^ m][:per_group] for m in range(groups)]
        mean = sum(jnp.sum(a * b, axis=0, keepdims=True) for a, b in zip(p, q))
        dl = jnp.concatenate([a * (b - mean) for a, b in zip(p, q)], axis=0).astype(BF16)
        term = nn_dot(dl, x0_ref[...] if s == 0 else xs_ref[s - 1])
        if s == 0:
            gx_ref[...] = (own_ref[...] + near_ref[...] + far_ref[...] + tn_dot(dl, wr_scr[...])).astype(BF16)
            acc[...] = term
        else:
            acc[...] += term
    for a in range(groups):

        @pl.when(ep == a)
        def _():
            for m in range(groups):
                gr_ref[span(a ^ m), :] = acc[span(m), :]


def solution(mesh):
    dp, ep = mesh.shape["dp"], mesh.shape["ep"]
    n_dev = dp * ep
    tok_spec = P(("dp", "ep"), None)
    exp_spec = P("ep", None, None)

    def swap(v, bit):
        return lax.ppermute(v, ("dp", "ep"), [(s, s ^ bit) for s in range(n_dev)])

    def device_step(x_loc, route_idx, w_router, w_gate, w_up, w_down, dy_loc):
        toks, dim = x_loc.shape
        top_k = route_idx.shape[1]
        n_exp = w_router.shape[1]
        n_loc, _, ff = w_gate.shape
        me = lax.axis_index("ep")
        ep_arr = me.reshape(1).astype(jnp.int32)
        vmem = pl.BlockSpec(memory_space=pltpu.VMEM)
        params = pltpu.CompilerParams(vmem_limit_bytes=VMEM_LIMIT)

        m_shape = (2, ep, PAD, toks)
        hbm = pl.BlockSpec(memory_space=pl.ANY)
        main = n_loc * 2 * SLOTS
        pairs = n_dev // 2
        sds = jax.ShapeDtypeStruct
        others = n_dev - 1
        x_rows, x_more, d_rows, d_more, g_rows, g_more, xs, act01, dz01, ms, hot, q01 = pl.pallas_call(
            functools.partial(near_kernel, n_loc),
            out_shape=[
                sds((pairs, main, dim), BF16),
                sds((pairs, 2 * EXTRA, dim), BF16),
                sds((pairs, main, dim), BF16),
                sds((pairs, 2 * EXTRA, dim), BF16),
                sds((ep // 2, main, dim), BF16),
                sds((ep // 2, 2 * EXTRA, dim), BF16),
                sds((others, toks, dim), BF16),
                sds((n_loc, 2 * SLOTS, ff), BF16),
                sds((n_loc, 2 * SLOTS, 2 * ff), BF16),
                sds((n_dev,) + m_shape, F32),
                sds((n_dev, 128), jnp.int32),
                sds((2 * n_loc, toks), F32),
            ],
            in_specs=[vmem] * 4 + [hbm] * 3,
            out_specs=[hbm] * 9 + [vmem] * 3,
            scratch_shapes=[
                pltpu.VMEM((others, toks, dim), BF16),
                pltpu.VMEM((others, toks, dim), BF16),
                pltpu.VMEM((others, top_k, toks), jnp.int32),
                pltpu.VMEM((2, main + 2 * EXTRA, dim), BF16),
                pltpu.VMEM((2, main + 2 * EXTRA, dim), BF16),
                pltpu.VMEM((2, main + 2 * EXTRA, dim), BF16),
                pltpu.VMEM((2, dim, ff), BF16),
                pltpu.VMEM((2, dim, ff), BF16),
                pltpu.VMEM((2, ff, dim), BF16),
                pltpu.VMEM((n_loc, 2 * SLOTS, ff), BF16),
                pltpu.VMEM((n_loc, 2 * SLOTS, 2 * ff), BF16),
                pltpu.SemaphoreType.DMA((others, 3)),
                pltpu.SemaphoreType.DMA((others, 3)),
                pltpu.SemaphoreType.DMA((others + 2,)),
                pltpu.SemaphoreType.DMA((2, 6)),
                pltpu.SemaphoreType.DMA((2, 3)),
            ],
            compiler_params=pltpu.CompilerParams(collective_id=0, has_side_effects=True, vmem_limit_bytes=VMEM_LIMIT),
            cost_estimate=pl.CostEstimate(flops=2 * 10**10, bytes_accessed=5 * 10**7, transcendentals=0),
            name="near",
        )(x_loc, dy_loc, route_idx.T, w_router.T, w_gate, w_up, w_down)

        w_specs = lambda im: [pl.BlockSpec((1, dim, ff), im), pl.BlockSpec((1, dim, ff), im), pl.BlockSpec((1, ff, dim), im)]
        im3 = lambda e, hot, ep_ref: (e, 0, 0)
        rows_at = lambda e, hot, ep_ref: (0, e, 0)
        fix = lambda shape: pl.BlockSpec(shape, lambda e, hot, ep_ref: (0,) * len(shape), pipeline_mode=pl.Buffered(1))
        n_row = (n_dev - 2) * SLOTS
        *gx_part, q_loc, grad_down, dz, dz_more = pl.pallas_call(
            functools.partial(pass1_kernel, n_loc, (2, 3, 0, 1)),
            out_shape=[sds((toks, dim), F32)] * ep
            + [
                sds((ep * n_loc, toks), F32),
                sds((n_loc, ff, dim), F32),
                sds((n_loc, n_row, 2 * ff), BF16),
                sds((pairs, 2 * EXTRA, 2 * ff), BF16),
            ],
            grid_spec=pltpu.PrefetchScalarGridSpec(
                num_scalar_prefetch=2,
                grid=(n_loc,),
                in_specs=w_specs(im3)
                + [pl.BlockSpec((pairs - 1, 2 * SLOTS, dim), rows_at), pl.BlockSpec((pairs, 2 * SLOTS, dim), rows_at)]
                + [pl.BlockSpec((1, 2 * SLOTS, dim), rows_at), pl.BlockSpec((1, 2 * SLOTS, ff), im3), pl.BlockSpec((1, 2 * SLOTS, 2 * ff), im3), fix((2 * n_loc, toks))]
                + [hbm] * 3
                + [pl.BlockSpec((ep, 1, 1, PAD, toks), lambda e, hot, ep_ref: (0, 0, ep_ref[0], 0, 0))],
                out_specs=[hbm] * ep
                + [fix((ep * n_loc, toks)), pl.BlockSpec((1, ff, dim), im3), pl.BlockSpec((1, n_row, 2 * ff), im3)]
                + [fix((pairs, 2 * EXTRA, 2 * ff))],
                scratch_shapes=[
                    pltpu.VMEM((ep, n_loc * SPAN + TAIL, dim), BF16),
                    pltpu.VMEM((ep, toks, dim), F32),
                    pltpu.VMEM((pairs, 2 * EXTRA, dim), BF16),
                    pltpu.VMEM((pairs, 2 * EXTRA, dim), BF16),
                    pltpu.VMEM((ep // 2, 2 * EXTRA, dim), BF16),
                    pltpu.SemaphoreType.DMA((ep,)),
                    pltpu.SemaphoreType.DMA((3,)),
                ],
            ),
            compiler_params=params,
            cost_estimate=pl.CostEstimate(flops=4 * 10**10, bytes_accessed=10**8, transcendentals=0),
            name="pass1",
        )(hot, ep_arr, w_gate, w_up, w_down, x_rows, d_rows, g_rows, act01, dz01, q01, x_more, d_more, g_more, ms)

        for_peer, q_all = pl.pallas_call(
            back_kernel,
            out_shape=[sds((toks, dim), F32), sds((n_dev, ep * n_loc, toks), F32)],
            in_specs=[vmem, hbm, hbm],
            out_specs=[vmem] * 2,
            scratch_shapes=[
                pltpu.VMEM((toks, dim), F32),
                pltpu.VMEM((n_dev, ep * n_loc, toks), F32),
                pltpu.SemaphoreType.DMA((1,)),
                pltpu.SemaphoreType.DMA((1,)),
                pltpu.SemaphoreType.DMA((n_dev,)),
                pltpu.SemaphoreType.DMA((n_dev,)),
                pltpu.SemaphoreType.DMA((1,)),
            ],
            compiler_params=pltpu.CompilerParams(collective_id=1, has_side_effects=True, vmem_limit_bytes=VMEM_LIMIT),
            cost_estimate=pl.CostEstimate(flops=8 * 10**9, bytes_accessed=5 * 10**7, transcendentals=0),
            name="back",
        )(q_loc, gx_part[2], gx_part[3])
        for_peer, for_core = lax.optimization_barrier((for_peer, gx_part[1]))
        from_peer = swap(for_peer, 2)
        from_core = swap(for_core, 1)

        im3 = lambda e, hot: (e, 0, 0)
        rows_at = lambda e, hot: (0, e, 0)
        fix = lambda shape: pl.BlockSpec(shape, lambda e, hot: (0,) * len(shape), pipeline_mode=pl.Buffered(1))
        grad_gate, grad_up = pl.pallas_call(
            pass2_kernel,
            out_shape=[sds((n_loc, dim, ff), F32)] * 2,
            grid_spec=pltpu.PrefetchScalarGridSpec(
                num_scalar_prefetch=1,
                grid=(n_loc,),
                in_specs=[pl.BlockSpec((1, n_row, 2 * ff), im3), pl.BlockSpec((1, 2 * SLOTS, 2 * ff), im3)]
                + [pl.BlockSpec((pairs, 2 * SLOTS, dim), rows_at)]
                + [hbm] * 2,
                out_specs=[pl.BlockSpec((1, dim, ff), im3)] * 2,
                scratch_shapes=[
                    pltpu.VMEM((pairs, 2 * EXTRA, dim), BF16),
                    pltpu.VMEM((pairs, 2 * EXTRA, 2 * ff), BF16),
                    pltpu.SemaphoreType.DMA((2,)),
                ],
            ),
            compiler_params=params,
            cost_estimate=pl.CostEstimate(flops=6 * 10**10, bytes_accessed=2 * 10**8, transcendentals=0),
            name="pass2",
        )(hot, dz, dz01, x_rows, x_more, dz_more)

        fixed = lambda shape: pl.BlockSpec(shape, lambda i, ep_ref: (0,) * len(shape))
        grad_x, grad_rt = pl.pallas_call(
            functools.partial(finish_kernel, n_loc, ep),
            out_shape=[sds((toks, dim), BF16), sds((n_exp, dim), F32)],
            grid_spec=pltpu.PrefetchScalarGridSpec(
                num_scalar_prefetch=1,
                grid=(1,),
                in_specs=[fixed(v.shape) for v in (gx_part[0], from_core, from_peer, w_router.T, x_loc, xs)]
                + [pl.BlockSpec((n_dev, 1, ep, PAD, toks), lambda i, ep_ref: (0, 1, 0, 0, 0)), fixed(q_all.shape)],
                out_specs=[fixed((toks, dim)), fixed((n_exp, dim))],
                scratch_shapes=[pltpu.VMEM((n_exp, dim), BF16), pltpu.VMEM((n_exp, dim), F32)],
            ),
            compiler_params=params,
            cost_estimate=pl.CostEstimate(flops=4 * 10**9, bytes_accessed=10**7, transcendentals=0),
            name="finish",
        )(ep_arr, gx_part[0], from_core, from_peer, w_router.T, x_loc, xs, ms, q_all)
        grad_router = grad_rt.T
        return grad_x, grad_gate, grad_up, grad_down, grad_router

    return jax.shard_map(device_step, mesh=mesh, in_specs=(tok_spec, tok_spec, P(), exp_spec, exp_spec, exp_spec, tok_spec), out_specs=(tok_spec, exp_spec, exp_spec, exp_spec, P()), check_vma=False)
```
